16 devices in a mesh: dp: 16 (over z, y, x, core).
Axes of the slice: x: 2, y: 2, z: 2, core: 2. Of those that a mesh axis runs over, the one named last changes fastest.
Arguments:
- grad_embed: bfloat16 [16, 16384, 640], P('dp')
- grad_q: bfloat16 [16, 6, 640, 64], P('dp')
- grad_k: bfloat16 [16, 6, 640, 16], P('dp')
- grad_v: bfloat16 [16, 6, 640, 16], P('dp')
- grad_out: bfloat16 [16, 6, 64, 640], P('dp')
- grad_gate: bfloat16 [16, 6, 640, 128], P('dp')
- grad_up: bfloat16 [16, 6, 640, 128], P('dp')
- grad_down: bfloat16 [16, 6, 128, 640], P('dp')
- grad_norms: bfloat16 [16, 6, 4, 640], P('dp')
- grad_qk_norms: bfloat16 [16, 6, 2, 256], P('dp')
- first_moment: float32 [12593152], P('dp')
- second_moment: float32 [12593152], P('dp')
- master_param: float32 [12593152], P('dp')
- hyper_params: float32 [5], replicated
Outputs:
- output 1: bfloat16 [16384, 640], replicated
- output 2: bfloat16 [6, 640, 64], replicated
- output 3: bfloat16 [6, 640, 16], replicated
- output 4: bfloat16 [6, 640, 16], replicated
- output 5: bfloat16 [6, 64, 640], replicated
- output 6: bfloat16 [6, 640, 128], replicated
- output 7: bfloat16 [6, 640, 128], replicated
- output 8: bfloat16 [6, 128, 640], replicated
- output 9: bfloat16 [6, 4, 640], replicated
- output 10: bfloat16 [6, 2, 256], replicated
- output 11: float32 [12593152], P('dp')
- output 12: float32 [12593152], P('dp')
- output 13: float32 [12593152], P('dp')
All inputs are finite; a program needn't handle non-finite values.
Results may differ from the reference program's by a relative error of at most 0.001.
Values are sent between devices in bfloat16 or wider.
A program may use at most 1 GiB of HBM per device.

```python
import math
import jax
import jax.numpy as jnp

D_MODEL = 640
FF_WIDTH = 2048
Q_HEADS = 4
KV_HEADS = 1
HEAD_DIM = 256
VOCAB_SIZE = 262144
TP_RANKS = 16
NUM_LAYERS = 6
DATA_PAR = 16
ADAM_STEP = 7

ADAM_EPS = 1e-8
CLIP_EPS = 1e-6
Q_COLS = Q_HEADS * HEAD_DIM // TP_RANKS
KV_COLS = KV_HEADS * HEAD_DIM // TP_RANKS
FF_COLS = FF_WIDTH // TP_RANKS
VOCAB_ROWS = VOCAB_SIZE // TP_RANKS
PARAM_SHAPES = ((VOCAB_ROWS, D_MODEL), (NUM_LAYERS, D_MODEL, Q_COLS), (NUM_LAYERS, D_MODEL, KV_COLS), (NUM_LAYERS, D_MODEL, KV_COLS), (NUM_LAYERS, Q_COLS, D_MODEL), (NUM_LAYERS, D_MODEL, FF_COLS), (NUM_LAYERS, D_MODEL, FF_COLS), (NUM_LAYERS, FF_COLS, D_MODEL), (NUM_LAYERS, 4, D_MODEL), (NUM_LAYERS, 2, HEAD_DIM))
PARAM_SIZES = tuple(math.prod(tensor_dims) for tensor_dims in PARAM_SHAPES)
PARAMS_TOTAL = sum(PARAM_SIZES)
DECAY_LEN = PARAMS_TOTAL - PARAM_SIZES[8] - PARAM_SIZES[9]
GRAD_NAMES = ("grad_embed", "grad_q", "grad_k", "grad_v", "grad_out", "grad_gate", "grad_up", "grad_down", "grad_norms", "grad_qk_norms")


def setup_inputs(seed: int = 0) -> dict:
    key_list = jax.random.split(jax.random.key(seed), 16)
    grad_scale = math.sqrt(DATA_PAR)
    inputs = {}
    square_sum = jnp.float32(0.0)
    for tensor_index, tensor_dims in enumerate(PARAM_SHAPES):
        noise_draw = jax.random.normal(key_list[tensor_index], (DATA_PAR,) + tensor_dims, jnp.float32)
        grad_arr = (grad_scale * noise_draw).astype(jnp.bfloat16)
        mean_grad = jnp.sum(grad_arr, axis=0, dtype=jnp.float32) / DATA_PAR
        square_sum = square_sum + jnp.sum(mean_grad * mean_grad)
        inputs[GRAD_NAMES[tensor_index]] = grad_arr
    inputs["first_moment"] = 0.1 * jax.random.normal(key_list[10], (PARAMS_TOTAL,), jnp.float32)
    inputs["second_moment"] = 0.015 * jnp.exp(0.5 * jax.random.normal(key_list[11], (PARAMS_TOTAL,), jnp.float32))
    inputs["master_param"] = 0.5 * jax.random.normal(key_list[12], (PARAMS_TOTAL,), jnp.float32)
    hyper_draw = jax.random.uniform(key_list[13], (5,), jnp.float32)
    inputs["hyper_params"] = jnp.stack([0.05 + 0.1 * hyper_draw[0], 0.8 + 0.15 * hyper_draw[1], 0.9 + 0.09 * hyper_draw[2], 0.3 + 1.2 * hyper_draw[3], (0.3 + 0.4 * hyper_draw[4]) * jnp.sqrt(square_sum)])
    return inputs


def reference(grad_embed, grad_q, grad_k, grad_v, grad_out, grad_gate, grad_up, grad_down, grad_norms, grad_qk_norms, first_moment, second_moment, master_param, hyper_params):
    grads = (grad_embed, grad_q, grad_k, grad_v, grad_out, grad_gate, grad_up, grad_down, grad_norms, grad_qk_norms)
    mean_grad = jnp.concatenate([jnp.sum(grad_arr, axis=0, dtype=jnp.float32).reshape(-1) for grad_arr in grads]) / DATA_PAR
    learn_rate = hyper_params[0]
    beta_one = hyper_params[1]
    beta_two = hyper_params[2]
    weight_decay = hyper_params[3]
    grad_norm = jnp.sqrt(jnp.sum(mean_grad * mean_grad))
    clip_scale = jnp.minimum(1.0, hyper_params[4] / (grad_norm + CLIP_EPS))
    clipped = mean_grad * clip_scale
    moment_one = beta_one * first_moment + (1.0 - beta_one) * clipped
    moment_two = beta_two * second_moment + (1.0 - beta_two) * (clipped * clipped)
    m_hat = moment_one / (1.0 - beta_one ** ADAM_STEP)
    v_hat = moment_two / (1.0 - beta_two ** ADAM_STEP)
    keep_decay = jnp.arange(PARAMS_TOTAL) < DECAY_LEN
    direction = m_hat / (jnp.sqrt(v_hat) + ADAM_EPS) + jnp.where(keep_decay, weight_decay * master_param, 0.0)
    new_master = master_param - learn_rate * direction
    new_params = new_master.astype(jnp.bfloat16)
    out_list = []
    start_pos = 0
    for tensor_dims, tensor_size in zip(PARAM_SHAPES, PARAM_SIZES):
        out_list.append(new_params[start_pos:start_pos + tensor_size].reshape(tensor_dims))
        start_pos = start_pos + tensor_size
    return (out_list[0], out_list[1], out_list[2], out_list[3], out_list[4], out_list[5], out_list[6], out_list[7], out_list[8], out_list[9], moment_one, moment_two, new_master)
```

```python
import functools
import math
import jax
import jax.numpy as jnp
from jax import lax
from jax.experimental import pallas as pl
from jax.experimental.pallas import tpu as pltpu
from jax.sharding import PartitionSpec as P

ADAM_STEP = 7
ADAM_EPS = 1e-8
CLIP_EPS = 1e-6
GRAD_COUNT = 10
MESH = pl.DeviceIdType.MESH

DEVS = 16
WIDTH = 640
SHARD_ROWS = 6149
TILE_ROWS = 40
EMBED_TILES = 2048
ALL_TILES = 2460
DECAY_ROWS = 98240
FIRST_TAIL = 13
TAIL_START = (SHARD_ROWS * FIRST_TAIL) // TILE_ROWS
RS_TILES = 52
TAIL_TILES = (SHARD_ROWS * 15) // TILE_ROWS + 3 * RS_TILES - TAIL_START
AG_TILES = 51
LEAD = 40
G_ROWS = LEAD + 3 * RS_TILES * TILE_ROWS
ORDERS = ((2, 4, 8), (4, 8, 2), (8, 2, 4))


def flip(dev, stride):
    return dev + stride - 2 * stride * lax.rem(dev // stride, 2)


def rs_start(dev):
    return (SHARD_ROWS * dev) // TILE_ROWS


def ag_start(dev):
    return (SHARD_ROWS * dev + TILE_ROWS - 1) // TILE_ROWS


def flip_mask(dev, order, mask):
    for bit, stride in enumerate(order):
        if mask >> bit & 1:
            dev = flip(dev, stride)
    return dev


def kernel(emb, tail, m_in, v_in, p_in, hyp, vout, m_out, v_out, p_out,
           own, r1, s1, r2, r3, mom, vel, par, ext, grad, stage, nsend, nrecv,
           own_sem, r1_send, r1_recv, r2_send, r2_recv, r3_send, r3_recv, st_sem,
           ext_send, ext_recv, n_send, n_recv, ag_send, ag_recv, d2d_send, d2d_recv, loc_sem):
    me = lax.axis_index("dp")
    partner = flip(me, 1)

    def remote(src, dst, ssem, rsem, dev):
        return pltpu.make_async_remote_copy(
            src_ref=src, dst_ref=dst, send_sem=ssem, recv_sem=rsem, device_id=(dev,), device_id_type=MESH)

    def from_shard(owner, k, make):
        first = rs_start(owner) + k * RS_TILES

        @pl.when(owner < FIRST_TAIL)
        def _():
            make(emb.at[pl.ds(first, RS_TILES)]).start()

        @pl.when(owner >= FIRST_TAIL)
        def _():
            make(tail.at[pl.ds(first - TAIL_START, RS_TILES)]).start()

    def rs_owner(dev, k, f):
        return flip_mask(dev, ORDERS[k], (0 if f >= 2 else 2) + (4 if f % 2 == 0 else 0))

    state = [pltpu.make_async_copy(src, dst, st_sem.at[i])
             for i, (src, dst) in enumerate(((m_in, mom), (v_in, vel), (p_in, par)))]

    for f in range(4):
        for k in range(3):
            from_shard(rs_owner(me, k, f), k,
                       lambda src, k=k, f=f: pltpu.make_async_copy(src, own.at[k, f], own_sem.at[k, f]))
    barrier = pltpu.get_barrier_semaphore()
    for j in range(1, DEVS):
        pl.semaphore_signal(barrier, inc=1, device_id=(lax.rem(me + j, DEVS),), device_id_type=MESH)
    pl.semaphore_wait(barrier, DEVS - 1)

    for f in range(4):
        for k in range(3):
            for slot in range(3):
                dev = partner if slot == 2 else flip(me, ORDERS[k][0])
                if slot == 1:
                    dev = flip(dev, 1)
                from_shard(rs_owner(dev, k, f), k, lambda src, k=k, f=f, slot=slot, dev=dev: remote(
                    src, r1.at[slot, k, f], r1_send.at[slot, k, f], r1_recv.at[slot, k, f], dev))
    before = lax.rem(me + DEVS - 1, DEVS)
    ext_copies = [remote(src.at[pl.ds(0, TILE_ROWS)], ext.at[i], ext_send.at[i], ext_recv.at[i], before)
                  for i, src in enumerate((m_in, v_in, p_in))]
    for copy in ext_copies:
        copy.start()
    for copy in state:
        copy.start()

    def r1_copy(slot, k, f):
        return remote(emb.at[pl.ds(0, RS_TILES)], r1.at[slot, k, f], r1_send.at[slot, k, f],
                      r1_recv.at[slot, k, f], partner)

    def r2_copy(k, f):
        return remote(s1.at[k, f], r2.at[k, f], r2_send.at[k, f], r2_recv.at[k, f], flip(me, ORDERS[k][1]))

    def r3_copy(k):
        return remote(s1.at[k, 2], r3.at[k], r3_send.at[k], r3_recv.at[k], flip(me, ORDERS[k][2]))

    for f in range(4):
        for k in range(3):
            pltpu.make_async_copy(emb.at[pl.ds(0, RS_TILES)], own.at[k, f], own_sem.at[k, f]).wait()
            for slot in (2, 0, 1):
                r1_copy(slot, k, f).wait_recv()

            def add_four(t, _, k=k, f=f):
                s1[k, f, t] = ((own[k, f, t].astype(jnp.float32) + r1[2, k, f, t].astype(jnp.float32))
                               + (r1[0, k, f, t].astype(jnp.float32) + r1[1, k, f, t].astype(jnp.float32)))
                return 0

            lax.fori_loop(0, RS_TILES, add_four, 0, unroll=2)
            if f < 2:
                r2_copy(k, f).start()
    for f in range(2):
        for k in range(3):
            r2_copy(k, f).wait_recv()

            def add_two(t, _, k=k, f=f):
                s1[k, 2 + f, t] = s1[k, 2 + f, t] + r2[k, f, t]
                return 0

            lax.fori_loop(0, RS_TILES, add_two, 0, unroll=2)
            if f == 0:
                r3_copy(k).start()

    shift = LEAD - (SHARD_ROWS * me - TILE_ROWS * rs_start(me))
    for k in range(3):
        r3_copy(k).wait_recv()

        def finish(t, _, k=k):
            total = (s1[k, 3, t] + r3[k, t]) * (1.0 / DEVS)
            row = shift + TILE_ROWS * (k * RS_TILES + t)
            for j in range(WIDTH // 128):
                grad[pl.ds(row + j, 8, stride=WIDTH // 128), :] = total[:, 128 * j:128 * (j + 1)]
            return 0

        lax.fori_loop(0, RS_TILES, finish, 0, unroll=2)

    def squares(i, acc):
        part = grad[pl.ds(pl.multiple_of(LEAD + i * 40, 8), 40), :]
        return acc + part * part

    acc = lax.fori_loop(0, 153, squares, jnp.zeros((40, 128), jnp.float32), unroll=3)
    nsend[...] = acc[0:8] + acc[8:16] + acc[16:24] + acc[24:32] + acc[32:40]
    for row in (6120, 6128, 6136):
        part = grad[pl.ds(LEAD + row, 8), :]
        nsend[...] = nsend[...] + part * part
    part = grad[pl.ds(LEAD + 6144, 5), :]
    nsend[0:5, :] = nsend[0:5, :] + part * part

    def n_copy(j):
        return remote(nsend, nrecv.at[me], n_send.at[j], n_recv.at[me], lax.rem(me + j, DEVS))

    for j in range(1, DEVS):
        n_copy(j).start()

    def full(value):
        return jnp.full((8, 128), value, jnp.float32)

    learn_rate, beta_one, beta_two, decay, max_norm = [full(hyp[i]) for i in range(5)]
    rest_one, rest_two = 1.0 - beta_one, 1.0 - beta_two
    hat_one = 1.0 / (1.0 - lax.integer_pow(beta_one, ADAM_STEP))
    hat_two = 1.0 / (1.0 - lax.integer_pow(beta_two, ADAM_STEP))
    for copy in state:
        copy.wait()
    for copy in ext_copies:
        copy.wait_recv()

    for j in range(1, DEVS):
        n_copy(j).wait_send()
        source = lax.rem(me + DEVS - j, DEVS)
        remote(nsend, nrecv.at[source], n_send.at[j], n_recv.at[source], partner).wait_recv()
    nrecv[me] = nsend[...]
    total = nrecv[0]
    for j in range(1, DEVS):
        total = total + nrecv[j]
    total = jnp.sum(jnp.sum(total, axis=1, keepdims=True), axis=0, keepdims=True)
    clip = jnp.minimum(1.0, max_norm / (jnp.sqrt(jnp.broadcast_to(total, (8, 128))) + CLIP_EPS))

    def wide(value, rows):
        if rows <= 8:
            return value[:rows]
        return jnp.concatenate([value] * (rows // 8), axis=0)

    def adam(g, m, v, p, first_row, rows):
        clipped = g * wide(clip, rows)
        m = wide(beta_one, rows) * m + wide(rest_one, rows) * clipped
        v = wide(beta_two, rows) * v + wide(rest_two, rows) * (clipped * clipped)
        index = first_row + lax.broadcasted_iota(jnp.int32, (rows, 128), 0)
        update = (m * wide(hat_one, rows)) / (jnp.sqrt(v * wide(hat_two, rows)) + ADAM_EPS)
        update = update + jnp.where(index < DECAY_ROWS, wide(decay, rows) * p, 0.0)
        return m, v, p - wide(learn_rate, rows) * update

    def adam_rows(row, rows):
        at = pl.ds(row, rows)
        shifted = pl.ds(row + LEAD, rows)
        m, v, p = adam(grad[shifted, :], mom[at, :], vel[at, :], par[at, :], SHARD_ROWS * me + row, rows)
        mom[at, :] = m
        vel[at, :] = v
        par[at, :] = p
        grad[shifted, :] = p

    def adam_block(i, _):
        adam_rows(pl.multiple_of(i * 40, 8), 40)
        return 0

    def ag_sizes(owner, k, run):
        if k < 2:
            run(AG_TILES)
            return
        longer = ag_start(owner + 1) - ag_start(owner) == 3 * AG_TILES + 1

        @pl.when(longer)
        def _():
            run(AG_TILES + 1)

        @pl.when(jnp.logical_not(longer))
        def _():
            run(AG_TILES)

    def ag_each(k, mask, run, dev=me):
        owner = flip_mask(dev, ORDERS[k], mask)
        first = ag_start(owner) + k * AG_TILES
        ag_sizes(owner, k, lambda size: run(vout.at[pl.ds(first, size)], size))

    def ag_link(k, mask, link):
        dev = flip(me, ORDERS[k][link])
        slot = mask + (1 << link)

        def copy(dst, size):
            src = stage.at[k, pl.ds(0, size)] if mask == 0 else dst
            return remote(src, dst, ag_send.at[k, slot], ag_recv.at[k, slot], dev)

        ag_each(k, mask, lambda dst, size: copy(dst, size).start())
        pending.append(lambda: ag_each(k, mask, lambda dst, size: copy(dst, size).wait_send()))

    def ag_across(k, mask):
        def copy(dst, size):
            src = stage.at[k, pl.ds(0, size)] if mask == 0 else dst
            return remote(src, dst, d2d_send.at[k, mask], d2d_recv.at[k, mask], partner)

        ag_each(k, mask, lambda dst, size: copy(dst, size).start())
        pending.append(lambda: ag_each(k, mask, lambda dst, size: copy(dst, size).wait_send()))

    def ag_arrived(k, mask):
        ag_each(k, mask, lambda dst, size: remote(
            dst, dst, ag_send.at[k, mask], ag_recv.at[k, mask], partner).wait_recv())

    pending = []
    bounds = ((0, 52), (52, 103), (103, 153))
    base = LEAD + TILE_ROWS * ag_start(me) - SHARD_ROWS * me
    for k in range(3):
        lax.fori_loop(bounds[k][0], bounds[k][1], adam_block, 0, unroll=1)
        if k == 2:
            adam_rows(6120, 24)
            adam_rows(6144, 5)
            at = pl.ds(LEAD + SHARD_ROWS, 40)
            _, _, p = adam(grad[at, :], ext[0], ext[1], ext[2], SHARD_ROWS * (me + 1), 40)
            grad[at, :] = p

        def pack(t, _, k=k):
            row = base + TILE_ROWS * (k * AG_TILES + t)
            for j in range(WIDTH // 128):
                stage[k, t, :, 128 * j:128 * (j + 1)] = grad[
                    pl.ds(row + j, 8, stride=WIDTH // 128), :].astype(jnp.bfloat16)
            return 0

        lax.fori_loop(0, AG_TILES + (1 if k == 2 else 0), pack, 0, unroll=1)
        ag_link(k, 0, 0)
    for k in range(3):
        ag_link(k, 0, 1)
    for k in range(3):
        ag_link(k, 0, 2)
    results = [pltpu.make_async_copy(src, dst, st_sem.at[i])
               for i, (src, dst) in enumerate(((mom, m_out), (vel, v_out), (par, p_out)))]
    for copy in results:
        copy.start()

    def ag_local(k):
        return lambda dst, size: pltpu.make_async_copy(stage.at[k, pl.ds(0, size)], dst, loc_sem.at[k])

    for k in range(3):
        ag_across(k, 0)
        ag_each(k, 0, lambda dst, size, k=k: ag_local(k)(dst, size).start())
    for k in range(3):
        ag_arrived(k, 1)
        ag_link(k, 1, 1)
        ag_across(k, 1)
    for k in range(3):
        ag_link(k, 1, 2)
    for k in range(3):
        ag_arrived(k, 2)
        ag_link(k, 2, 2)
        ag_across(k, 2)
    for k in range(3):
        ag_arrived(k, 4)
        ag_across(k, 4)
    for k in range(3):
        ag_arrived(k, 3)
        ag_link(k, 3, 2)
        ag_across(k, 3)
    for mask in (5, 6, 7):
        for k in range(3):
            ag_arrived(k, mask)
            ag_across(k, mask)
    for k in range(3):
        ag_each(k, 0, lambda dst, size, k=k: ag_local(k)(dst, size).wait())
    for mask in range(8):
        for k in range(3):
            ag_each(k, mask, lambda dst, size, k=k, mask=mask: remote(
                dst, dst, d2d_send.at[k, mask], d2d_recv.at[k, mask], partner).wait_recv(), partner)
    for wait in pending:
        wait()
    for copy in results:
        copy.wait()
    for copy in ext_copies:
        copy.wait_send()
    for f in range(4):
        for k in range(3):
            for slot in range(3):
                r1_copy(slot, k, f).wait_send()
            if f < 2:
                r2_copy(k, f).wait_send()
    for k in range(3):
        r3_copy(k).wait_send()


def solution(mesh):
    def local_update(*arrays):
        grads = arrays[:GRAD_COUNT]
        state = [arr.reshape(SHARD_ROWS, 128) for arr in arrays[GRAD_COUNT:GRAD_COUNT + 3]]
        shapes = [grad_arr.shape[1:] for grad_arr in grads]
        sizes = [math.prod(tensor_dims) for tensor_dims in shapes]
        emb = grads[0].reshape(EMBED_TILES, 8, WIDTH)
        tail_len = (TAIL_TILES + TAIL_START - EMBED_TILES) * 8 * WIDTH
        flat = [grad_arr.reshape(-1) for grad_arr in grads[1:]]
        flat.append(jnp.zeros((tail_len - sum(sizes[1:]),), jnp.bfloat16))
        tail = jnp.concatenate(flat).reshape(-1, 8, WIDTH)
        tail = jnp.concatenate([emb[TAIL_START:], tail], axis=0)
        any_spec = pl.BlockSpec(memory_space=pl.ANY)
        dma = pltpu.SemaphoreType.DMA
        bf16, f32 = jnp.bfloat16, jnp.float32
        vout, first, second, master = pl.pallas_call(
            kernel,
            out_shape=[jax.ShapeDtypeStruct((ALL_TILES, 8, WIDTH), bf16)]
            + [jax.ShapeDtypeStruct((SHARD_ROWS, 128), f32)] * 3,
            in_specs=[any_spec] * 5 + [pl.BlockSpec(memory_space=pltpu.SMEM)],
            out_specs=[any_spec] * 4,
            scratch_shapes=[
                pltpu.VMEM((3, 4, RS_TILES, 8, WIDTH), bf16),
                pltpu.VMEM((3, 3, 4, RS_TILES, 8, WIDTH), bf16),
                pltpu.VMEM((3, 4, RS_TILES, 8, WIDTH), f32),
                pltpu.VMEM((3, 2, RS_TILES, 8, WIDTH), f32),
                pltpu.VMEM((3, RS_TILES, 8, WIDTH), f32),
                pltpu.VMEM((SHARD_ROWS, 128), f32),
                pltpu.VMEM((SHARD_ROWS, 128), f32),
                pltpu.VMEM((SHARD_ROWS, 128), f32),
                pltpu.VMEM((3, TILE_ROWS, 128), f32),
                pltpu.VMEM((G_ROWS, 128), f32),
                pltpu.VMEM((3, AG_TILES + 1, 8, WIDTH), bf16),
                pltpu.VMEM((8, 128), f32),
                pltpu.VMEM((DEVS, 8, 128), f32),
                dma((3, 4)), dma((3, 3, 4)), dma((3, 3, 4)), dma((3, 2)), dma((3, 2)), dma((3,)), dma((3,)),
                dma((3,)), dma((3,)), dma((3,)), dma((DEVS,)), dma((DEVS,)),
                dma((3, 8)), dma((3, 8)), dma((3, 8)), dma((3, 8)), dma((3,)),
            ],
            compiler_params=pltpu.CompilerParams(
                collective_id=0, has_side_effects=True, vmem_limit_bytes=66_500_000),
        )(emb, tail, *state, arrays[GRAD_COUNT + 3])
        outs = [vout[:EMBED_TILES].reshape(shapes[0])]
        flat = vout[EMBED_TILES:].reshape(-1)
        start = 0
        for dims, size in zip(shapes[1:], sizes[1:]):
            outs.append(flat[start:start + size].reshape(dims))
            start += size
        return tuple(outs) + tuple(arr.reshape(-1) for arr in (first, second, master))

    in_specs = tuple([P("dp")] * GRAD_COUNT + [P("dp"), P("dp"), P("dp"), P()])
    out_specs = tuple([P()] * GRAD_COUNT + [P("dp"), P("dp"), P("dp")])
    return jax.shard_map(local_update, mesh=mesh, in_specs=in_specs, out_specs=out_specs, check_vma=False)
```

```python
import functools
import math
import jax
import jax.numpy as jnp
from jax import lax
from jax.experimental import pallas as pl
from jax.experimental.pallas import tpu as pltpu
from jax.sharding import PartitionSpec as P

ADAM_STEP = 7
ADAM_EPS = 1e-8
CLIP_EPS = 1e-6
GRAD_COUNT = 10
MESH = pl.DeviceIdType.MESH

DEVS = 16
OTHERS = range(1, DEVS)
THIRDS = range(3)
PAIR = range(2)
LANES = 128
WIDTH = 640
SHARD_ROWS = 6149
TILE_ROWS = 40
EMBED_TILES = 2048
ALL_TILES = 2460
DECAY_ROWS = 98240
FIRST_TAIL = 13
TAIL_START = (SHARD_ROWS * FIRST_TAIL) // TILE_ROWS
RS_TILES = 52
TAIL_TILES = (SHARD_ROWS * 15) // TILE_ROWS + 3 * RS_TILES - TAIL_START
AG_TILES = 51
LEAD = 40
G_ROWS = LEAD + 3 * RS_TILES * TILE_ROWS
ORDERS = ((2, 4, 8), (4, 8, 2), (8, 2, 4))


def flip(dev, stride):
    return dev + stride - 2 * stride * lax.rem(dev // stride, 2)


def rs_start(dev):
    return (SHARD_ROWS * dev) // TILE_ROWS


def ag_start(dev):
    return (SHARD_ROWS * dev + TILE_ROWS - 1) // TILE_ROWS


def flip_mask(dev, order, mask):
    for bit, stride in enumerate(order):
        if mask >> bit & 1:
            dev = flip(dev, stride)
    return dev


SMALL = {}
for _name, _tiles in (("q", 48), ("k", 12), ("v", 12), ("out", 48), ("gate", 96), ("up", 96),
                      ("down", 96), ("norms", 3), ("qk", 1)):
    SMALL[_name] = (EMBED_TILES if not SMALL else sum(SMALL[_last]), _tiles)
    _last = _name
LAYERS = 6
COLS = WIDTH // LANES
OUT_TILES = 48 * RS_TILES
SPARE = 42 * RS_TILES
PIECE_ROWS = RS_TILES * TILE_ROWS


def slot_tiles(slot, k, f):
    index = 36 + f * 3 + k if slot == 3 else (slot * 3 + k) * 4 + f
    return pl.ds(index * RS_TILES, RS_TILES)


def sum_rows(k, f):
    return pl.ds((f * 3 + k) * PIECE_ROWS, PIECE_ROWS)


def put_tile(dst, tile, rows, first, stride):
    for j in range(COLS):
        dst[tile, :, LANES * j:LANES * (j + 1)] = rows[pl.ds(first + j, 8, stride=stride), :].astype(jnp.bfloat16)


def pack_wide(src, dst, first_tile, rows, tiles):
    def step(i, _):
        rows[pl.ds(pl.multiple_of(i * 80, 16), 80), :] = src[pl.ds(pl.multiple_of(i * 80, 16), 80), :].astype(jnp.float32)
        for half in PAIR:
            put_tile(dst, first_tile + 2 * i + half, rows, i * 80 + half * 40, COLS)
        return 0

    lax.fori_loop(0, tiles // 2, step, 0)


def pack_narrow(src, dst, first_tile, rows, width):
    folds = LANES // width
    lane = lax.broadcasted_iota(jnp.int32, (8, LANES), 1) // width
    for layer in range(LAYERS):
        block = src[pl.ds(layer * width // 8, width // 8)].astype(jnp.float32).reshape(width, WIDTH)
        rows[pl.ds(layer * WIDTH, WIDTH), :] = jnp.concatenate([block] * folds, axis=0).T
    tiles = LAYERS * width // 8

    def step(t, _):
        for j in range(COLS):
            first = folds * (40 * t + j)
            value = rows[pl.ds(first, 8, stride=folds * COLS), :]
            for fold in range(1, folds):
                value = jnp.where(lane == fold, rows[pl.ds(first + fold, 8, stride=folds * COLS), :], value)
            dst[first_tile + t, :, LANES * j:LANES * (j + 1)] = value.astype(jnp.bfloat16)
        return 0

    lax.fori_loop(0, tiles, step, 0)


def unpack_wide(src, first_tile, dst, rows, tiles):
    def step(i, _):
        for half in PAIR:
            for j in range(COLS):
                rows[pl.ds(i * 80 + half * 40 + j, 8, stride=COLS), :] = src[
                    first_tile + 2 * i + half, :, LANES * j:LANES * (j + 1)].astype(jnp.float32)
        dst[pl.ds(pl.multiple_of(i * 80, 16), 80), :] = rows[pl.ds(pl.multiple_of(i * 80, 16), 80), :].astype(jnp.bfloat16)
        return 0

    lax.fori_loop(0, tiles // 2, step, 0)


def unpack_narrow(src, first_tile, dst, rows, width):
    folds = LANES // width
    tiles = LAYERS * width // 8

    def step(t, _):
        for j in range(COLS):
            value = src[first_tile + t, :, LANES * j:LANES * (j + 1)].astype(jnp.float32)
            for fold in range(folds):
                turned = value if fold == 0 else pltpu.roll(value, LANES - fold * width, 1)
                rows[pl.ds(folds * (40 * t + j) + fold, 8, stride=folds * COLS), :] = turned
        return 0

    lax.fori_loop(0, tiles, step, 0)
    for layer in range(LAYERS):
        block = rows[pl.ds(layer * WIDTH, WIDTH), :].T[:width]
        dst[pl.ds(layer * width // 8, width // 8)] = block.reshape(width // 8, 8, WIDTH).astype(jnp.bfloat16)


def kernel(emb, gq, gk, gv, go, gg, gu, gd, gn, gqk, m_in, v_in, p_in, hyp, mom, vel, par, vout, tail,
           s1, r2, r3, ext, nsend, nrecv, wide_raw, q_raw, k_raw, v_raw, n_raw, qk_raw, n_tiles,
           raw_sem, relay_sem, tail_sem,
           own_sem, r1_send, r1_recv, r2_send, r2_recv, r3_send, r3_recv, st_sem,
           ext_send, ext_recv, n_send, n_recv, ag_send, ag_recv, d2d_send, d2d_recv):
    grad = s1.at[pl.ds(0, G_ROWS)]
    me = lax.axis_index("dp")
    partner = flip(me, 1)

    def remote(src, dst, ssem, rsem, dev):
        return pltpu.make_async_remote_copy(
            src_ref=src, dst_ref=dst, send_sem=ssem, recv_sem=rsem, device_id=(dev,), device_id_type=MESH)

    def from_shard(owner, k, make, embed=True, small=True):
        first = rs_start(owner) + k * RS_TILES

        if embed:
            @pl.when(owner < FIRST_TAIL)
            def _():
                make(emb.at[pl.ds(first, RS_TILES)]).start()

        if small:
            @pl.when(owner >= FIRST_TAIL)
            def _():
                make(tail.at[pl.ds(first - TAIL_START, RS_TILES)]).start()

    def rs_owner(dev, k, f):
        return flip_mask(dev, ORDERS[k], (0 if f >= 2 else 2) + (4 if f % 2 == 0 else 0))

    state = [pltpu.make_async_copy(src, dst, st_sem.at[i])
             for i, (src, dst) in enumerate(((m_in, mom), (v_in, vel), (p_in, par)))]

    def load_own(f, embed=True, small=True):
        for k in THIRDS:
            from_shard(rs_owner(me, k, f), k, lambda src, k=k: pltpu.make_async_copy(
                src, vout.at[slot_tiles(3, k, f)], own_sem.at[k, f]), embed, small)

    def send_first(f, embed=True, small=True):
        for k in THIRDS:
            for slot in THIRDS:
                dev = partner if slot == 2 else flip(me, ORDERS[k][0])
                if slot == 1:
                    dev = flip(dev, 1)
                from_shard(rs_owner(dev, k, f), k, lambda src, k=k, slot=slot, dev=dev: remote(
                    src, vout.at[slot_tiles(slot, k, f)], r1_send.at[slot, k, f], r1_recv.at[slot, k, f], dev),
                    embed, small)

    raw = [pltpu.make_async_copy(src, dst, raw_sem.at[i]) for i, (src, dst) in enumerate((
        (gg, wide_raw.at[0]), (gu, wide_raw.at[1]), (gq, q_raw), (gk, k_raw), (gv, v_raw), (gn, n_raw), (gqk, qk_raw)))]
    for copy in raw:
        copy.start()
    edge = EMBED_TILES - TAIL_START
    relayed = []
    start = SPARE
    for i, (src, first, tiles) in enumerate(((go, SMALL["out"][0], 48), (gd, SMALL["down"][0], 96),
                                             (emb.at[pl.ds(TAIL_START, edge)], TAIL_START, edge))):
        part = vout.at[pl.ds(start, tiles)]
        copy = pltpu.make_async_copy(src, part, relay_sem.at[i])
        copy.start()
        relayed.append((copy, pltpu.make_async_copy(part, tail.at[pl.ds(first - TAIL_START, tiles)], tail_sem.at[i])))
        start += tiles
    for f in PAIR:
        load_own(f, small=False)
    barrier = pltpu.get_barrier_semaphore()
    for j in OTHERS:
        pl.semaphore_signal(barrier, inc=1, device_id=(lax.rem(me + j, DEVS),), device_id_type=MESH)
    pl.semaphore_wait(barrier, DEVS - 1)
    for f in PAIR:
        send_first(f, small=False)

    for copy, onward in relayed:
        copy.wait()
        onward.start()
    onwards = [onward for _, onward in relayed]

    raw_names = list(SMALL)

    def to_tail(src, name):
        first, tiles = SMALL[name]
        copy = pltpu.make_async_copy(src, tail.at[pl.ds(first - TAIL_START, tiles)], tail_sem.at[3 + raw_names.index(name)])
        copy.start()
        onwards.append(copy)

    spare = start
    for i, name in enumerate(("gate", "up")):
        raw[i].wait()
        pack_wide(wide_raw.at[i], vout, spare, grad, 96)
        to_tail(vout.at[pl.ds(spare, 96)], name)
        onwards.pop().wait()
    for i, (name, src, width) in enumerate((("q", q_raw, 64), ("k", k_raw, 16), ("v", v_raw, 16))):
        raw[2 + i].wait()
        pack_narrow(src, vout, spare, grad, width)
        tiles = SMALL[name][1]
        to_tail(vout.at[pl.ds(spare, tiles)], name)
        spare += tiles
    raw[5].wait()
    raw[6].wait()
    for i in THIRDS:
        n_tiles[i] = jnp.concatenate([n_raw[2 * i].astype(jnp.float32), n_raw[2 * i + 1].astype(jnp.float32)],
                                     axis=0).astype(jnp.bfloat16)
    grad[24:40, :] = jnp.zeros((16, LANES), jnp.float32)
    for layer in range(LAYERS):
        pair = qk_raw[layer].astype(jnp.float32)
        for i in PAIR:
            for half in PAIR:
                row = (2 * layer + i) * 2 + half
                grad[row:row + 1, :] = pair[i:i + 1, LANES * half:LANES * (half + 1)]
    put_tile(n_tiles, 3, grad, 0, COLS)
    to_tail(n_tiles.at[pl.ds(0, 3)], "norms")
    to_tail(n_tiles.at[pl.ds(3, 1)], "qk")
    for copy in onwards:
        copy.wait()
    for f in PAIR:
        send_first(f, embed=False)
        load_own(f, embed=False)
    for f in range(2, 4):
        send_first(f)
        load_own(f)
    before = lax.rem(me + DEVS - 1, DEVS)
    ext_copies = [remote(src.at[pl.ds(0, TILE_ROWS)], ext.at[i], ext_send.at[i], ext_recv.at[i], before)
                  for i, src in enumerate((m_in, v_in, p_in))]
    for copy in ext_copies:
        copy.start()
    for copy in state:
        copy.start()

    def r1_copy(slot, k, f):
        return remote(emb.at[pl.ds(0, RS_TILES)], vout.at[slot_tiles(slot, k, f)], r1_send.at[slot, k, f],
                      r1_recv.at[slot, k, f], partner)

    def r2_copy(k, f):
        return remote(s1.at[sum_rows(k, f)], r2.at[k, f], r2_send.at[k, f], r2_recv.at[k, f], flip(me, ORDERS[k][1]))

    def r3_copy(k):
        return remote(s1.at[sum_rows(k, 2)], r3.at[k], r3_send.at[k], r3_recv.at[k], flip(me, ORDERS[k][2]))

    for f in range(4):
        for k in THIRDS:
            pltpu.make_async_copy(
                emb.at[pl.ds(0, RS_TILES)], vout.at[slot_tiles(3, k, f)], own_sem.at[k, f]).wait()
            for slot in (2, 0, 1):
                r1_copy(slot, k, f).wait_recv()

            def add_four(t, _, k=k, f=f):
                a, b, c, d = [vout[slot_tiles(slot, k, f).start + t].astype(jnp.float32) for slot in (3, 2, 0, 1)]
                total = (a + b) + (c + d)
                row = sum_rows(k, f).start + TILE_ROWS * t
                for j in range(COLS):
                    s1[pl.ds(pl.multiple_of(row + 8 * j, 8), 8), :] = total[:, LANES * j:LANES * (j + 1)]
                return 0

            lax.fori_loop(0, RS_TILES, add_four, 0, unroll=2)
            if f < 2:
                r2_copy(k, f).start()
    for f in PAIR:
        for k in THIRDS:
            r2_copy(k, f).wait_recv()

            def add_two(t, _, k=k, f=f):
                row = pl.multiple_of(TILE_ROWS * t, 8)
                at = pl.ds(pl.multiple_of(sum_rows(k, 2 + f).start + TILE_ROWS * t, 8), TILE_ROWS)
                s1[at, :] = s1[at, :] + r2[k, f, pl.ds(row, TILE_ROWS), :]
                return 0

            lax.fori_loop(0, RS_TILES, add_two, 0, unroll=2)
            if f == 0:
                r3_copy(k).start()

    shift = LEAD - (SHARD_ROWS * me - TILE_ROWS * rs_start(me))
    for k in THIRDS:
        for f in PAIR:
            r2_copy(k, f).wait_send()
    for k in THIRDS:
        r3_copy(k).wait_recv()

        def finish(t, _, k=k):
            row = pl.multiple_of(TILE_ROWS * t, 8)
            at = pl.ds(pl.multiple_of(sum_rows(k, 3).start + TILE_ROWS * t, 8), TILE_ROWS)
            total = (s1[at, :] + r3[k, pl.ds(row, TILE_ROWS), :]) * (1.0 / DEVS)
            row = shift + TILE_ROWS * (k * RS_TILES + t)
            for j in range(COLS):
                grad[pl.ds(row + j, 8, stride=COLS), :] = total[8 * j:8 * (j + 1), :]
            return 0

        lax.fori_loop(0, RS_TILES, finish, 0, unroll=2)

    def squares(i, acc):
        part = grad[pl.ds(pl.multiple_of(LEAD + i * 40, 8), 40), :]
        return acc + part * part

    acc = lax.fori_loop(0, 153, squares, jnp.zeros((40, LANES), jnp.float32), unroll=3)
    nsend[...] = acc[0:8] + acc[8:16] + acc[16:24] + acc[24:32] + acc[32:40]
    for row in (6120, 6128, 6136):
        part = grad[pl.ds(LEAD + row, 8), :]
        nsend[...] = nsend[...] + part * part
    part = grad[pl.ds(LEAD + 6144, 5), :]
    nsend[0:5, :] = nsend[0:5, :] + part * part

    def n_copy(j):
        return remote(nsend, nrecv.at[me], n_send.at[j], n_recv.at[me], lax.rem(me + j, DEVS))

    for j in OTHERS:
        n_copy(j).start()

    def full(value):
        return jnp.full((8, LANES), value, jnp.float32)

    learn_rate, beta_one, beta_two, decay, max_norm = [full(hyp[i]) for i in range(5)]
    rest_one, rest_two = 1.0 - beta_one, 1.0 - beta_two
    hat_one = 1.0 / (1.0 - lax.integer_pow(beta_one, ADAM_STEP))
    hat_two = 1.0 / (1.0 - lax.integer_pow(beta_two, ADAM_STEP))
    for copy in state:
        copy.wait()
    for copy in ext_copies:
        copy.wait_recv()

    for j in OTHERS:
        n_copy(j).wait_send()
        source = lax.rem(me + DEVS - j, DEVS)
        remote(nsend, nrecv.at[source], n_send.at[j], n_recv.at[source], partner).wait_recv()
    nrecv[me] = nsend[...]
    total = nrecv[0]
    for j in OTHERS:
        total = total + nrecv[j]
    total = jnp.sum(jnp.sum(total, axis=1, keepdims=True), axis=0, keepdims=True)
    clip = jnp.minimum(1.0, max_norm / (jnp.sqrt(jnp.broadcast_to(total, (8, LANES))) + CLIP_EPS))

    def wide(value, rows):
        if rows <= 8:
            return value[:rows]
        return jnp.concatenate([value] * (rows // 8), axis=0)

    def adam(g, m, v, p, first_row, rows):
        clipped = g * wide(clip, rows)
        m = wide(beta_one, rows) * m + wide(rest_one, rows) * clipped
        v = wide(beta_two, rows) * v + wide(rest_two, rows) * (clipped * clipped)
        index = first_row + lax.broadcasted_iota(jnp.int32, (rows, LANES), 0)
        update = (m * wide(hat_one, rows)) / (jnp.sqrt(v * wide(hat_two, rows)) + ADAM_EPS)
        update = update + jnp.where(index < DECAY_ROWS, wide(decay, rows) * p, 0.0)
        return m, v, p - wide(learn_rate, rows) * update

    def adam_rows(row, rows):
        at = pl.ds(row, rows)
        shifted = pl.ds(row + LEAD, rows)
        m, v, p = adam(grad[shifted, :], mom[at, :], vel[at, :], par[at, :], SHARD_ROWS * me + row, rows)
        mom[at, :] = m
        vel[at, :] = v
        par[at, :] = p
        grad[shifted, :] = p

    def adam_block(i, _):
        adam_rows(pl.multiple_of(i * 40, 8), 40)
        return 0

    def ag_sizes(owner, k, run):
        if k < 2:
            run(AG_TILES)
            return
        longer = ag_start(owner + 1) - ag_start(owner) == 3 * AG_TILES + 1

        @pl.when(longer)
        def _():
            run(AG_TILES + 1)

        @pl.when(jnp.logical_not(longer))
        def _():
            run(AG_TILES)

    def ag_each(k, mask, run, dev=me):
        owner = flip_mask(dev, ORDERS[k], mask)
        first = ag_start(owner) + k * AG_TILES
        ag_sizes(owner, k, lambda size: run(vout.at[pl.ds(first, size)], size))

    def ag_link(k, mask, link):
        dev = flip(me, ORDERS[k][link])
        slot = mask + (1 << link)

        def copy(dst, size):
            return remote(dst, dst, ag_send.at[k, slot], ag_recv.at[k, slot], dev)

        ag_each(k, mask, lambda dst, size: copy(dst, size).start())
        pending.append(lambda: ag_each(k, mask, lambda dst, size: copy(dst, size).wait_send()))

    def ag_across(k, mask):
        def copy(dst, size):
            return remote(dst, dst, d2d_send.at[k, mask], d2d_recv.at[k, mask], partner)

        ag_each(k, mask, lambda dst, size: copy(dst, size).start())
        pending.append(lambda: ag_each(k, mask, lambda dst, size: copy(dst, size).wait_send()))

    def ag_arrived(k, mask):
        ag_each(k, mask, lambda dst, size: remote(
            dst, dst, ag_send.at[k, mask], ag_recv.at[k, mask], partner).wait_recv())

    pending = []
    bounds = ((0, 52), (52, 103), (103, 153))
    base = LEAD + TILE_ROWS * ag_start(me) - SHARD_ROWS * me
    for k in THIRDS:
        lax.fori_loop(bounds[k][0], bounds[k][1], adam_block, 0, unroll=1)
        if k == 2:
            adam_rows(6120, 24)
            adam_rows(6144, 5)
            at = pl.ds(LEAD + SHARD_ROWS, 40)
            _, _, p = adam(grad[at, :], ext[0], ext[1], ext[2], SHARD_ROWS * (me + 1), 40)
            grad[at, :] = p

        first = ag_start(me) + k * AG_TILES

        def pack(t, _, k=k, first=first):
            put_tile(vout, first + t, grad, base + TILE_ROWS * (k * AG_TILES + t), COLS)
            return 0

        count = ag_start(me + 1) - first if k == 2 else AG_TILES
        lax.fori_loop(0, count, pack, 0)
        ag_link(k, 0, 0)
    for k in THIRDS:
        ag_link(k, 0, 1)
    for k in THIRDS:
        ag_link(k, 0, 2)
    for k in THIRDS:
        ag_across(k, 0)
    for k in THIRDS:
        ag_arrived(k, 1)
        ag_link(k, 1, 1)
        ag_across(k, 1)
    for k in THIRDS:
        ag_link(k, 1, 2)
    for k in THIRDS:
        ag_arrived(k, 2)
        ag_link(k, 2, 2)
        ag_across(k, 2)
    for k in THIRDS:
        ag_arrived(k, 4)
        ag_across(k, 4)
    for k in THIRDS:
        ag_arrived(k, 3)
        ag_link(k, 3, 2)
        ag_across(k, 3)
    for mask in (5, 6, 7):
        for k in THIRDS:
            ag_arrived(k, mask)
            ag_across(k, mask)
    for mask in range(8):
        for k in THIRDS:
            ag_each(k, mask, lambda dst, size, k=k, mask=mask: remote(
                dst, dst, d2d_send.at[k, mask], d2d_recv.at[k, mask], partner).wait_recv(), partner)
    for wait in pending:
        wait()
    for copy in ext_copies:
        copy.wait_send()
    for f in range(4):
        for k in THIRDS:
            for slot in THIRDS:
                r1_copy(slot, k, f).wait_send()
    for k in THIRDS:
        r3_copy(k).wait_send()


def flush(mom, vel, par, vout, embed, oq, ok, ov, oo, og, ou, od, on, oqk, m_out, v_out, p_out,
          rows, wide_out, q_out, k_out, v_new, n_out, qk_out, sem):
    copies = []

    def send(src, dst):
        copy = pltpu.make_async_copy(src, dst, sem.at[len(copies)])
        copy.start()
        copies.append(copy)

    for i in range(4):
        part = pl.ds(i * EMBED_TILES // 4, EMBED_TILES // 4)
        send(vout.at[part], embed.at[part])
    for src, dst in ((mom, m_out), (vel, v_out), (par, p_out)):
        send(src, dst)
    for name, dst in (("out", oo), ("down", od)):
        send(vout.at[pl.ds(*SMALL[name])], dst)
    for i, (name, dst) in enumerate((("gate", og), ("up", ou))):
        unpack_wide(vout, SMALL[name][0], wide_out.at[i], rows, 96)
        send(wide_out.at[i], dst)
    for name, block, dst, width in (("q", q_out, oq, 64), ("k", k_out, ok, 16), ("v", v_new, ov, 16)):
        unpack_narrow(vout, SMALL[name][0], block, rows, width)
        send(block, dst)
    for i in THIRDS:
        tile = vout[SMALL["norms"][0] + i].astype(jnp.float32)
        n_out[2 * i] = tile[0:4].astype(jnp.bfloat16)
        n_out[2 * i + 1] = tile[4:8].astype(jnp.bfloat16)
    send(n_out, on)
    for j in range(COLS):
        rows[pl.ds(j, 8, stride=COLS), :] = vout[SMALL["qk"][0], :, LANES * j:LANES * (j + 1)].astype(jnp.float32)
    for layer in range(LAYERS):
        four = rows[4 * layer:4 * layer + 4, :]
        pair = [jnp.concatenate([four[2 * i:2 * i + 1], four[2 * i + 1:2 * i + 2]], axis=1) for i in PAIR]
        qk_out[layer] = jnp.concatenate(pair, axis=0).astype(jnp.bfloat16)
    send(qk_out, oqk)
    for copy in copies:
        copy.wait()


def solution(mesh):
    def local_update(*arrays):
        grads = [arr.reshape(arr.shape[1:]) for arr in arrays[:GRAD_COUNT]]
        state = [arr.reshape(SHARD_ROWS, LANES) for arr in arrays[GRAD_COUNT:GRAD_COUNT + 3]]
        shapes = [grad_arr.shape for grad_arr in grads]
        any_spec = pl.BlockSpec(memory_space=pl.ANY)
        vmem_spec = pl.BlockSpec(memory_space=pltpu.VMEM)
        dma = pltpu.SemaphoreType.DMA
        bf16, f32 = jnp.bfloat16, jnp.float32
        tiled = []
        for i, grad_arr in enumerate(grads[:8]):
            if i in (1, 2, 3):
                grad_arr = jnp.swapaxes(grad_arr, 1, 2)
            tiled.append(grad_arr.reshape(-1, LANES) if i in (5, 6) else grad_arr.reshape(-1, 8, WIDTH))
        tiled += grads[8:]
        small = [jax.ShapeDtypeStruct(arr.shape, bf16) for arr in tiled[1:]]
        *kept, _ = pl.pallas_call(
            kernel,
            out_shape=[pltpu.VMEM((SHARD_ROWS, LANES), f32)] * 3
            + [pltpu.VMEM((OUT_TILES, 8, WIDTH), bf16)]
            + [pltpu.HBM((TAIL_TILES, 8, WIDTH), bf16)],
            in_specs=[any_spec] * 13 + [pl.BlockSpec(memory_space=pltpu.SMEM)],
            out_specs=[vmem_spec] * 4 + [any_spec],
            scratch_shapes=[
                pltpu.VMEM((3 * 4 * PIECE_ROWS, LANES), f32),
                pltpu.VMEM((3, 2, PIECE_ROWS, LANES), f32),
                pltpu.VMEM((3, PIECE_ROWS, LANES), f32),
                pltpu.VMEM((3, TILE_ROWS, LANES), f32),
                pltpu.VMEM((8, LANES), f32),
                pltpu.VMEM((DEVS, 8, LANES), f32),
                pltpu.VMEM((2, 3840, LANES), bf16),
                pltpu.VMEM((48, 8, WIDTH), bf16),
                pltpu.VMEM((12, 8, WIDTH), bf16),
                pltpu.VMEM((12, 8, WIDTH), bf16),
                pltpu.VMEM(shapes[8], bf16),
                pltpu.VMEM(shapes[9], bf16),
                pltpu.VMEM((4, 8, WIDTH), bf16),
                dma((7,)), dma((3,)), dma((3 + len(SMALL),)),
                dma((3, 4)), dma((3, 3, 4)), dma((3, 3, 4)), dma((3, 2)), dma((3, 2)), dma((3,)), dma((3,)),
                dma((3,)), dma((3,)), dma((3,)), dma((DEVS,)), dma((DEVS,)),
                dma((3, 8)), dma((3, 8)), dma((3, 8)), dma((3, 8)),
            ],
            compiler_params=pltpu.CompilerParams(
                collective_id=0, has_side_effects=True, vmem_limit_bytes=26_500_000),
        )(*tiled, *state, arrays[GRAD_COUNT + 3])
        kept = [pltpu.with_memory_space_constraint(arr, pltpu.VMEM) for arr in kept]
        outs = pl.pallas_call(
            flush,
            out_shape=[jax.ShapeDtypeStruct((EMBED_TILES, 8, WIDTH), bf16)] + small
            + [jax.ShapeDtypeStruct((SHARD_ROWS, LANES), f32)] * 3,
            in_specs=[vmem_spec] * 4,
            out_specs=[any_spec] * 13,
            scratch_shapes=[
                pltpu.VMEM((3840, LANES), f32),
                pltpu.VMEM((2, 3840, LANES), bf16),
                pltpu.VMEM((48, 8, WIDTH), bf16),
                pltpu.VMEM((12, 8, WIDTH), bf16),
                pltpu.VMEM((12, 8, WIDTH), bf16),
                pltpu.VMEM(shapes[8], bf16),
                pltpu.VMEM(shapes[9], bf16),
                dma((20,)),
            ],
            compiler_params=pltpu.CompilerParams(has_side_effects=True, vmem_limit_bytes=5_200_000),
        )(*kept)
        params = []
        for i, dims in enumerate(shapes):
            if i in (1, 2, 3):
                params.append(jnp.swapaxes(outs[i].reshape(dims[0], dims[2], dims[1]), 1, 2))
            else:
                params.append(outs[i].reshape(dims))
        return tuple(params) + tuple(arr.reshape(-1) for arr in outs[GRAD_COUNT:])

    in_specs = tuple([P("dp")] * GRAD_COUNT + [P("dp"), P("dp"), P("dp"), P()])
    out_specs = tuple([P()] * GRAD_COUNT + [P("dp"), P("dp"), P("dp")])
    return jax.shard_map(local_update, mesh=mesh, in_specs=in_specs, out_specs=out_specs, check_vma=False)
```

```python
import functools
import math
import jax
import jax.numpy as jnp
from jax import lax
from jax.experimental import pallas as pl
from jax.experimental.pallas import tpu as pltpu
from jax.sharding import PartitionSpec as P

ADAM_STEP = 7
ADAM_EPS = 1e-8
CLIP_EPS = 1e-6
GRAD_COUNT = 10
MESH = pl.DeviceIdType.MESH

DEVS = 16
OTHERS = range(1, DEVS)
THIRDS = range(3)
PAIR = range(2)
LANES = 128
WIDTH = 640
SHARD_ROWS = 6149
TILE_ROWS = 40
EMBED_TILES = 2048
ALL_TILES = 2460
DECAY_ROWS = 98240
FIRST_TAIL = 13
TAIL_START = (SHARD_ROWS * FIRST_TAIL) // TILE_ROWS
RS_TILES = 52
TAIL_TILES = (SHARD_ROWS * 15) // TILE_ROWS + 3 * RS_TILES - TAIL_START
AG_TILES = 51
LEAD = 40
G_ROWS = LEAD + 3 * RS_TILES * TILE_ROWS
ORDERS = ((2, 4, 8), (4, 8, 2), (8, 2, 4))


def flip(dev, stride):
    return dev + stride - 2 * stride * lax.rem(dev // stride, 2)


def rs_start(dev):
    return (SHARD_ROWS * dev) // TILE_ROWS


def ag_start(dev):
    return (SHARD_ROWS * dev + TILE_ROWS - 1) // TILE_ROWS


def flip_mask(dev, order, mask):
    for bit, stride in enumerate(order):
        if mask >> bit & 1:
            dev = flip(dev, stride)
    return dev


SMALL = {}
for _name, _tiles in (("q", 48), ("k", 12), ("v", 12), ("out", 48), ("gate", 96), ("up", 96),
                      ("down", 96), ("norms", 3), ("qk", 1)):
    SMALL[_name] = (EMBED_TILES if not SMALL else sum(SMALL[_last]), _tiles)
    _last = _name
LAYERS = 6
COLS = WIDTH // LANES
OUT_TILES = 48 * RS_TILES
SPARE = 42 * RS_TILES
PIECE_ROWS = RS_TILES * TILE_ROWS


def slot_tiles(slot, k, f):
    index = 36 + f * 3 + k if slot == 3 else (slot * 3 + k) * 4 + f
    return pl.ds(index * RS_TILES, RS_TILES)


def sum_rows(k, f):
    return pl.ds((f * 3 + k) * PIECE_ROWS, PIECE_ROWS)


def put_tile(dst, tile, rows, first, stride):
    for j in range(COLS):
        dst[tile, :, LANES * j:LANES * (j + 1)] = rows[pl.ds(first + j, 8, stride=stride), :].astype(jnp.bfloat16)


def pack_wide(src, dst, first_tile, rows, tiles):
    def step(i, _):
        rows[pl.ds(pl.multiple_of(i * 80, 16), 80), :] = src[pl.ds(pl.multiple_of(i * 80, 16), 80), :].astype(jnp.float32)
        for half in PAIR:
            put_tile(dst, first_tile + 2 * i + half, rows, i * 80 + half * 40, COLS)
        return 0

    lax.fori_loop(0, tiles // 2, step, 0)


def pack_narrow(src, dst, first_tile, rows, width):
    folds = LANES // width
    lane = lax.broadcasted_iota(jnp.int32, (8, LANES), 1) // width
    for layer in range(LAYERS):
        block = src[pl.ds(layer * width // 8, width // 8)].astype(jnp.float32).reshape(width, WIDTH)
        rows[pl.ds(layer * WIDTH, WIDTH), :] = jnp.concatenate([block] * folds, axis=0).T
    tiles = LAYERS * width // 8

    def step(t, _):
        for j in range(COLS):
            first = folds * (40 * t + j)
            value = rows[pl.ds(first, 8, stride=folds * COLS), :]
            for fold in range(1, folds):
                value = jnp.where(lane == fold, rows[pl.ds(first + fold, 8, stride=folds * COLS), :], value)
            dst[first_tile + t, :, LANES * j:LANES * (j + 1)] = value.astype(jnp.bfloat16)
        return 0

    lax.fori_loop(0, tiles, step, 0)


def unpack_wide(src, first_tile, dst, rows, tiles):
    def step(i, _):
        for half in PAIR:
            for j in range(COLS):
                rows[pl.ds(i * 80 + half * 40 + j, 8, stride=COLS), :] = src[
                    first_tile + 2 * i + half, :, LANES * j:LANES * (j + 1)].astype(jnp.float32)
        dst[pl.ds(pl.multiple_of(i * 80, 16), 80), :] = rows[pl.ds(pl.multiple_of(i * 80, 16), 80), :].astype(jnp.bfloat16)
        return 0

    lax.fori_loop(0, tiles // 2, step, 0)


def unpack_narrow(src, first_tile, dst, rows, width):
    folds = LANES // width
    tiles = LAYERS * width // 8

    def step(t, _):
        for j in range(COLS):
            value = src[first_tile + t, :, LANES * j:LANES * (j + 1)].astype(jnp.float32)
            for fold in range(folds):
                turned = value if fold == 0 else pltpu.roll(value, LANES - fold * width, 1)
                rows[pl.ds(folds * (40 * t + j) + fold, 8, stride=folds * COLS), :] = turned
        return 0

    lax.fori_loop(0, tiles, step, 0)
    for layer in range(LAYERS):
        block = rows[pl.ds(layer * WIDTH, WIDTH), :].T[:width]
        dst[pl.ds(layer * width // 8, width // 8)] = block.reshape(width // 8, 8, WIDTH).astype(jnp.bfloat16)


def kernel(emb, gq, gk, gv, go, gg, gu, gd, gn, gqk, m_in, v_in, p_in, hyp, mom, vel, par, vout, tail,
           s1, r2, r3, ext, nsend, nrecv, wide_raw, q_raw, k_raw, v_raw, n_raw, qk_raw, n_tiles,
           raw_sem, relay_sem, tail_sem,
           own_sem, r1_send, r1_recv, r2_send, r2_recv, r3_send, r3_recv, st_sem,
           ext_send, ext_recv, n_send, n_recv, ag_send, ag_recv, d2d_send, d2d_recv):
    grad = s1.at[pl.ds(0, G_ROWS)]
    me = lax.axis_index("dp")
    partner = flip(me, 1)

    def remote(src, dst, ssem, rsem, dev):
        return pltpu.make_async_remote_copy(
            src_ref=src, dst_ref=dst, send_sem=ssem, recv_sem=rsem, device_id=(dev,), device_id_type=MESH)

    def from_shard(owner, k, make, embed=True, small=True):
        first = rs_start(owner) + k * RS_TILES

        if embed:
            @pl.when(owner < FIRST_TAIL)
            def _():
                make(emb.at[pl.ds(first, RS_TILES)]).start()

        if small:
            @pl.when(owner >= FIRST_TAIL)
            def _():
                make(tail.at[pl.ds(first - TAIL_START, RS_TILES)]).start()

    def rs_owner(dev, k, f):
        return flip_mask(dev, ORDERS[k], (0 if f >= 2 else 2) + (4 if f % 2 == 0 else 0))

    state = [pltpu.make_async_copy(src, dst, st_sem.at[i])
             for i, (src, dst) in enumerate(((m_in, mom), (v_in, vel), (p_in, par)))]

    def load_own(f, embed=True, small=True):
        for k in THIRDS:
            from_shard(rs_owner(me, k, f), k, lambda src, k=k: pltpu.make_async_copy(
                src, vout.at[slot_tiles(3, k, f)], own_sem.at[k, f]), embed, small)

    def send_first(f, embed=True, small=True):
        for k in THIRDS:
            for slot in THIRDS:
                dev = partner if slot == 2 else flip(me, ORDERS[k][0])
                if slot == 1:
                    dev = flip(dev, 1)
                from_shard(rs_owner(dev, k, f), k, lambda src, k=k, slot=slot, dev=dev: remote(
                    src, vout.at[slot_tiles(slot, k, f)], r1_send.at[slot, k, f], r1_recv.at[slot, k, f], dev),
                    embed, small)

    barrier = pltpu.get_barrier_semaphore()
    for j in OTHERS:
        pl.semaphore_signal(barrier, inc=1, device_id=(lax.rem(me + j, DEVS),), device_id_type=MESH)
    raw = [pltpu.make_async_copy(src, dst, raw_sem.at[i]) for i, (src, dst) in enumerate((
        (gg, wide_raw.at[0]), (gu, wide_raw.at[1]), (gq, q_raw), (gk, k_raw), (gv, v_raw), (gn, n_raw), (gqk, qk_raw)))]
    for copy in raw:
        copy.start()
    edge = EMBED_TILES - TAIL_START
    relayed = []
    start = SPARE
    for i, (src, first, tiles) in enumerate(((go, SMALL["out"][0], 48), (gd, SMALL["down"][0], 96),
                                             (emb.at[pl.ds(TAIL_START, edge)], TAIL_START, edge))):
        part = vout.at[pl.ds(start, tiles)]
        copy = pltpu.make_async_copy(src, part, relay_sem.at[i])
        copy.start()
        relayed.append((copy, pltpu.make_async_copy(part, tail.at[pl.ds(first - TAIL_START, tiles)], tail_sem.at[i])))
        start += tiles
    for f in PAIR:
        load_own(f, small=False)
    pl.semaphore_wait(barrier, DEVS - 1)
    for f in PAIR:
        send_first(f, small=False)

    for copy, onward in relayed:
        copy.wait()
        onward.start()
    onwards = [onward for _, onward in relayed]

    raw_names = list(SMALL)

    def to_tail(src, name):
        first, tiles = SMALL[name]
        copy = pltpu.make_async_copy(src, tail.at[pl.ds(first - TAIL_START, tiles)], tail_sem.at[3 + raw_names.index(name)])
        copy.start()
        onwards.append(copy)

    spare = start
    for i, name in enumerate(("gate", "up")):
        raw[i].wait()
        pack_wide(wide_raw.at[i], vout, spare, grad, 96)
        to_tail(vout.at[pl.ds(spare, 96)], name)
        onwards.pop().wait()
    for i, (name, src, width) in enumerate((("q", q_raw, 64), ("k", k_raw, 16), ("v", v_raw, 16))):
        raw[2 + i].wait()
        pack_narrow(src, vout, spare, grad, width)
        tiles = SMALL[name][1]
        to_tail(vout.at[pl.ds(spare, tiles)], name)
        spare += tiles
    raw[5].wait()
    raw[6].wait()
    for i in THIRDS:
        n_tiles[i] = jnp.concatenate([n_raw[2 * i].astype(jnp.float32), n_raw[2 * i + 1].astype(jnp.float32)],
                                     axis=0).astype(jnp.bfloat16)
    grad[24:40, :] = jnp.zeros((16, LANES), jnp.float32)
    for layer in range(LAYERS):
        pair = qk_raw[layer].astype(jnp.float32)
        for i in PAIR:
            for half in PAIR:
                row = (2 * layer + i) * 2 + half
                grad[row:row + 1, :] = pair[i:i + 1, LANES * half:LANES * (half + 1)]
    put_tile(n_tiles, 3, grad, 0, COLS)
    to_tail(n_tiles.at[pl.ds(0, 3)], "norms")
    to_tail(n_tiles.at[pl.ds(3, 1)], "qk")
    for copy in onwards:
        copy.wait()
    for f in PAIR:
        send_first(f, embed=False)
        load_own(f, embed=False)
    for f in range(2, 4):
        send_first(f)
        load_own(f)
    before = lax.rem(me + DEVS - 1, DEVS)
    ext_copies = [remote(src.at[pl.ds(0, TILE_ROWS)], ext.at[i], ext_send.at[i], ext_recv.at[i], before)
                  for i, src in enumerate((m_in, v_in, p_in))]
    for copy in ext_copies:
        copy.start()
    for copy in state:
        copy.start()

    def r1_copy(slot, k, f):
        return remote(emb.at[pl.ds(0, RS_TILES)], vout.at[slot_tiles(slot, k, f)], r1_send.at[slot, k, f],
                      r1_recv.at[slot, k, f], partner)

    def r2_copy(k, f):
        return remote(s1.at[sum_rows(k, f)], r2.at[k, f], r2_send.at[k, f], r2_recv.at[k, f], flip(me, ORDERS[k][1]))

    def r3_copy(k):
        return remote(s1.at[sum_rows(k, 2)], r3.at[k], r3_send.at[k], r3_recv.at[k], flip(me, ORDERS[k][2]))

    for f in range(4):
        for k in THIRDS:
            pltpu.make_async_copy(
                emb.at[pl.ds(0, RS_TILES)], vout.at[slot_tiles(3, k, f)], own_sem.at[k, f]).wait()
            for slot in (2, 0, 1):
                r1_copy(slot, k, f).wait_recv()

            def add_four(t, _, k=k, f=f):
                a, b, c, d = [vout[slot_tiles(slot, k, f).start + t].astype(jnp.float32) for slot in (3, 2, 0, 1)]
                total = (a + b) + (c + d)
                row = sum_rows(k, f).start + TILE_ROWS * t
                for j in range(COLS):
                    s1[pl.ds(pl.multiple_of(row + 8 * j, 8), 8), :] = total[:, LANES * j:LANES * (j + 1)]
                return 0

            lax.fori_loop(0, RS_TILES, add_four, 0, unroll=2)
            if f < 2:
                r2_copy(k, f).start()
    for f in PAIR:
        for k in THIRDS:
            r2_copy(k, f).wait_recv()

            def add_two(t, _, k=k, f=f):
                row = pl.multiple_of(TILE_ROWS * t, 8)
                at = pl.ds(pl.multiple_of(sum_rows(k, 2 + f).start + TILE_ROWS * t, 8), TILE_ROWS)
                s1[at, :] = s1[at, :] + r2[k, f, pl.ds(row, TILE_ROWS), :]
                return 0

            lax.fori_loop(0, RS_TILES, add_two, 0, unroll=2)
            if f == 0:
                r3_copy(k).start()

    shift = LEAD - (SHARD_ROWS * me - TILE_ROWS * rs_start(me))
    for k in THIRDS:
        for f in PAIR:
            r2_copy(k, f).wait_send()
    for k in THIRDS:
        r3_copy(k).wait_recv()

        def finish(t, _, k=k):
            row = pl.multiple_of(TILE_ROWS * t, 8)
            at = pl.ds(pl.multiple_of(sum_rows(k, 3).start + TILE_ROWS * t, 8), TILE_ROWS)
            total = (s1[at, :] + r3[k, pl.ds(row, TILE_ROWS), :]) * (1.0 / DEVS)
            row = shift + TILE_ROWS * (k * RS_TILES + t)
            for j in range(COLS):
                grad[pl.ds(row + j, 8, stride=COLS), :] = total[8 * j:8 * (j + 1), :]
            return 0

        lax.fori_loop(0, RS_TILES, finish, 0, unroll=2)

    def squares(i, acc):
        part = grad[pl.ds(pl.multiple_of(LEAD + i * 40, 8), 40), :]
        return acc + part * part

    acc = lax.fori_loop(0, 153, squares, jnp.zeros((40, LANES), jnp.float32), unroll=3)
    nsend[...] = acc[0:8] + acc[8:16] + acc[16:24] + acc[24:32] + acc[32:40]
    for row in (6120, 6128, 6136):
        part = grad[pl.ds(LEAD + row, 8), :]
        nsend[...] = nsend[...] + part * part
    part = grad[pl.ds(LEAD + 6144, 5), :]
    nsend[0:5, :] = nsend[0:5, :] + part * part

    def n_copy(j):
        return remote(nsend, nrecv.at[me], n_send.at[j], n_recv.at[me], lax.rem(me + j, DEVS))

    for j in OTHERS:
        n_copy(j).start()

    def full(value):
        return jnp.full((8, LANES), value, jnp.float32)

    learn_rate, beta_one, beta_two, decay, max_norm = [full(hyp[i]) for i in range(5)]
    rest_one, rest_two = 1.0 - beta_one, 1.0 - beta_two
    hat_one = 1.0 / (1.0 - lax.integer_pow(beta_one, ADAM_STEP))
    hat_two = 1.0 / (1.0 - lax.integer_pow(beta_two, ADAM_STEP))
    for copy in state:
        copy.wait()
    for copy in ext_copies:
        copy.wait_recv()

    for j in OTHERS:
        n_copy(j).wait_send()
        source = lax.rem(me + DEVS - j, DEVS)
        remote(nsend, nrecv.at[source], n_send.at[j], n_recv.at[source], partner).wait_recv()
    nrecv[me] = nsend[...]
    total = nrecv[0]
    for j in OTHERS:
        total = total + nrecv[j]
    total = jnp.sum(jnp.sum(total, axis=1, keepdims=True), axis=0, keepdims=True)
    clip = jnp.minimum(1.0, max_norm / (jnp.sqrt(jnp.broadcast_to(total, (8, LANES))) + CLIP_EPS))

    def wide(value, rows):
        if rows <= 8:
            return value[:rows]
        return jnp.concatenate([value] * (rows // 8), axis=0)

    def adam(g, m, v, p, first_row, rows):
        clipped = g * wide(clip, rows)
        m = wide(beta_one, rows) * m + wide(rest_one, rows) * clipped
        v = wide(beta_two, rows) * v + wide(rest_two, rows) * (clipped * clipped)
        index = first_row + lax.broadcasted_iota(jnp.int32, (rows, LANES), 0)
        update = (m * wide(hat_one, rows)) / (jnp.sqrt(v * wide(hat_two, rows)) + ADAM_EPS)
        update = update + jnp.where(index < DECAY_ROWS, wide(decay, rows) * p, 0.0)
        return m, v, p - wide(learn_rate, rows) * update

    def adam_rows(row, rows):
        at = pl.ds(row, rows)
        shifted = pl.ds(row + LEAD, rows)
        m, v, p = adam(grad[shifted, :], mom[at, :], vel[at, :], par[at, :], SHARD_ROWS * me + row, rows)
        mom[at, :] = m
        vel[at, :] = v
        par[at, :] = p
        grad[shifted, :] = p

    def adam_block(i, _):
        adam_rows(pl.multiple_of(i * 40, 8), 40)
        return 0

    def ag_sizes(owner, k, run):
        if k < 2:
            run(AG_TILES)
            return
        longer = ag_start(owner + 1) - ag_start(owner) == 3 * AG_TILES + 1

        @pl.when(longer)
        def _():
            run(AG_TILES + 1)

        @pl.when(jnp.logical_not(longer))
        def _():
            run(AG_TILES)

    def ag_each(k, mask, run, dev=me):
        owner = flip_mask(dev, ORDERS[k], mask)
        first = ag_start(owner) + k * AG_TILES
        ag_sizes(owner, k, lambda size: run(vout.at[pl.ds(first, size)], size))

    def ag_link(k, mask, link, start=True):
        dev = flip(me, ORDERS[k][link])
        slot = mask + (1 << link)

        def copy(dst, size):
            return remote(dst, dst, ag_send.at[k, slot], ag_recv.at[k, slot], dev)

        if start:
            ag_each(k, mask, lambda dst, size: copy(dst, size).start())
        pending.append(lambda: ag_each(k, mask, lambda dst, size: copy(dst, size).wait_send()))

    def ag_across(k, mask, start=True):
        def copy(dst, size):
            return remote(dst, dst, d2d_send.at[k, mask], d2d_recv.at[k, mask], partner)

        if start:
            ag_each(k, mask, lambda dst, size: copy(dst, size).start())
        pending.append(lambda: ag_each(k, mask, lambda dst, size: copy(dst, size).wait_send()))

    def ag_arrived(k, mask):
        ag_each(k, mask, lambda dst, size: remote(
            dst, dst, ag_send.at[k, mask], ag_recv.at[k, mask], partner).wait_recv())

    pending = []
    base = LEAD + TILE_ROWS * ag_start(me) - SHARD_ROWS * me

    def own_part(k, skip, count, blocks):
        lax.fori_loop(*blocks, adam_block, 0)
        if k == 2:
            adam_rows(6120, 24)
            adam_rows(6144, 5)
            at = pl.ds(LEAD + SHARD_ROWS, TILE_ROWS)
            _, _, p = adam(grad[at, :], ext[0], ext[1], ext[2], SHARD_ROWS * (me + 1), TILE_ROWS)
            grad[at, :] = p
        first = ag_start(me) + k * AG_TILES

        def pack(t, _):
            put_tile(vout, first + t, grad, base + TILE_ROWS * (k * AG_TILES + t), COLS)
            return 0

        lax.fori_loop(skip, skip + (ag_start(me + 1) - first if k == 2 else count), pack, 0)

        def send(size):
            part = vout.at[pl.ds(first + skip, size)]
            for link in THIRDS:
                slot = 1 << link
                remote(part, part, ag_send.at[k, slot], ag_recv.at[k, slot], flip(me, ORDERS[k][link])).start()
            remote(part, part, d2d_send.at[k, 0], d2d_recv.at[k, 0], partner).start()

        if k == 2:
            ag_sizes(me, k, send)
        else:
            send(count)

    own_part(0, 0, 13, (0, 14))
    own_part(0, 13, 13, (14, 27))
    own_part(0, 26, 25, (27, 52))
    own_part(1, 0, AG_TILES, (52, 103))
    own_part(2, 0, None, (103, 153))
    for k in THIRDS:
        for link in THIRDS:
            ag_link(k, 0, link, start=False)
        ag_across(k, 0, start=False)
    for k in THIRDS:
        ag_arrived(k, 1)
        ag_link(k, 1, 1)
        ag_across(k, 1)
    for k in THIRDS:
        ag_link(k, 1, 2)
    for k in THIRDS:
        ag_arrived(k, 2)
        ag_link(k, 2, 2)
        ag_across(k, 2)
    for k in THIRDS:
        ag_arrived(k, 4)
        ag_across(k, 4)
    for k in THIRDS:
        ag_arrived(k, 3)
        ag_link(k, 3, 2)
        ag_across(k, 3)
    for mask in (5, 6, 7):
        for k in THIRDS:
            ag_arrived(k, mask)
            ag_across(k, mask)
    for mask in range(8):
        for k in THIRDS:
            ag_each(k, mask, lambda dst, size, k=k, mask=mask: remote(
                dst, dst, d2d_send.at[k, mask], d2d_recv.at[k, mask], partner).wait_recv(), partner)
    for wait in pending:
        wait()
    for copy in ext_copies:
        copy.wait_send()
    for f in range(4):
        for k in THIRDS:
            for slot in THIRDS:
                r1_copy(slot, k, f).wait_send()
    for k in THIRDS:
        r3_copy(k).wait_send()


def flush(mom, vel, par, vout, embed, oq, ok, ov, oo, og, ou, od, on, oqk, m_out, v_out, p_out,
          rows, wide_out, q_out, k_out, v_new, n_out, qk_out, sem):
    copies = []

    def send(src, dst):
        copy = pltpu.make_async_copy(src, dst, sem.at[len(copies)])
        copy.start()
        copies.append(copy)

    for i in range(4):
        part = pl.ds(i * EMBED_TILES // 4, EMBED_TILES // 4)
        send(vout.at[part], embed.at[part])
    for src, dst in ((mom, m_out), (vel, v_out), (par, p_out)):
        send(src, dst)
    for name, dst in (("out", oo), ("down", od)):
        send(vout.at[pl.ds(*SMALL[name])], dst)
    for i, (name, dst) in enumerate((("gate", og), ("up", ou))):
        unpack_wide(vout, SMALL[name][0], wide_out.at[i], rows, 96)
        send(wide_out.at[i], dst)
    for name, block, dst, width in (("q", q_out, oq, 64), ("k", k_out, ok, 16), ("v", v_new, ov, 16)):
        unpack_narrow(vout, SMALL[name][0], block, rows, width)
        send(block, dst)
    for i in THIRDS:
        tile = vout[SMALL["norms"][0] + i].astype(jnp.float32)
        n_out[2 * i] = tile[0:4].astype(jnp.bfloat16)
        n_out[2 * i + 1] = tile[4:8].astype(jnp.bfloat16)
    send(n_out, on)
    for j in range(COLS):
        rows[pl.ds(j, 8, stride=COLS), :] = vout[SMALL["qk"][0], :, LANES * j:LANES * (j + 1)].astype(jnp.float32)
    for layer in range(LAYERS):
        four = rows[4 * layer:4 * layer + 4, :]
        pair = [jnp.concatenate([four[2 * i:2 * i + 1], four[2 * i + 1:2 * i + 2]], axis=1) for i in PAIR]
        qk_out[layer] = jnp.concatenate(pair, axis=0).astype(jnp.bfloat16)
    send(qk_out, oqk)
    for copy in copies:
        copy.wait()


def solution(mesh):
    def local_update(*arrays):
        grads = [arr.reshape(arr.shape[1:]) for arr in arrays[:GRAD_COUNT]]
        state = [arr.reshape(SHARD_ROWS, LANES) for arr in arrays[GRAD_COUNT:GRAD_COUNT + 3]]
        shapes = [grad_arr.shape for grad_arr in grads]
        any_spec = pl.BlockSpec(memory_space=pl.ANY)
        vmem_spec = pl.BlockSpec(memory_space=pltpu.VMEM)
        dma = pltpu.SemaphoreType.DMA
        bf16, f32 = jnp.bfloat16, jnp.float32
        tiled = []
        for i, grad_arr in enumerate(grads[:8]):
            if i in (1, 2, 3):
                grad_arr = jnp.swapaxes(grad_arr, 1, 2)
            tiled.append(grad_arr.reshape(-1, LANES) if i in (5, 6) else grad_arr.reshape(-1, 8, WIDTH))
        tiled += grads[8:]
        small = [jax.ShapeDtypeStruct(arr.shape, bf16) for arr in tiled[1:]]
        *kept, _ = pl.pallas_call(
            kernel,
            out_shape=[pltpu.VMEM((SHARD_ROWS, LANES), f32)] * 3
            + [pltpu.VMEM((OUT_TILES, 8, WIDTH), bf16)]
            + [pltpu.HBM((TAIL_TILES, 8, WIDTH), bf16)],
            in_specs=[any_spec] * 13 + [pl.BlockSpec(memory_space=pltpu.SMEM)],
            out_specs=[vmem_spec] * 4 + [any_spec],
            scratch_shapes=[
                pltpu.VMEM((3 * 4 * PIECE_ROWS, LANES), f32),
                pltpu.VMEM((3, 2, PIECE_ROWS, LANES), f32),
                pltpu.VMEM((3, PIECE_ROWS, LANES), f32),
                pltpu.VMEM((3, TILE_ROWS, LANES), f32),
                pltpu.VMEM((8, LANES), f32),
                pltpu.VMEM((DEVS, 8, LANES), f32),
                pltpu.VMEM((2, 3840, LANES), bf16),
                pltpu.VMEM((48, 8, WIDTH), bf16),
                pltpu.VMEM((12, 8, WIDTH), bf16),
                pltpu.VMEM((12, 8, WIDTH), bf16),
                pltpu.VMEM(shapes[8], bf16),
                pltpu.VMEM(shapes[9], bf16),
                pltpu.VMEM((4, 8, WIDTH), bf16),
                dma((7,)), dma((3,)), dma((3 + len(SMALL),)),
                dma((3, 4)), dma((3, 3, 4)), dma((3, 3, 4)), dma((3, 2)), dma((3, 2)), dma((3,)), dma((3,)),
                dma((3,)), dma((3,)), dma((3,)), dma((DEVS,)), dma((DEVS,)),
                dma((3, 8)), dma((3, 8)), dma((3, 8)), dma((3, 8)),
            ],
            compiler_params=pltpu.CompilerParams(
                collective_id=0, has_side_effects=True, vmem_limit_bytes=26_500_000),
        )(*tiled, *state, arrays[GRAD_COUNT + 3])
        kept = [pltpu.with_memory_space_constraint(arr, pltpu.VMEM) for arr in kept]
        outs = pl.pallas_call(
            flush,
            out_shape=[jax.ShapeDtypeStruct((EMBED_TILES, 8, WIDTH), bf16)] + small
            + [jax.ShapeDtypeStruct((SHARD_ROWS, LANES), f32)] * 3,
            in_specs=[vmem_spec] * 4,
            out_specs=[any_spec] * 13,
            scratch_shapes=[
                pltpu.VMEM((3840, LANES), f32),
                pltpu.VMEM((2, 3840, LANES), bf16),
                pltpu.VMEM((48, 8, WIDTH), bf16),
                pltpu.VMEM((12, 8, WIDTH), bf16),
                pltpu.VMEM((12, 8, WIDTH), bf16),
                pltpu.VMEM(shapes[8], bf16),
                pltpu.VMEM(shapes[9], bf16),
                dma((20,)),
            ],
            compiler_params=pltpu.CompilerParams(has_side_effects=True, vmem_limit_bytes=5_200_000),
        )(*kept)
        params = []
        for i, dims in enumerate(shapes):
            if i in (1, 2, 3):
                params.append(jnp.swapaxes(outs[i].reshape(dims[0], dims[2], dims[1]), 1, 2))
            else:
                params.append(outs[i].reshape(dims))
        return tuple(params) + tuple(arr.reshape(-1) for arr in outs[GRAD_COUNT:])

    in_specs = tuple([P("dp")] * GRAD_COUNT + [P("dp"), P("dp"), P("dp"), P()])
    out_specs = tuple([P()] * GRAD_COUNT + [P("dp"), P("dp"), P("dp")])
    return jax.shard_map(local_update, mesh=mesh, in_specs=in_specs, out_specs=out_specs, check_vma=False)
```

```python
import functools
import math
import jax
import jax.numpy as jnp
from jax import lax
from jax.experimental import pallas as pl
from jax.experimental.pallas import tpu as pltpu
from jax.sharding import PartitionSpec as P

ADAM_STEP = 7
ADAM_EPS = 1e-8
CLIP_EPS = 1e-6
GRAD_COUNT = 10
MESH = pl.DeviceIdType.MESH

DEVS = 16
OTHERS = range(1, DEVS)
THIRDS = range(3)
PAIR = range(2)
LANES = 128
WIDTH = 640
SHARD_ROWS = 6149
TILE_ROWS = 40
EMBED_TILES = 2048
ALL_TILES = 2460
DECAY_ROWS = 98240
FIRST_TAIL = 13
TAIL_START = (SHARD_ROWS * FIRST_TAIL) // TILE_ROWS
RS_TILES = 52
TAIL_TILES = (SHARD_ROWS * 15) // TILE_ROWS + 3 * RS_TILES - TAIL_START
AG_TILES = 51
LEAD = 40
G_ROWS = LEAD + 3 * RS_TILES * TILE_ROWS
ORDERS = ((2, 4, 8), (4, 8, 2), (8, 2, 4))


def flip(dev, stride):
    return dev + stride - 2 * stride * lax.rem(dev // stride, 2)


def rs_start(dev):
    return (SHARD_ROWS * dev) // TILE_ROWS


def ag_start(dev):
    return (SHARD_ROWS * dev + TILE_ROWS - 1) // TILE_ROWS


def flip_mask(dev, order, mask):
    for bit, stride in enumerate(order):
        if mask >> bit & 1:
            dev = flip(dev, stride)
    return dev


SMALL = {}
for _name, _tiles in (("q", 48), ("k", 12), ("v", 12), ("out", 48), ("gate", 96), ("up", 96),
                      ("down", 96), ("norms", 3), ("qk", 1)):
    SMALL[_name] = (EMBED_TILES if not SMALL else sum(SMALL[_last]), _tiles)
    _last = _name
LAYERS = 6
COLS = WIDTH // LANES
OUT_TILES = 48 * RS_TILES
SPARE = 42 * RS_TILES
PIECE_ROWS = RS_TILES * TILE_ROWS


def slot_tiles(slot, k, f):
    index = 36 + f * 3 + k if slot == 3 else (slot * 3 + k) * 4 + f
    return pl.ds(index * RS_TILES, RS_TILES)


def sum_rows(k, f):
    return pl.ds((f * 3 + k) * PIECE_ROWS, PIECE_ROWS)


def put_tile(dst, tile, rows, first, stride):
    for j in range(COLS):
        dst[tile, :, LANES * j:LANES * (j + 1)] = rows[pl.ds(first + j, 8, stride=stride), :].astype(jnp.bfloat16)


def pack_wide(src, dst, first_tile, rows, tiles):
    def step(i, _):
        rows[pl.ds(pl.multiple_of(i * 80, 16), 80), :] = src[pl.ds(pl.multiple_of(i * 80, 16), 80), :].astype(jnp.float32)
        for half in PAIR:
            put_tile(dst, first_tile + 2 * i + half, rows, i * 80 + half * 40, COLS)
        return 0

    lax.fori_loop(0, tiles // 2, step, 0)


def pack_narrow(src, dst, first_tile, rows, width):
    folds = LANES // width
    lane = lax.broadcasted_iota(jnp.int32, (8, LANES), 1) // width
    for layer in range(LAYERS):
        block = src[pl.ds(layer * width // 8, width // 8)].astype(jnp.float32).reshape(width, WIDTH)
        rows[pl.ds(layer * WIDTH, WIDTH), :] = jnp.concatenate([block] * folds, axis=0).T
    tiles = LAYERS * width // 8

    def step(t, _):
        for j in range(COLS):
            first = folds * (40 * t + j)
            value = rows[pl.ds(first, 8, stride=folds * COLS), :]
            for fold in range(1, folds):
                value = jnp.where(lane == fold, rows[pl.ds(first + fold, 8, stride=folds * COLS), :], value)
            dst[first_tile + t, :, LANES * j:LANES * (j + 1)] = value.astype(jnp.bfloat16)
        return 0

    lax.fori_loop(0, tiles, step, 0)


def unpack_wide(src, first_tile, dst, rows, tiles):
    def step(i, _):
        for half in PAIR:
            for j in range(COLS):
                rows[pl.ds(i * 80 + half * 40 + j, 8, stride=COLS), :] = src[
                    first_tile + 2 * i + half, :, LANES * j:LANES * (j + 1)].astype(jnp.float32)
        dst[pl.ds(pl.multiple_of(i * 80, 16), 80), :] = rows[pl.ds(pl.multiple_of(i * 80, 16), 80), :].astype(jnp.bfloat16)
        return 0

    lax.fori_loop(0, tiles // 2, step, 0)


def unpack_narrow(src, first_tile, dst, rows, width):
    folds = LANES // width
    tiles = LAYERS * width // 8

    def step(t, _):
        for j in range(COLS):
            value = src[first_tile + t, :, LANES * j:LANES * (j + 1)].astype(jnp.float32)
            for fold in range(folds):
                turned = value if fold == 0 else pltpu.roll(value, LANES - fold * width, 1)
                rows[pl.ds(folds * (40 * t + j) + fold, 8, stride=folds * COLS), :] = turned
        return 0

    lax.fori_loop(0, tiles, step, 0)
    for layer in range(LAYERS):
        block = rows[pl.ds(layer * WIDTH, WIDTH), :].T[:width]
        dst[pl.ds(layer * width // 8, width // 8)] = block.reshape(width // 8, 8, WIDTH).astype(jnp.bfloat16)


def kernel(emb, gq, gk, gv, go, gg, gu, gd, gn, gqk, m_in, v_in, p_in, hyp_in, mom, vel, par, vout, tail,
           s1, r2, r3, ext, hyp, nsend, nrecv, wide_raw, q_raw, k_raw, v_raw, n_raw, qk_raw, n_tiles,
           raw_sem, relay_sem, tail_sem,
           own_sem, r1_send, r1_recv, r2_send, r2_recv, r3_send, r3_recv, st_sem,
           ext_send, ext_recv, n_send, n_recv, ag_send, ag_recv, d2d_send, d2d_recv):
    grad = s1.at[pl.ds(0, G_ROWS)]
    me = lax.axis_index("dp")
    partner = flip(me, 1)

    def remote(src, dst, ssem, rsem, dev):
        return pltpu.make_async_remote_copy(
            src_ref=src, dst_ref=dst, send_sem=ssem, recv_sem=rsem, device_id=(dev,), device_id_type=MESH)

    def from_shard(owner, k, make, embed=True, small=True):
        first = rs_start(owner) + k * RS_TILES

        if embed:
            @pl.when(owner < FIRST_TAIL)
            def _():
                make(emb.at[pl.ds(first, RS_TILES)]).start()

        if small:
            @pl.when(owner >= FIRST_TAIL)
            def _():
                make(tail.at[pl.ds(first - TAIL_START, RS_TILES)]).start()

    def rs_owner(dev, k, f):
        return flip_mask(dev, ORDERS[k], (0 if f >= 2 else 2) + (4 if f % 2 == 0 else 0))

    state = [pltpu.make_async_copy(src, dst, st_sem.at[i])
             for i, (src, dst) in enumerate(((m_in, mom), (v_in, vel), (p_in, par), (hyp_in, hyp)))]

    def load_own(f, embed=True, small=True):
        for k in THIRDS:
            from_shard(rs_owner(me, k, f), k, lambda src, k=k: pltpu.make_async_copy(
                src, vout.at[slot_tiles(3, k, f)], own_sem.at[k, f]), embed, small)

    def send_first(f, embed=True, small=True):
        for k in THIRDS:
            for slot in THIRDS:
                dev = partner if slot == 2 else flip(me, ORDERS[k][0])
                if slot == 1:
                    dev = flip(dev, 1)
                from_shard(rs_owner(dev, k, f), k, lambda src, k=k, slot=slot, dev=dev: remote(
                    src, vout.at[slot_tiles(slot, k, f)], r1_send.at[slot, k, f], r1_recv.at[slot, k, f], dev),
                    embed, small)

    barrier = pltpu.get_barrier_semaphore()
    near = [flip(me, order[0]) for order in ORDERS]
    near += [flip(dev, 1) for dev in near] + [partner]
    for dev in near:
        pl.semaphore_signal(barrier, inc=1, device_id=(dev,), device_id_type=MESH)
    raw = [pltpu.make_async_copy(src, dst, raw_sem.at[i]) for i, (src, dst) in enumerate((
        (gg, wide_raw.at[0]), (gu, wide_raw.at[1]), (gq, q_raw), (gk, k_raw), (gv, v_raw), (gn, n_raw), (gqk, qk_raw)))]
    for copy in raw:
        copy.start()
    edge = EMBED_TILES - TAIL_START
    relayed = []
    start = SPARE
    for i, (src, first, tiles) in enumerate(((go, SMALL["out"][0], 48), (gd, SMALL["down"][0], 96),
                                             (emb.at[pl.ds(TAIL_START, edge)], TAIL_START, edge))):
        part = vout.at[pl.ds(start, tiles)]
        copy = pltpu.make_async_copy(src, part, relay_sem.at[i])
        copy.start()
        relayed.append((copy, pltpu.make_async_copy(part, tail.at[pl.ds(first - TAIL_START, tiles)], tail_sem.at[i])))
        start += tiles
    for f in PAIR:
        load_own(f, small=False)
    pl.semaphore_wait(barrier, len(near))
    for f in THIRDS:
        send_first(f, small=False)

    for copy, onward in relayed:
        copy.wait()
        onward.start()
    onwards = [onward for _, onward in relayed]

    raw_names = list(SMALL)

    def to_tail(src, name):
        first, tiles = SMALL[name]
        copy = pltpu.make_async_copy(src, tail.at[pl.ds(first - TAIL_START, tiles)], tail_sem.at[3 + raw_names.index(name)])
        copy.start()
        onwards.append(copy)

    spare = start
    for i, name in enumerate(("gate", "up")):
        raw[i].wait()
        pack_wide(wide_raw.at[i], vout, spare, grad, 96)
        to_tail(vout.at[pl.ds(spare, 96)], name)
        onwards.pop().wait()
    for i, (name, src, width) in enumerate((("q", q_raw, 64), ("k", k_raw, 16), ("v", v_raw, 16))):
        raw[2 + i].wait()
        pack_narrow(src, vout, spare, grad, width)
        tiles = SMALL[name][1]
        to_tail(vout.at[pl.ds(spare, tiles)], name)
        spare += tiles
    raw[5].wait()
    raw[6].wait()
    for i in THIRDS:
        n_tiles[i] = jnp.concatenate([n_raw[2 * i].astype(jnp.float32), n_raw[2 * i + 1].astype(jnp.float32)],
                                     axis=0).astype(jnp.bfloat16)
    grad[24:40, :] = jnp.zeros((16, LANES), jnp.float32)
    for layer in range(LAYERS):
        pair = qk_raw[layer].astype(jnp.float32)
        for i in PAIR:
            for half in PAIR:
                row = (2 * layer + i) * 2 + half
                grad[row:row + 1, :] = pair[i:i + 1, LANES * half:LANES * (half + 1)]
    put_tile(n_tiles, 3, grad, 0, COLS)
    to_tail(n_tiles.at[pl.ds(0, 3)], "norms")
    to_tail(n_tiles.at[pl.ds(3, 1)], "qk")
    for copy in onwards:
        copy.wait()
    for f in range(4):
        send_first(f, embed=f == 3)
        load_own(f, embed=f > 1)
    before = lax.rem(me + DEVS - 1, DEVS)
    ext_copies = [remote(src.at[pl.ds(0, TILE_ROWS)], ext.at[i], ext_send.at[i], ext_recv.at[i], before)
                  for i, src in enumerate((m_in, v_in, p_in))]
    for copy in state:
        copy.start()

    def r1_copy(slot, k, f):
        return remote(emb.at[pl.ds(0, RS_TILES)], vout.at[slot_tiles(slot, k, f)], r1_send.at[slot, k, f],
                      r1_recv.at[slot, k, f], partner)

    def r2_copy(k, f):
        return remote(s1.at[sum_rows(k, f)], r2.at[k, f], r2_send.at[k, f], r2_recv.at[k, f], flip(me, ORDERS[k][1]))

    def r3_copy(k):
        return remote(s1.at[sum_rows(k, 2)], r3.at[k], r3_send.at[k], r3_recv.at[k], flip(me, ORDERS[k][2]))

    for f in range(4):
        for k in THIRDS:
            pltpu.make_async_copy(
                emb.at[pl.ds(0, RS_TILES)], vout.at[slot_tiles(3, k, f)], own_sem.at[k, f]).wait()
            for slot in (2, 0, 1):
                r1_copy(slot, k, f).wait_recv()

            def add_four(t, _, k=k, f=f):
                a, b, c, d = [vout[slot_tiles(slot, k, f).start + t].astype(jnp.float32) for slot in (3, 2, 0, 1)]
                total = (a + b) + (c + d)
                row = sum_rows(k, f).start + TILE_ROWS * t
                for j in range(COLS):
                    s1[pl.ds(pl.multiple_of(row + 8 * j, 8), 8), :] = total[:, LANES * j:LANES * (j + 1)]
                return 0

            lax.fori_loop(0, RS_TILES, add_four, 0, unroll=2)
            if f < 2:
                r2_copy(k, f).start()
    for f in PAIR:
        for k in THIRDS:
            r2_copy(k, f).wait_recv()

            def add_two(t, _, k=k, f=f):
                row = pl.multiple_of(TILE_ROWS * t, 8)
                at = pl.ds(pl.multiple_of(sum_rows(k, 2 + f).start + TILE_ROWS * t, 8), TILE_ROWS)
                s1[at, :] = s1[at, :] + r2[k, f, pl.ds(row, TILE_ROWS), :]
                return 0

            lax.fori_loop(0, RS_TILES, add_two, 0, unroll=2)
            if f == 0:
                r3_copy(k).start()

    shift = LEAD - (SHARD_ROWS * me - TILE_ROWS * rs_start(me))
    for k in THIRDS:
        for f in PAIR:
            r2_copy(k, f).wait_send()
    for k in THIRDS:
        r3_copy(k).wait_recv()

        def finish(t, _, k=k):
            row = pl.multiple_of(TILE_ROWS * t, 8)
            at = pl.ds(pl.multiple_of(sum_rows(k, 3).start + TILE_ROWS * t, 8), TILE_ROWS)
            total = (s1[at, :] + r3[k, pl.ds(row, TILE_ROWS), :]) * (1.0 / DEVS)
            row = shift + TILE_ROWS * (k * RS_TILES + t)
            for j in range(COLS):
                grad[pl.ds(row + j, 8, stride=COLS), :] = total[8 * j:8 * (j + 1), :]
            return 0

        lax.fori_loop(0, RS_TILES, finish, 0, unroll=2)
    for copy in ext_copies:
        copy.start()

    def squares(i, acc):
        part = grad[pl.ds(pl.multiple_of(LEAD + i * 40, 8), 40), :]
        return acc + part * part

    acc = lax.fori_loop(0, 153, squares, jnp.zeros((40, LANES), jnp.float32), unroll=3)
    nsend[...] = acc[0:8] + acc[8:16] + acc[16:24] + acc[24:32] + acc[32:40]
    for row in (6120, 6128, 6136):
        part = grad[pl.ds(LEAD + row, 8), :]
        nsend[...] = nsend[...] + part * part
    part = grad[pl.ds(LEAD + 6144, 5), :]
    nsend[0:5, :] = nsend[0:5, :] + part * part

    def n_copy(j):
        return remote(nsend, nrecv.at[me], n_send.at[j], n_recv.at[me], lax.rem(me + j, DEVS))

    for j in OTHERS:
        n_copy(j).start()

    for copy in state:
        copy.wait()

    def full(value):
        return jnp.full((8, LANES), value, jnp.float32)

    learn_rate, beta_one, beta_two, decay, max_norm = [full(hyp[i]) for i in range(5)]
    rest_one, rest_two = 1.0 - beta_one, 1.0 - beta_two
    hat_one = 1.0 / (1.0 - lax.integer_pow(beta_one, ADAM_STEP))
    hat_two = 1.0 / (1.0 - lax.integer_pow(beta_two, ADAM_STEP))
    for copy in ext_copies:
        copy.wait_recv()

    for j in OTHERS:
        n_copy(j).wait_send()
        source = lax.rem(me + DEVS - j, DEVS)
        remote(nsend, nrecv.at[source], n_send.at[j], n_recv.at[source], partner).wait_recv()
    nrecv[me] = nsend[...]
    total = nrecv[0]
    for j in OTHERS:
        total = total + nrecv[j]
    total = jnp.sum(jnp.sum(total, axis=1, keepdims=True), axis=0, keepdims=True)
    clip = jnp.minimum(1.0, max_norm / (jnp.sqrt(jnp.broadcast_to(total, (8, LANES))) + CLIP_EPS))

    def wide(value, rows):
        if rows <= 8:
            return value[:rows]
        return jnp.concatenate([value] * (rows // 8), axis=0)

    def adam(g, m, v, p, first_row, rows):
        clipped = g * wide(clip, rows)
        m = wide(beta_one, rows) * m + wide(rest_one, rows) * clipped
        v = wide(beta_two, rows) * v + wide(rest_two, rows) * (clipped * clipped)
        index = first_row + lax.broadcasted_iota(jnp.int32, (rows, LANES), 0)
        update = (m * wide(hat_one, rows)) / (jnp.sqrt(v * wide(hat_two, rows)) + ADAM_EPS)
        update = update + jnp.where(index < DECAY_ROWS, wide(decay, rows) * p, 0.0)
        return m, v, p - wide(learn_rate, rows) * update

    def adam_rows(row, rows):
        at = pl.ds(row, rows)
        shifted = pl.ds(row + LEAD, rows)
        m, v, p = adam(grad[shifted, :], mom[at, :], vel[at, :], par[at, :], SHARD_ROWS * me + row, rows)
        mom[at, :] = m
        vel[at, :] = v
        par[at, :] = p
        grad[shifted, :] = p

    def adam_block(i, _):
        adam_rows(pl.multiple_of(i * 40, 8), 40)
        return 0

    def ag_sizes(owner, k, run):
        if k < 2:
            run(AG_TILES)
            return
        longer = ag_start(owner + 1) - ag_start(owner) == 3 * AG_TILES + 1

        @pl.when(longer)
        def _():
            run(AG_TILES + 1)

        @pl.when(jnp.logical_not(longer))
        def _():
            run(AG_TILES)

    def ag_each(k, mask, run, dev=me):
        owner = flip_mask(dev, ORDERS[k], mask)
        first = ag_start(owner) + k * AG_TILES
        ag_sizes(owner, k, lambda size: run(vout.at[pl.ds(first, size)], size))

    def ag_link(k, mask, link, start=True):
        dev = flip(me, ORDERS[k][link])
        slot = mask + (1 << link)

        def copy(dst, size):
            return remote(dst, dst, ag_send.at[k, slot], ag_recv.at[k, slot], dev)

        if start:
            ag_each(k, mask, lambda dst, size: copy(dst, size).start())
        pending.append(lambda: ag_each(k, mask, lambda dst, size: copy(dst, size).wait_send()))

    def ag_across(k, mask, start=True):
        def copy(dst, size):
            return remote(dst, dst, d2d_send.at[k, mask], d2d_recv.at[k, mask], partner)

        if start:
            ag_each(k, mask, lambda dst, size: copy(dst, size).start())
        pending.append(lambda: ag_each(k, mask, lambda dst, size: copy(dst, size).wait_send()))

    def ag_arrived(k, mask):
        ag_each(k, mask, lambda dst, size: remote(
            dst, dst, ag_send.at[k, mask], ag_recv.at[k, mask], partner).wait_recv())

    pending = []
    base = LEAD + TILE_ROWS * ag_start(me) - SHARD_ROWS * me

    def own_part(k, skip, count, blocks):
        lax.fori_loop(*blocks, adam_block, 0)
        if k == 2:
            adam_rows(6120, 24)
            adam_rows(6144, 5)
            at = pl.ds(LEAD + SHARD_ROWS, TILE_ROWS)
            _, _, p = adam(grad[at, :], ext[0], ext[1], ext[2], SHARD_ROWS * (me + 1), TILE_ROWS)
            grad[at, :] = p
        first = ag_start(me) + k * AG_TILES

        def pack(t, _):
            put_tile(vout, first + t, grad, base + TILE_ROWS * (k * AG_TILES + t), COLS)
            return 0

        lax.fori_loop(skip, skip + (ag_start(me + 1) - first if k == 2 else count), pack, 0)

        def send(size):
            part = vout.at[pl.ds(first + skip, size)]
            for link in THIRDS:
                slot = 1 << link
                remote(part, part, ag_send.at[k, slot], ag_recv.at[k, slot], flip(me, ORDERS[k][link])).start()
            remote(part, part, d2d_send.at[k, 0], d2d_recv.at[k, 0], partner).start()

        if k == 2:
            ag_sizes(me, k, send)
        else:
            send(count)

    own_part(0, 0, 13, (0, 14))
    own_part(0, 13, 13, (14, 27))
    own_part(0, 26, 25, (27, 52))
    own_part(1, 0, AG_TILES, (52, 103))
    own_part(2, 0, None, (103, 153))
    for k in THIRDS:
        for link in THIRDS:
            ag_link(k, 0, link, start=False)
        ag_across(k, 0, start=False)
    for k in THIRDS:
        ag_arrived(k, 1)
        ag_link(k, 1, 1)
        ag_across(k, 1)
    for k in THIRDS:
        ag_link(k, 1, 2)
    for k in THIRDS:
        ag_arrived(k, 2)
        ag_link(k, 2, 2)
        ag_across(k, 2)
    for k in THIRDS:
        ag_arrived(k, 4)
        ag_across(k, 4)
    for k in THIRDS:
        ag_arrived(k, 3)
        ag_link(k, 3, 2)
        ag_across(k, 3)
    for mask in (5, 6, 7):
        for k in THIRDS:
            ag_arrived(k, mask)
            ag_across(k, mask)
    for mask in range(8):
        for k in THIRDS:
            ag_each(k, mask, lambda dst, size, k=k, mask=mask: remote(
                dst, dst, d2d_send.at[k, mask], d2d_recv.at[k, mask], partner).wait_recv(), partner)
    for wait in pending:
        wait()
    for copy in ext_copies:
        copy.wait_send()
    for f in range(4):
        for k in THIRDS:
            for slot in THIRDS:
                r1_copy(slot, k, f).wait_send()
    for k in THIRDS:
        r3_copy(k).wait_send()


def flush(mom, vel, par, vout, embed, oq, ok, ov, oo, og, ou, od, on, oqk, m_out, v_out, p_out,
          rows, wide_out, q_out, k_out, v_new, n_out, qk_out, sem):
    copies = []

    def send(src, dst):
        copy = pltpu.make_async_copy(src, dst, sem.at[len(copies)])
        copy.start()
        copies.append(copy)

    for i in range(4):
        part = pl.ds(i * EMBED_TILES // 4, EMBED_TILES // 4)
        send(vout.at[part], embed.at[part])
    for src, dst in ((mom, m_out), (vel, v_out), (par, p_out)):
        send(src, dst)
    for name, dst in (("out", oo), ("down", od)):
        send(vout.at[pl.ds(*SMALL[name])], dst)
    for i, (name, dst) in enumerate((("gate", og), ("up", ou))):
        unpack_wide(vout, SMALL[name][0], wide_out.at[i], rows, 96)
        send(wide_out.at[i], dst)
    for name, block, dst, width in (("q", q_out, oq, 64), ("k", k_out, ok, 16), ("v", v_new, ov, 16)):
        unpack_narrow(vout, SMALL[name][0], block, rows, width)
        send(block, dst)
    for i in THIRDS:
        tile = vout[SMALL["norms"][0] + i].astype(jnp.float32)
        n_out[2 * i] = tile[0:4].astype(jnp.bfloat16)
        n_out[2 * i + 1] = tile[4:8].astype(jnp.bfloat16)
    send(n_out, on)
    for j in range(COLS):
        rows[pl.ds(j, 8, stride=COLS), :] = vout[SMALL["qk"][0], :, LANES * j:LANES * (j + 1)].astype(jnp.float32)
    for layer in range(LAYERS):
        four = rows[4 * layer:4 * layer + 4, :]
        pair = [jnp.concatenate([four[2 * i:2 * i + 1], four[2 * i + 1:2 * i + 2]], axis=1) for i in PAIR]
        qk_out[layer] = jnp.concatenate(pair, axis=0).astype(jnp.bfloat16)
    send(qk_out, oqk)
    for copy in copies:
        copy.wait()


def solution(mesh):
    def local_update(*arrays):
        grads = [arr.reshape(arr.shape[1:]) for arr in arrays[:GRAD_COUNT]]
        state = [arr.reshape(SHARD_ROWS, LANES) for arr in arrays[GRAD_COUNT:GRAD_COUNT + 3]]
        shapes = [grad_arr.shape for grad_arr in grads]
        any_spec = pl.BlockSpec(memory_space=pl.ANY)
        vmem_spec = pl.BlockSpec(memory_space=pltpu.VMEM)
        dma = pltpu.SemaphoreType.DMA
        bf16, f32 = jnp.bfloat16, jnp.float32
        tiled = []
        for i, grad_arr in enumerate(grads[:8]):
            if i in (1, 2, 3):
                grad_arr = jnp.swapaxes(grad_arr, 1, 2)
            tiled.append(grad_arr.reshape(-1, LANES) if i in (5, 6) else grad_arr.reshape(-1, 8, WIDTH))
        tiled += grads[8:]
        small = [jax.ShapeDtypeStruct(arr.shape, bf16) for arr in tiled[1:]]
        *kept, _ = pl.pallas_call(
            kernel,
            out_shape=[pltpu.VMEM((SHARD_ROWS, LANES), f32)] * 3
            + [pltpu.VMEM((OUT_TILES, 8, WIDTH), bf16)]
            + [pltpu.HBM((TAIL_TILES, 8, WIDTH), bf16)],
            in_specs=[any_spec] * 14,
            out_specs=[vmem_spec] * 4 + [any_spec],
            scratch_shapes=[
                pltpu.VMEM((3 * 4 * PIECE_ROWS, LANES), f32),
                pltpu.VMEM((3, 2, PIECE_ROWS, LANES), f32),
                pltpu.VMEM((3, PIECE_ROWS, LANES), f32),
                pltpu.VMEM((3, TILE_ROWS, LANES), f32),
                pltpu.SMEM((5,), f32),
                pltpu.VMEM((8, LANES), f32),
                pltpu.VMEM((DEVS, 8, LANES), f32),
                pltpu.VMEM((2, 3840, LANES), bf16),
                pltpu.VMEM((48, 8, WIDTH), bf16),
                pltpu.VMEM((12, 8, WIDTH), bf16),
                pltpu.VMEM((12, 8, WIDTH), bf16),
                pltpu.VMEM(shapes[8], bf16),
                pltpu.VMEM(shapes[9], bf16),
                pltpu.VMEM((4, 8, WIDTH), bf16),
                dma((7,)), dma((3,)), dma((3 + len(SMALL),)),
                dma((3, 4)), dma((3, 3, 4)), dma((3, 3, 4)), dma((3, 2)), dma((3, 2)), dma((3,)), dma((3,)),
                dma((4,)), dma((3,)), dma((3,)), dma((DEVS,)), dma((DEVS,)),
                dma((3, 8)), dma((3, 8)), dma((3, 8)), dma((3, 8)),
            ],
            compiler_params=pltpu.CompilerParams(
                collective_id=0, has_side_effects=True, vmem_limit_bytes=26_500_000),
        )(*tiled, *state, arrays[GRAD_COUNT + 3])
        kept = [pltpu.with_memory_space_constraint(arr, pltpu.VMEM) for arr in kept]
        outs = pl.pallas_call(
            flush,
            out_shape=[jax.ShapeDtypeStruct((EMBED_TILES, 8, WIDTH), bf16)] + small
            + [jax.ShapeDtypeStruct((SHARD_ROWS, LANES), f32)] * 3,
            in_specs=[vmem_spec] * 4,
            out_specs=[any_spec] * 13,
            scratch_shapes=[
                pltpu.VMEM((3840, LANES), f32),
                pltpu.VMEM((2, 3840, LANES), bf16),
                pltpu.VMEM((48, 8, WIDTH), bf16),
                pltpu.VMEM((12, 8, WIDTH), bf16),
                pltpu.VMEM((12, 8, WIDTH), bf16),
                pltpu.VMEM(shapes[8], bf16),
                pltpu.VMEM(shapes[9], bf16),
                dma((20,)),
            ],
            compiler_params=pltpu.CompilerParams(has_side_effects=True, vmem_limit_bytes=5_200_000),
        )(*kept)
        params = []
        for i, dims in enumerate(shapes):
            if i in (1, 2, 3):
                params.append(jnp.swapaxes(outs[i].reshape(dims[0], dims[2], dims[1]), 1, 2))
            else:
                params.append(outs[i].reshape(dims))
        return tuple(params) + tuple(arr.reshape(-1) for arr in outs[GRAD_COUNT:])

    in_specs = tuple([P("dp")] * GRAD_COUNT + [P("dp"), P("dp"), P("dp"), P()])
    out_specs = tuple([P()] * GRAD_COUNT + [P("dp"), P("dp"), P("dp")])
    return jax.shard_map(local_update, mesh=mesh, in_specs=in_specs, out_specs=out_specs, check_vma=False)
```

```python
import functools
import math
import jax
import jax.numpy as jnp
from jax import lax
from jax.experimental import pallas as pl
from jax.experimental.pallas import tpu as pltpu
from jax.sharding import PartitionSpec as P

ADAM_STEP = 7
ADAM_EPS = 1e-8
CLIP_EPS = 1e-6
GRAD_COUNT = 10
MESH = pl.DeviceIdType.MESH

DEVS = 16
OTHERS = range(1, DEVS)
THIRDS = range(3)
PAIR = range(2)
LANES = 128
WIDTH = 640
SHARD_ROWS = 6149
TILE_ROWS = 40
EMBED_TILES = 2048
ALL_TILES = 2460
DECAY_ROWS = 98240
FIRST_TAIL = 13
TAIL_START = (SHARD_ROWS * FIRST_TAIL) // TILE_ROWS
RS_TILES = 52
TAIL_TILES = (SHARD_ROWS * 15) // TILE_ROWS + 3 * RS_TILES - TAIL_START
AG_TILES = 51
PART_TILES = 13
LAST_PART = 3
FLUSH_PARTS = 16
LEAD = 40
G_ROWS = LEAD + 3 * RS_TILES * TILE_ROWS
ORDERS = ((2, 4, 8), (4, 8, 2), (8, 2, 4))


def flip(dev, stride):
    return dev + stride - 2 * stride * lax.rem(dev // stride, 2)


def rs_start(dev):
    return (SHARD_ROWS * dev) // TILE_ROWS


def ag_start(dev):
    return (SHARD_ROWS * dev + TILE_ROWS - 1) // TILE_ROWS


def flip_mask(dev, order, mask):
    for bit, stride in enumerate(order):
        if mask >> bit & 1:
            dev = flip(dev, stride)
    return dev


SMALL = {}
for _name, _tiles in (("q", 48), ("k", 12), ("v", 12), ("out", 48), ("gate", 96), ("up", 96),
                      ("down", 96), ("norms", 3), ("qk", 1)):
    SMALL[_name] = (EMBED_TILES if not SMALL else sum(SMALL[_last]), _tiles)
    _last = _name
LAYERS = 6
COLS = WIDTH // LANES
OUT_TILES = 48 * RS_TILES
SPARE = 42 * RS_TILES
PIECE_ROWS = RS_TILES * TILE_ROWS
HALF_TILES = RS_TILES // 2
HALF_ROWS = PIECE_ROWS // 2


def slot_tiles(slot, k, f):
    index = 36 + f * 3 + k if slot == 3 else (slot * 3 + k) * 4 + f
    return pl.ds(index * RS_TILES, RS_TILES)


def sum_rows(k, f):
    return pl.ds((f * 3 + k) * PIECE_ROWS, PIECE_ROWS)


def put_tile(dst, tile, rows, first, stride):
    for j in range(COLS):
        dst[tile, :, LANES * j:LANES * (j + 1)] = rows[pl.ds(first + j, 8, stride=stride), :].astype(jnp.bfloat16)


def pack_wide(src, dst, first_tile, rows, tiles):
    def step(i, _):
        rows[pl.ds(pl.multiple_of(i * 80, 16), 80), :] = src[pl.ds(pl.multiple_of(i * 80, 16), 80), :].astype(jnp.float32)
        for half in PAIR:
            put_tile(dst, first_tile + 2 * i + half, rows, i * 80 + half * 40, COLS)
        return 0

    lax.fori_loop(0, tiles // 2, step, 0)


def pack_narrow(src, dst, first_tile, rows, width):
    folds = LANES // width
    lane = lax.broadcasted_iota(jnp.int32, (8, LANES), 1) // width
    for layer in range(LAYERS):
        block = src[pl.ds(layer * width // 8, width // 8)].astype(jnp.float32).reshape(width, WIDTH)
        rows[pl.ds(layer * WIDTH, WIDTH), :] = jnp.concatenate([block] * folds, axis=0).T
    tiles = LAYERS * width // 8

    def step(t, _):
        for j in range(COLS):
            first = folds * (40 * t + j)
            value = rows[pl.ds(first, 8, stride=folds * COLS), :]
            for fold in range(1, folds):
                value = jnp.where(lane == fold, rows[pl.ds(first + fold, 8, stride=folds * COLS), :], value)
            dst[first_tile + t, :, LANES * j:LANES * (j + 1)] = value.astype(jnp.bfloat16)
        return 0

    lax.fori_loop(0, tiles, step, 0)


def unpack_wide(src, first_tile, dst, rows, tiles):
    def step(i, _):
        for half in PAIR:
            for j in range(COLS):
                rows[pl.ds(i * 80 + half * 40 + j, 8, stride=COLS), :] = src[
                    first_tile + 2 * i + half, :, LANES * j:LANES * (j + 1)].astype(jnp.float32)
        dst[pl.ds(pl.multiple_of(i * 80, 16), 80), :] = rows[pl.ds(pl.multiple_of(i * 80, 16), 80), :].astype(jnp.bfloat16)
        return 0

    lax.fori_loop(0, tiles // 2, step, 0)


def unpack_narrow(src, first_tile, dst, rows, width):
    folds = LANES // width
    tiles = LAYERS * width // 8

    def step(t, _):
        for j in range(COLS):
            value = src[first_tile + t, :, LANES * j:LANES * (j + 1)].astype(jnp.float32)
            for fold in range(folds):
                turned = value if fold == 0 else pltpu.roll(value, LANES - fold * width, 1)
                rows[pl.ds(folds * (40 * t + j) + fold, 8, stride=folds * COLS), :] = turned
        return 0

    lax.fori_loop(0, tiles, step, 0)
    for layer in range(LAYERS):
        block = rows[pl.ds(layer * WIDTH, WIDTH), :].T[:width]
        dst[pl.ds(layer * width // 8, width // 8)] = block.reshape(width // 8, 8, WIDTH).astype(jnp.bfloat16)


def kernel(emb, gq, gk, gv, go, gg, gu, gd, gn, gqk, m_in, v_in, p_in, hyp_in, mom, vel, par, vout, tail,
           s1, r2, r3, ext, hyp, nsend, nrecv, wide_raw, q_raw, k_raw, v_raw, n_raw, qk_raw, n_tiles,
           raw_sem, relay_sem, tail_sem,
           own_sem, r1_send, r1_recv, r2_send, r2_recv, r3_send, r3_recv, st_sem,
           ext_send, ext_recv, n_send, n_recv, ag_send, ag_recv, d2d_send, d2d_recv, last_recv):
    grad = s1.at[pl.ds(0, G_ROWS)]
    me = lax.axis_index("dp")
    partner = flip(me, 1)

    def remote(src, dst, ssem, rsem, dev):
        return pltpu.make_async_remote_copy(
            src_ref=src, dst_ref=dst, send_sem=ssem, recv_sem=rsem, device_id=(dev,), device_id_type=MESH)

    def from_shard(owner, k, make, embed=True, small=True):
        first = rs_start(owner) + k * RS_TILES

        if embed:
            @pl.when(owner < FIRST_TAIL)
            def _():
                make(emb.at[pl.ds(first, RS_TILES)]).start()

        if small:
            @pl.when(owner >= FIRST_TAIL)
            def _():
                make(tail.at[pl.ds(first - TAIL_START, RS_TILES)]).start()

    def rs_owner(dev, k, f):
        return flip_mask(dev, ORDERS[k], (0 if f >= 2 else 2) + (4 if f % 2 == 0 else 0))

    state = [pltpu.make_async_copy(src, dst, st_sem.at[i])
             for i, (src, dst) in enumerate(((m_in, mom), (v_in, vel), (p_in, par), (hyp_in, hyp)))]

    def load_own(f, embed=True, small=True):
        for k in THIRDS:
            from_shard(rs_owner(me, k, f), k, lambda src, k=k: pltpu.make_async_copy(
                src, vout.at[slot_tiles(3, k, f)], own_sem.at[k, f]), embed, small)

    def send_first(f, embed=True, small=True):
        for k in THIRDS:
            for slot in THIRDS:
                dev = partner if slot == 2 else flip(me, ORDERS[k][0])
                if slot == 1:
                    dev = flip(dev, 1)
                from_shard(rs_owner(dev, k, f), k, lambda src, k=k, slot=slot, dev=dev: remote(
                    src, vout.at[slot_tiles(slot, k, f)], r1_send.at[slot, k, f], r1_recv.at[slot, k, f], dev),
                    embed, small)

    barrier = pltpu.get_barrier_semaphore()
    near = [flip(me, order[0]) for order in ORDERS]
    near += [flip(dev, 1) for dev in near] + [partner]
    for dev in near:
        pl.semaphore_signal(barrier, inc=1, device_id=(dev,), device_id_type=MESH)
    raw = [pltpu.make_async_copy(src, dst, raw_sem.at[i]) for i, (src, dst) in enumerate((
        (gg, wide_raw.at[0]), (gu, wide_raw.at[1]), (gq, q_raw), (gk, k_raw), (gv, v_raw), (gn, n_raw), (gqk, qk_raw)))]
    for copy in raw:
        copy.start()
    edge = EMBED_TILES - TAIL_START
    relayed = []
    start = SPARE
    for i, (src, first, tiles) in enumerate(((go, SMALL["out"][0], 48), (gd, SMALL["down"][0], 96),
                                             (emb.at[pl.ds(TAIL_START, edge)], TAIL_START, edge))):
        part = vout.at[pl.ds(start, tiles)]
        copy = pltpu.make_async_copy(src, part, relay_sem.at[i])
        copy.start()
        relayed.append((copy, pltpu.make_async_copy(part, tail.at[pl.ds(first - TAIL_START, tiles)], tail_sem.at[i])))
        start += tiles
    for f in PAIR:
        load_own(f, small=False)
    pl.semaphore_wait(barrier, len(near))
    for f in THIRDS:
        send_first(f, small=False)

    for copy, onward in relayed:
        copy.wait()
        onward.start()
    onwards = [onward for _, onward in relayed]

    raw_names = list(SMALL)

    def to_tail(src, name):
        first, tiles = SMALL[name]
        copy = pltpu.make_async_copy(src, tail.at[pl.ds(first - TAIL_START, tiles)], tail_sem.at[3 + raw_names.index(name)])
        copy.start()
        onwards.append(copy)

    spare = start
    for i, name in enumerate(("gate", "up")):
        raw[i].wait()
        pack_wide(wide_raw.at[i], vout, spare, grad, 96)
        to_tail(vout.at[pl.ds(spare, 96)], name)
        onwards.pop().wait()
    for i, (name, src, width) in enumerate((("q", q_raw, 64), ("k", k_raw, 16), ("v", v_raw, 16))):
        raw[2 + i].wait()
        pack_narrow(src, vout, spare, grad, width)
        tiles = SMALL[name][1]
        to_tail(vout.at[pl.ds(spare, tiles)], name)
        spare += tiles
    raw[5].wait()
    raw[6].wait()
    for i in THIRDS:
        n_tiles[i] = jnp.concatenate([n_raw[2 * i].astype(jnp.float32), n_raw[2 * i + 1].astype(jnp.float32)],
                                     axis=0).astype(jnp.bfloat16)
    grad[24:40, :] = jnp.zeros((16, LANES), jnp.float32)
    for layer in range(LAYERS):
        pair = qk_raw[layer].astype(jnp.float32)
        for i in PAIR:
            for half in PAIR:
                row = (2 * layer + i) * 2 + half
                grad[row:row + 1, :] = pair[i:i + 1, LANES * half:LANES * (half + 1)]
    put_tile(n_tiles, 3, grad, 0, COLS)
    to_tail(n_tiles.at[pl.ds(0, 3)], "norms")
    to_tail(n_tiles.at[pl.ds(3, 1)], "qk")
    for copy in onwards:
        copy.wait()
    for f in range(4):
        send_first(f, embed=f == 3)
        load_own(f, embed=f > 1)
    before = lax.rem(me + DEVS - 1, DEVS)
    ext_copies = [remote(src.at[pl.ds(0, TILE_ROWS)], ext.at[i], ext_send.at[i], ext_recv.at[i], before)
                  for i, src in enumerate((m_in, v_in, p_in))]
    for copy in state:
        copy.start()

    def r1_copy(slot, k, f):
        return remote(emb.at[pl.ds(0, RS_TILES)], vout.at[slot_tiles(slot, k, f)], r1_send.at[slot, k, f],
                      r1_recv.at[slot, k, f], partner)

    def r2_copy(k, f):
        return remote(s1.at[sum_rows(k, f)], r2.at[k, f], r2_send.at[k, f], r2_recv.at[k, f], flip(me, ORDERS[k][1]))

    def r3_copy(k, half):
        src = pl.ds(sum_rows(k, 2).start + half * HALF_ROWS, HALF_ROWS)
        dst = pl.ds(half * HALF_ROWS, HALF_ROWS)
        return remote(s1.at[src], r3.at[k, dst], r3_send.at[k, half], r3_recv.at[k, half], flip(me, ORDERS[k][2]))

    for f in range(4):
        for k in THIRDS:
            pltpu.make_async_copy(
                emb.at[pl.ds(0, RS_TILES)], vout.at[slot_tiles(3, k, f)], own_sem.at[k, f]).wait()
            for slot in (2, 0, 1):
                r1_copy(slot, k, f).wait_recv()

            def add_four(t, _, k=k, f=f):
                a, b, c, d = [vout[slot_tiles(slot, k, f).start + t].astype(jnp.float32) for slot in (3, 2, 0, 1)]
                total = (a + b) + (c + d)
                row = sum_rows(k, f).start + TILE_ROWS * t
                for j in range(COLS):
                    s1[pl.ds(pl.multiple_of(row + 8 * j, 8), 8), :] = total[:, LANES * j:LANES * (j + 1)]
                return 0

            lax.fori_loop(0, RS_TILES, add_four, 0, unroll=2)
            if f < 2:
                r2_copy(k, f).start()
    for f in PAIR:
        for k in THIRDS:
            r2_copy(k, f).wait_recv()

            def add_two(t, _, k=k, f=f):
                row = pl.multiple_of(TILE_ROWS * t, 8)
                at = pl.ds(pl.multiple_of(sum_rows(k, 2 + f).start + TILE_ROWS * t, 8), TILE_ROWS)
                s1[at, :] = s1[at, :] + r2[k, f, pl.ds(row, TILE_ROWS), :]
                return 0

            for half in PAIR:
                lax.fori_loop(half * HALF_TILES, (half + 1) * HALF_TILES, add_two, 0, unroll=2)
                if f == 0:
                    r3_copy(k, half).start()

    shift = LEAD - (SHARD_ROWS * me - TILE_ROWS * rs_start(me))
    for k in THIRDS:
        for f in PAIR:
            r2_copy(k, f).wait_send()
    def squares(i, acc):
        part = grad[pl.ds(pl.multiple_of(i * TILE_ROWS, 8), TILE_ROWS), :]
        return acc + part * part

    def finish(k, t, carry):
        row = pl.multiple_of(TILE_ROWS * t, 8)
        at = pl.ds(pl.multiple_of(sum_rows(k, 3).start + TILE_ROWS * t, 8), TILE_ROWS)
        total = (s1[at, :] + r3[k, pl.ds(row, TILE_ROWS), :]) * (1.0 / DEVS)
        row = shift + TILE_ROWS * (k * RS_TILES + t)
        for j in range(COLS):
            grad[pl.ds(row + j, 8, stride=COLS), :] = total[8 * j:8 * (j + 1), :]
        return carry

    acc = jnp.zeros((TILE_ROWS, LANES), jnp.float32)
    end = (LEAD + SHARD_ROWS) // TILE_ROWS
    for half in PAIR:
        for k in THIRDS:
            r3_copy(k, half).wait_recv()
            lax.fori_loop(half * HALF_TILES, (half + 1) * HALF_TILES, functools.partial(finish, k), 0, unroll=2)
        for k in THIRDS:
            first = k * RS_TILES + 1
            middle = first + HALF_TILES - 1
            blocks = (middle, min(first + RS_TILES, end)) if half else (first, middle)
            acc = lax.fori_loop(*blocks, squares, acc, unroll=3)
    for copy in ext_copies:
        copy.start()
    nsend[...] = acc[0:8] + acc[8:16] + acc[16:24] + acc[24:32] + acc[32:40]
    start = end * TILE_ROWS
    for row, rows in ((start, 8), (start + 8, 8), (start + 16, 8), (start + 24, 5)):
        part = grad[pl.ds(row, rows), :]
        nsend[0:rows, :] = nsend[0:rows, :] + part * part

    others = [flip_mask(me, (1, 2, 4, 8), mask) for mask in sorted(OTHERS, key=lambda mask: -(mask // 2).bit_count())]

    def n_copy(i, source):
        return remote(nsend, nrecv.at[source], n_send.at[i], n_recv.at[source], others[i])

    for i in range(len(others)):
        n_copy(i, me).start()

    for copy in state:
        copy.wait()

    def full(value):
        return jnp.full((8, LANES), value, jnp.float32)

    learn_rate, beta_one, beta_two, decay, max_norm = [full(hyp[i]) for i in range(5)]
    rest_one, rest_two = 1.0 - beta_one, 1.0 - beta_two
    hat_one = 1.0 / (1.0 - lax.integer_pow(beta_one, ADAM_STEP))
    hat_two = 1.0 / (1.0 - lax.integer_pow(beta_two, ADAM_STEP))
    for copy in ext_copies:
        copy.wait_recv()

    for i, dev in enumerate(others):
        n_copy(i, me).wait_send()
        n_copy(i, dev).wait_recv()
    nrecv[me] = nsend[...]
    total = nrecv[0]
    for j in OTHERS:
        total = total + nrecv[j]
    total = jnp.sum(jnp.sum(total, axis=1, keepdims=True), axis=0, keepdims=True)
    clip = jnp.minimum(1.0, max_norm / (jnp.sqrt(jnp.broadcast_to(total, (8, LANES))) + CLIP_EPS))

    def wide(value, rows):
        if rows <= 8:
            return value[:rows]
        return jnp.concatenate([value] * (rows // 8), axis=0)

    def adam(g, m, v, p, first_row, rows):
        clipped = g * wide(clip, rows)
        m = wide(beta_one, rows) * m + wide(rest_one, rows) * clipped
        v = wide(beta_two, rows) * v + wide(rest_two, rows) * (clipped * clipped)
        index = first_row + lax.broadcasted_iota(jnp.int32, (rows, LANES), 0)
        update = (m * wide(hat_one, rows)) / (jnp.sqrt(v * wide(hat_two, rows)) + ADAM_EPS)
        update = update + jnp.where(index < DECAY_ROWS, wide(decay, rows) * p, 0.0)
        return m, v, p - wide(learn_rate, rows) * update

    def adam_rows(row, rows):
        at = pl.ds(row, rows)
        shifted = pl.ds(row + LEAD, rows)
        m, v, p = adam(grad[shifted, :], mom[at, :], vel[at, :], par[at, :], SHARD_ROWS * me + row, rows)
        mom[at, :] = m
        vel[at, :] = v
        par[at, :] = p
        grad[shifted, :] = p

    def adam_block(i, _):
        adam_rows(pl.multiple_of(i * 40, 8), 40)
        return 0

    def ag_sizes(owner, k, run):
        if k < 2:
            run(AG_TILES)
            return
        longer = ag_start(owner + 1) - ag_start(owner) == 3 * AG_TILES + 1

        @pl.when(longer)
        def _():
            run(AG_TILES + 1)

        @pl.when(jnp.logical_not(longer))
        def _():
            run(AG_TILES)

    def ag_each(k, mask, run, dev=me):
        owner = flip_mask(dev, ORDERS[k], mask)
        first = ag_start(owner) + k * AG_TILES
        ag_sizes(owner, k, lambda size: run(vout.at[pl.ds(first, size)], size))

    def ag_link(k, mask, link, start=True):
        dev = flip(me, ORDERS[k][link])
        slot = mask + (1 << link)

        def copy(dst, size):
            return remote(dst, dst, ag_send.at[k, slot], ag_recv.at[k, slot], dev)

        if start:
            ag_each(k, mask, lambda dst, size: copy(dst, size).start())
        pending.append(lambda: ag_each(k, mask, lambda dst, size: copy(dst, size).wait_send()))

    def ag_part(k, mask, i, run):
        owner = flip_mask(me, ORDERS[k], mask)
        first = ag_start(owner) + k * AG_TILES + i * PART_TILES
        if i < LAST_PART:
            run(vout.at[pl.ds(first, PART_TILES)])
        else:
            ag_sizes(owner, k, lambda size: run(vout.at[pl.ds(first, size - LAST_PART * PART_TILES)]))

    def last_copy(k, i, part):
        return remote(part, part, ag_send.at[k, 7], last_recv.at[k, i], flip(me, ORDERS[k][2]))

    def across_copy(k, part):
        return remote(part, part, d2d_send.at[k, 7], d2d_recv.at[k, 7], partner)

    def ag_across(k, mask, start=True):
        def copy(dst, size):
            return remote(dst, dst, d2d_send.at[k, mask], d2d_recv.at[k, mask], partner)

        if start:
            ag_each(k, mask, lambda dst, size: copy(dst, size).start())
        pending.append(lambda: ag_each(k, mask, lambda dst, size: copy(dst, size).wait_send()))

    def ag_arrived(k, mask):
        ag_each(k, mask, lambda dst, size: remote(
            dst, dst, ag_send.at[k, mask], ag_recv.at[k, mask], partner).wait_recv())

    pending = []
    base = LEAD + TILE_ROWS * ag_start(me) - SHARD_ROWS * me

    def own_part(k, skip, count, blocks):
        lax.fori_loop(*blocks, adam_block, 0)
        if k == 2:
            adam_rows(6120, 24)
            adam_rows(6144, 5)
            at = pl.ds(LEAD + SHARD_ROWS, TILE_ROWS)
            _, _, p = adam(grad[at, :], ext[0], ext[1], ext[2], SHARD_ROWS * (me + 1), TILE_ROWS)
            grad[at, :] = p
        first = ag_start(me) + k * AG_TILES

        def pack(t, _):
            put_tile(vout, first + t, grad, base + TILE_ROWS * (k * AG_TILES + t), COLS)
            return 0

        lax.fori_loop(skip, skip + (ag_start(me + 1) - first if k == 2 else count), pack, 0)

        def send(size):
            part = vout.at[pl.ds(first + skip, size)]
            for link in THIRDS:
                slot = 1 << link
                remote(part, part, ag_send.at[k, slot], ag_recv.at[k, slot], flip(me, ORDERS[k][link])).start()
            remote(part, part, d2d_send.at[k, 0], d2d_recv.at[k, 0], partner).start()

        if k == 2:
            ag_sizes(me, k, send)
        else:
            send(count)

    own_part(0, 0, 7, (0, 8))
    own_part(0, 7, 14, (8, 22))
    own_part(0, 21, 30, (22, 52))
    own_part(1, 0, AG_TILES, (52, 103))
    own_part(2, 0, None, (103, 153))
    for k in THIRDS:
        for link in THIRDS:
            ag_link(k, 0, link, start=False)
        ag_across(k, 0, start=False)
    for k in THIRDS:
        ag_arrived(k, 1)
        ag_link(k, 1, 1)
        ag_across(k, 1)
    for k in THIRDS:
        ag_link(k, 1, 2)
    for k in THIRDS:
        ag_arrived(k, 2)
        ag_link(k, 2, 2)
        ag_across(k, 2)
    for k in THIRDS:
        ag_arrived(k, 4)
        ag_across(k, 4)
    for k in THIRDS:
        ag_arrived(k, 3)
        for i in range(LAST_PART + 1):
            ag_part(k, 3, i, lambda part, k=k, i=i: last_copy(k, i, part).start())
        ag_link(k, 3, 2, start=False)
        ag_across(k, 3)
    for mask in (5, 6):
        for k in THIRDS:
            ag_arrived(k, mask)
            ag_across(k, mask)
    for i in range(LAST_PART + 1):
        for k in THIRDS:
            ag_part(k, 7, i, lambda part, k=k, i=i: last_copy(k, i, part).wait_recv())
            ag_part(k, 7, i, lambda part, k=k, i=i: across_copy(k, part).start())
    for k in THIRDS:
        ag_across(k, 7, start=False)
    for mask in range(8):
        for k in THIRDS:
            ag_each(k, mask, lambda dst, size, k=k, mask=mask: remote(
                dst, dst, d2d_send.at[k, mask], d2d_recv.at[k, mask], partner).wait_recv(), partner)
    for wait in pending:
        wait()
    for copy in ext_copies:
        copy.wait_send()
    for f in range(4):
        for k in THIRDS:
            for slot in THIRDS:
                r1_copy(slot, k, f).wait_send()
    for k in THIRDS:
        for half in PAIR:
            r3_copy(k, half).wait_send()


def flush(mom, vel, par, vout, embed, oq, ok, ov, oo, og, ou, od, on, oqk, m_out, v_out, p_out,
          rows, wide_out, q_out, k_out, v_new, n_out, qk_out, sem):
    copies = []

    def send(src, dst):
        copy = pltpu.make_async_copy(src, dst, sem.at[len(copies)])
        copy.start()
        copies.append(copy)

    for i in range(FLUSH_PARTS):
        part = pl.ds(i * (EMBED_TILES // FLUSH_PARTS), EMBED_TILES // FLUSH_PARTS)
        send(vout.at[part], embed.at[part])
    for src, dst in ((mom, m_out), (vel, v_out), (par, p_out)):
        send(src, dst)
    for name, dst in (("out", oo), ("down", od)):
        send(vout.at[pl.ds(*SMALL[name])], dst)
    for i, (name, dst) in enumerate((("gate", og), ("up", ou))):
        unpack_wide(vout, SMALL[name][0], wide_out.at[i], rows, 96)
        send(wide_out.at[i], dst)
    for name, block, dst, width in (("q", q_out, oq, 64), ("k", k_out, ok, 16), ("v", v_new, ov, 16)):
        unpack_narrow(vout, SMALL[name][0], block, rows, width)
        send(block, dst)
    for i in THIRDS:
        tile = vout[SMALL["norms"][0] + i].astype(jnp.float32)
        n_out[2 * i] = tile[0:4].astype(jnp.bfloat16)
        n_out[2 * i + 1] = tile[4:8].astype(jnp.bfloat16)
    send(n_out, on)
    for j in range(COLS):
        rows[pl.ds(j, 8, stride=COLS), :] = vout[SMALL["qk"][0], :, LANES * j:LANES * (j + 1)].astype(jnp.float32)
    for layer in range(LAYERS):
        four = rows[4 * layer:4 * layer + 4, :]
        pair = [jnp.concatenate([four[2 * i:2 * i + 1], four[2 * i + 1:2 * i + 2]], axis=1) for i in PAIR]
        qk_out[layer] = jnp.concatenate(pair, axis=0).astype(jnp.bfloat16)
    send(qk_out, oqk)
    for copy in copies:
        copy.wait()


def solution(mesh):
    def local_update(*arrays):
        grads = [arr.reshape(arr.shape[1:]) for arr in arrays[:GRAD_COUNT]]
        state = [arr.reshape(SHARD_ROWS, LANES) for arr in arrays[GRAD_COUNT:GRAD_COUNT + 3]]
        shapes = [grad_arr.shape for grad_arr in grads]
        any_spec = pl.BlockSpec(memory_space=pl.ANY)
        vmem_spec = pl.BlockSpec(memory_space=pltpu.VMEM)
        dma = pltpu.SemaphoreType.DMA
        bf16, f32 = jnp.bfloat16, jnp.float32
        tiled = []
        for i, grad_arr in enumerate(grads[:8]):
            if i in (1, 2, 3):
                grad_arr = jnp.swapaxes(grad_arr, 1, 2)
            tiled.append(grad_arr.reshape(-1, LANES) if i in (5, 6) else grad_arr.reshape(-1, 8, WIDTH))
        tiled += grads[8:]
        small = [jax.ShapeDtypeStruct(arr.shape, bf16) for arr in tiled[1:]]
        *kept, _ = pl.pallas_call(
            kernel,
            out_shape=[pltpu.VMEM((SHARD_ROWS, LANES), f32)] * 3
            + [pltpu.VMEM((OUT_TILES, 8, WIDTH), bf16)]
            + [pltpu.HBM((TAIL_TILES, 8, WIDTH), bf16)],
            in_specs=[any_spec] * 14,
            out_specs=[vmem_spec] * 4 + [any_spec],
            scratch_shapes=[
                pltpu.VMEM((3 * 4 * PIECE_ROWS, LANES), f32),
                pltpu.VMEM((3, 2, PIECE_ROWS, LANES), f32),
                pltpu.VMEM((3, PIECE_ROWS, LANES), f32),
                pltpu.VMEM((3, TILE_ROWS, LANES), f32),
                pltpu.SMEM((5,), f32),
                pltpu.VMEM((8, LANES), f32),
                pltpu.VMEM((DEVS, 8, LANES), f32),
                pltpu.VMEM((2, 3840, LANES), bf16),
                pltpu.VMEM((48, 8, WIDTH), bf16),
                pltpu.VMEM((12, 8, WIDTH), bf16),
                pltpu.VMEM((12, 8, WIDTH), bf16),
                pltpu.VMEM(shapes[8], bf16),
                pltpu.VMEM(shapes[9], bf16),
                pltpu.VMEM((4, 8, WIDTH), bf16),
                dma((7,)), dma((3,)), dma((3 + len(SMALL),)),
                dma((3, 4)), dma((3, 3, 4)), dma((3, 3, 4)), dma((3, 2)), dma((3, 2)), dma((3, 2)), dma((3, 2)),
                dma((4,)), dma((3,)), dma((3,)), dma((DEVS,)), dma((DEVS,)),
                dma((3, 8)), dma((3, 8)), dma((3, 8)), dma((3, 8)), dma((3, LAST_PART + 1)),
            ],
            compiler_params=pltpu.CompilerParams(
                collective_id=0, has_side_effects=True, vmem_limit_bytes=26_500_000),
        )(*tiled, *state, arrays[GRAD_COUNT + 3])
        kept = [pltpu.with_memory_space_constraint(arr, pltpu.VMEM) for arr in kept]
        outs = pl.pallas_call(
            flush,
            out_shape=[jax.ShapeDtypeStruct((EMBED_TILES, 8, WIDTH), bf16)] + small
            + [jax.ShapeDtypeStruct((SHARD_ROWS, LANES), f32)] * 3,
            in_specs=[vmem_spec] * 4,
            out_specs=[any_spec] * 13,
            scratch_shapes=[
                pltpu.VMEM((3840, LANES), f32),
                pltpu.VMEM((2, 3840, LANES), bf16),
                pltpu.VMEM((48, 8, WIDTH), bf16),
                pltpu.VMEM((12, 8, WIDTH), bf16),
                pltpu.VMEM((12, 8, WIDTH), bf16),
                pltpu.VMEM(shapes[8], bf16),
                pltpu.VMEM(shapes[9], bf16),
                dma((FLUSH_PARTS + 16,)),
            ],
            compiler_params=pltpu.CompilerParams(has_side_effects=True, vmem_limit_bytes=5_200_000),
        )(*kept)
        params = []
        for i, dims in enumerate(shapes):
            if i in (1, 2, 3):
                params.append(jnp.swapaxes(outs[i].reshape(dims[0], dims[2], dims[1]), 1, 2))
            else:
                params.append(outs[i].reshape(dims))
        return tuple(params) + tuple(arr.reshape(-1) for arr in outs[GRAD_COUNT:])

    in_specs = tuple([P("dp")] * GRAD_COUNT + [P("dp"), P("dp"), P("dp"), P()])
    out_specs = tuple([P()] * GRAD_COUNT + [P("dp"), P("dp"), P("dp")])
    return jax.shard_map(local_update, mesh=mesh, in_specs=in_specs, out_specs=out_specs, check_vma=False)
```

```python
import functools
import math
import jax
import jax.numpy as jnp
from jax import lax
from jax.experimental import pallas as pl
from jax.experimental.pallas import tpu as pltpu
from jax.sharding import PartitionSpec as P

ADAM_STEP = 7
ADAM_EPS = 1e-8
CLIP_EPS = 1e-6
GRAD_COUNT = 10
MESH = pl.DeviceIdType.MESH

DEVS = 16
OTHERS = range(1, DEVS)
THIRDS = range(3)
PAIR = range(2)
LANES = 128
WIDTH = 640
SHARD_ROWS = 6149
TILE_ROWS = 40
EMBED_TILES = 2048
ALL_TILES = 2460
DECAY_ROWS = 98240
FIRST_TAIL = 13
TAIL_START = (SHARD_ROWS * FIRST_TAIL) // TILE_ROWS
RS_TILES = 52
TAIL_TILES = (SHARD_ROWS * 15) // TILE_ROWS + 3 * RS_TILES - TAIL_START
AG_TILES = 51
PART_TILES = 15
LAST_PART = 3
FLUSH_PARTS = 4
LEAD = 40
G_ROWS = LEAD + 3 * RS_TILES * TILE_ROWS
ORDERS = ((2, 4, 8), (4, 8, 2), (8, 2, 4))


def flip(dev, stride):
    return dev + stride - 2 * stride * lax.rem(dev // stride, 2)


def rs_start(dev):
    return (SHARD_ROWS * dev) // TILE_ROWS


def ag_start(dev):
    return (SHARD_ROWS * dev + TILE_ROWS - 1) // TILE_ROWS


def flip_mask(dev, order, mask):
    for bit, stride in enumerate(order):
        if mask >> bit & 1:
            dev = flip(dev, stride)
    return dev


SMALL = {}
for _name, _tiles in (("q", 48), ("k", 12), ("v", 12), ("out", 48), ("gate", 96), ("up", 96),
                      ("down", 96), ("norms", 3), ("qk", 1)):
    SMALL[_name] = (EMBED_TILES if not SMALL else sum(SMALL[_last]), _tiles)
    _last = _name
LAYERS = 6
COLS = WIDTH // LANES
OUT_TILES = 48 * RS_TILES
SPARE = 42 * RS_TILES
PIECE_ROWS = RS_TILES * TILE_ROWS
HALF_TILES = RS_TILES // 2
HALF_ROWS = PIECE_ROWS // 2


def slot_tiles(slot, k, f):
    index = 36 + f * 3 + k if slot == 3 else (slot * 3 + k) * 4 + f
    return pl.ds(index * RS_TILES, RS_TILES)


def sum_rows(k, f):
    return pl.ds((f * 3 + k) * PIECE_ROWS, PIECE_ROWS)


def put_tile(dst, tile, rows, first, stride):
    for j in range(COLS):
        dst[tile, :, LANES * j:LANES * (j + 1)] = rows[pl.ds(first + j, 8, stride=stride), :].astype(jnp.bfloat16)


def pack_wide(src, dst, first_tile, rows, tiles):
    def step(i, _):
        rows[pl.ds(pl.multiple_of(i * 80, 16), 80), :] = src[pl.ds(pl.multiple_of(i * 80, 16), 80), :].astype(jnp.float32)
        for half in PAIR:
            put_tile(dst, first_tile + 2 * i + half, rows, i * 80 + half * 40, COLS)
        return 0

    lax.fori_loop(0, tiles // 2, step, 0)


def pack_narrow(src, dst, first_tile, rows, width):
    folds = LANES // width
    lane = lax.broadcasted_iota(jnp.int32, (8, LANES), 1) // width
    for layer in range(LAYERS):
        block = src[pl.ds(layer * width // 8, width // 8)].astype(jnp.float32).reshape(width, WIDTH)
        rows[pl.ds(layer * WIDTH, WIDTH), :] = jnp.concatenate([block] * folds, axis=0).T
    tiles = LAYERS * width // 8

    def step(t, _):
        for j in range(COLS):
            first = folds * (40 * t + j)
            value = rows[pl.ds(first, 8, stride=folds * COLS), :]
            for fold in range(1, folds):
                value = jnp.where(lane == fold, rows[pl.ds(first + fold, 8, stride=folds * COLS), :], value)
            dst[first_tile + t, :, LANES * j:LANES * (j + 1)] = value.astype(jnp.bfloat16)
        return 0

    lax.fori_loop(0, tiles, step, 0)


def unpack_wide(src, first_tile, dst, rows, tiles):
    def step(i, _):
        for half in PAIR:
            for j in range(COLS):
                rows[pl.ds(i * 80 + half * 40 + j, 8, stride=COLS), :] = src[
                    first_tile + 2 * i + half, :, LANES * j:LANES * (j + 1)].astype(jnp.float32)
        dst[pl.ds(pl.multiple_of(i * 80, 16), 80), :] = rows[pl.ds(pl.multiple_of(i * 80, 16), 80), :].astype(jnp.bfloat16)
        return 0

    lax.fori_loop(0, tiles // 2, step, 0)


def unpack_narrow(src, first_tile, dst, rows, width):
    folds = LANES // width
    tiles = LAYERS * width // 8

    def step(t, _):
        for j in range(COLS):
            value = src[first_tile + t, :, LANES * j:LANES * (j + 1)].astype(jnp.float32)
            for fold in range(folds):
                turned = value if fold == 0 else pltpu.roll(value, LANES - fold * width, 1)
                rows[pl.ds(folds * (40 * t + j) + fold, 8, stride=folds * COLS), :] = turned
        return 0

    lax.fori_loop(0, tiles, step, 0)
    for layer in range(LAYERS):
        block = rows[pl.ds(layer * WIDTH, WIDTH), :].T[:width]
        dst[pl.ds(layer * width // 8, width // 8)] = block.reshape(width // 8, 8, WIDTH).astype(jnp.bfloat16)


def kernel(emb, gq, gk, gv, go, gg, gu, gd, gn, gqk, m_in, v_in, p_in, hyp_in, mom, vel, par, vout, tail,
           s1, r2, r3, ext, hyp, ahead, nsend, nrecv, wide_raw, q_raw, k_raw, v_raw, n_raw, qk_raw, n_tiles,
           raw_sem, relay_sem, tail_sem,
           own_sem, r1_send, r1_recv, r2_send, r2_recv, r3_send, r3_recv, st_sem,
           ext_send, ext_recv, n_send, n_recv, ag_send, ag_recv, d2d_send, d2d_recv, last_recv, ahead_sem):
    grad = s1.at[pl.ds(0, G_ROWS)]
    me = lax.axis_index("dp")
    partner = flip(me, 1)

    def remote(src, dst, ssem, rsem, dev):
        return pltpu.make_async_remote_copy(
            src_ref=src, dst_ref=dst, send_sem=ssem, recv_sem=rsem, device_id=(dev,), device_id_type=MESH)

    def from_shard(owner, k, make, embed=True, small=True, act=lambda copy: copy.start()):
        first = rs_start(owner) + k * RS_TILES

        if embed:
            @pl.when(owner < FIRST_TAIL)
            def _():
                act(make(emb.at[pl.ds(first, RS_TILES)]))

        if small:
            @pl.when(owner >= FIRST_TAIL)
            def _():
                act(make(tail.at[pl.ds(first - TAIL_START, RS_TILES)]))

    def rs_owner(dev, k, f):
        return flip_mask(dev, ORDERS[k], (0 if f >= 2 else 2) + (4 if f % 2 == 0 else 0))

    state = [pltpu.make_async_copy(src, dst, st_sem.at[i])
             for i, (src, dst) in enumerate(((m_in, mom), (v_in, vel), (p_in, par), (hyp_in, hyp)))]

    def load_own(f, embed=True, small=True):
        for k in THIRDS:
            from_shard(rs_owner(me, k, f), k, lambda src, k=k: pltpu.make_async_copy(
                src, vout.at[slot_tiles(3, k, f)], own_sem.at[k, f]), embed, small)

    def first_owner(slot, k, f):
        dev = partner if slot == 2 else flip(me, ORDERS[k][0])
        if slot == 1:
            dev = flip(dev, 1)
        return dev, rs_owner(dev, k, f)

    def send_first(f, embed=True, small=True):
        for slot in THIRDS:
            for k in THIRDS:
                dev, owner = first_owner(slot, k, f)

                def make(src, k=k, slot=slot, dev=dev):
                    src = ahead.at[k] if embed and not small and f + slot == 0 else src
                    return remote(src, vout.at[slot_tiles(slot, k, f)], r1_send.at[slot, k, f],
                                  r1_recv.at[slot, k, f], dev)

                from_shard(owner, k, make, embed, small)

    def load_ahead(act):
        for k in THIRDS:
            from_shard(first_owner(0, k, 0)[1], k, lambda src, k=k: pltpu.make_async_copy(
                src, ahead.at[k], ahead_sem.at[k]), small=False, act=act)

    barrier = pltpu.get_barrier_semaphore()
    near = [flip(me, order[0]) for order in ORDERS]
    near += [flip(dev, 1) for dev in near] + [partner]
    for dev in near:
        pl.semaphore_signal(barrier, inc=1, device_id=(dev,), device_id_type=MESH)
    load_ahead(lambda copy: copy.start())
    raw = [pltpu.make_async_copy(src, dst, raw_sem.at[i]) for i, (src, dst) in enumerate((
        (gg, wide_raw.at[0]), (gu, wide_raw.at[1]), (gq, q_raw), (gk, k_raw), (gv, v_raw), (gn, n_raw), (gqk, qk_raw)))]
    for copy in raw:
        copy.start()
    edge = EMBED_TILES - TAIL_START
    relayed = []
    start = SPARE
    for i, (src, first, tiles) in enumerate(((go, SMALL["out"][0], 48), (gd, SMALL["down"][0], 96),
                                             (emb.at[pl.ds(TAIL_START, edge)], TAIL_START, edge))):
        part = vout.at[pl.ds(start, tiles)]
        copy = pltpu.make_async_copy(src, part, relay_sem.at[i])
        copy.start()
        relayed.append((copy, pltpu.make_async_copy(part, tail.at[pl.ds(first - TAIL_START, tiles)], tail_sem.at[i])))
        start += tiles
    for f in PAIR:
        load_own(f, small=False)
    load_ahead(lambda copy: copy.wait())
    pl.semaphore_wait(barrier, len(near))
    for f in THIRDS:
        send_first(f, small=False)

    for copy, onward in relayed:
        copy.wait()
        onward.start()
    onwards = [onward for _, onward in relayed]

    raw_names = list(SMALL)

    def to_tail(src, name):
        first, tiles = SMALL[name]
        copy = pltpu.make_async_copy(src, tail.at[pl.ds(first - TAIL_START, tiles)], tail_sem.at[3 + raw_names.index(name)])
        copy.start()
        onwards.append(copy)

    spare = start
    for i, name in enumerate(("gate", "up")):
        raw[i].wait()
        pack_wide(wide_raw.at[i], vout, spare, grad, 96)
        to_tail(vout.at[pl.ds(spare, 96)], name)
        onwards.pop().wait()
    for i, (name, src, width) in enumerate((("q", q_raw, 64), ("k", k_raw, 16), ("v", v_raw, 16))):
        raw[2 + i].wait()
        pack_narrow(src, vout, spare, grad, width)
        tiles = SMALL[name][1]
        to_tail(vout.at[pl.ds(spare, tiles)], name)
        spare += tiles
    raw[5].wait()
    raw[6].wait()
    for i in THIRDS:
        n_tiles[i] = jnp.concatenate([n_raw[2 * i].astype(jnp.float32), n_raw[2 * i + 1].astype(jnp.float32)],
                                     axis=0).astype(jnp.bfloat16)
    grad[24:40, :] = jnp.zeros((16, LANES), jnp.float32)
    for layer in range(LAYERS):
        pair = qk_raw[layer].astype(jnp.float32)
        for i in PAIR:
            for half in PAIR:
                row = (2 * layer + i) * 2 + half
                grad[row:row + 1, :] = pair[i:i + 1, LANES * half:LANES * (half + 1)]
    put_tile(n_tiles, 3, grad, 0, COLS)
    to_tail(n_tiles.at[pl.ds(0, 3)], "norms")
    to_tail(n_tiles.at[pl.ds(3, 1)], "qk")
    for copy in onwards:
        copy.wait()
    for f in range(4):
        send_first(f, embed=f == 3)
        load_own(f, embed=f > 1)
    before = lax.rem(me + DEVS - 1, DEVS)
    ext_copies = [remote(src.at[pl.ds(0, TILE_ROWS)], ext.at[i], ext_send.at[i], ext_recv.at[i], before)
                  for i, src in enumerate((m_in, v_in, p_in))]
    for copy in state:
        copy.start()

    def r1_copy(slot, k, f):
        return remote(emb.at[pl.ds(0, RS_TILES)], vout.at[slot_tiles(slot, k, f)], r1_send.at[slot, k, f],
                      r1_recv.at[slot, k, f], partner)

    def r2_copy(k, f):
        return remote(s1.at[sum_rows(k, f)], r2.at[k, f], r2_send.at[k, f], r2_recv.at[k, f], flip(me, ORDERS[k][1]))

    def r3_copy(k, half):
        src = pl.ds(sum_rows(k, 2).start + half * HALF_ROWS, HALF_ROWS)
        dst = pl.ds(half * HALF_ROWS, HALF_ROWS)
        return remote(s1.at[src], r3.at[k, dst], r3_send.at[k, half], r3_recv.at[k, half], flip(me, ORDERS[k][2]))

    for f in range(4):
        for k in THIRDS:
            pltpu.make_async_copy(
                emb.at[pl.ds(0, RS_TILES)], vout.at[slot_tiles(3, k, f)], own_sem.at[k, f]).wait()
            for slot in (2, 0, 1):
                r1_copy(slot, k, f).wait_recv()

            def add_four(t, _, k=k, f=f):
                a, b, c, d = [vout[slot_tiles(slot, k, f).start + t].astype(jnp.float32) for slot in (3, 2, 0, 1)]
                total = (a + b) + (c + d)
                row = sum_rows(k, f).start + TILE_ROWS * t
                for j in range(COLS):
                    s1[pl.ds(pl.multiple_of(row + 8 * j, 8), 8), :] = total[:, LANES * j:LANES * (j + 1)]
                return 0

            lax.fori_loop(0, RS_TILES, add_four, 0, unroll=2)
            if f < 2:
                r2_copy(k, f).start()
    for f in PAIR:
        for k in THIRDS:
            r2_copy(k, f).wait_recv()

            def add_two(t, _, k=k, f=f):
                row = pl.multiple_of(TILE_ROWS * t, 8)
                at = pl.ds(pl.multiple_of(sum_rows(k, 2 + f).start + TILE_ROWS * t, 8), TILE_ROWS)
                s1[at, :] = s1[at, :] + r2[k, f, pl.ds(row, TILE_ROWS), :]
                return 0

            for half in PAIR:
                lax.fori_loop(half * HALF_TILES, (half + 1) * HALF_TILES, add_two, 0, unroll=2)
                if f == 0:
                    r3_copy(k, half).start()

    shift = LEAD - (SHARD_ROWS * me - TILE_ROWS * rs_start(me))
    for k in THIRDS:
        for f in PAIR:
            r2_copy(k, f).wait_send()
    def squares(i, acc):
        part = grad[pl.ds(pl.multiple_of(i * TILE_ROWS, 8), TILE_ROWS), :]
        return acc + part * part

    def finish(k, t, carry):
        row = pl.multiple_of(TILE_ROWS * t, 8)
        at = pl.ds(pl.multiple_of(sum_rows(k, 3).start + TILE_ROWS * t, 8), TILE_ROWS)
        total = (s1[at, :] + r3[k, pl.ds(row, TILE_ROWS), :]) * (1.0 / DEVS)
        row = shift + TILE_ROWS * (k * RS_TILES + t)
        for j in range(COLS):
            grad[pl.ds(row + j, 8, stride=COLS), :] = total[8 * j:8 * (j + 1), :]
        return carry

    acc = jnp.zeros((TILE_ROWS, LANES), jnp.float32)
    end = (LEAD + SHARD_ROWS) // TILE_ROWS
    for half in PAIR:
        for k in THIRDS:
            r3_copy(k, half).wait_recv()
            lax.fori_loop(half * HALF_TILES, (half + 1) * HALF_TILES, functools.partial(finish, k), 0, unroll=2)
        for k in THIRDS:
            first = k * RS_TILES + 1
            middle = first + HALF_TILES - 1
            blocks = (middle, min(first + RS_TILES, end)) if half else (first, middle)
            acc = lax.fori_loop(*blocks, squares, acc, unroll=3)
    for copy in ext_copies:
        copy.start()
    nsend[...] = acc[0:8] + acc[8:16] + acc[16:24] + acc[24:32] + acc[32:40]
    start = end * TILE_ROWS
    for row, rows in ((start, 8), (start + 8, 8), (start + 16, 8), (start + 24, 5)):
        part = grad[pl.ds(row, rows), :]
        nsend[0:rows, :] = nsend[0:rows, :] + part * part

    others = [flip_mask(me, (1, 2, 4, 8), mask) for mask in sorted(OTHERS, key=lambda mask: -(mask // 2).bit_count())]

    def n_copy(i, source):
        return remote(nsend, nrecv.at[source], n_send.at[i], n_recv.at[source], others[i])

    for i in range(len(others)):
        n_copy(i, me).start()

    for copy in state:
        copy.wait()

    def full(value):
        return jnp.full((8, LANES), value, jnp.float32)

    learn_rate, beta_one, beta_two, decay, max_norm = [full(hyp[i]) for i in range(5)]
    rest_one, rest_two = 1.0 - beta_one, 1.0 - beta_two
    hat_one = 1.0 / (1.0 - lax.integer_pow(beta_one, ADAM_STEP))
    hat_two = 1.0 / (1.0 - lax.integer_pow(beta_two, ADAM_STEP))
    for copy in ext_copies:
        copy.wait_recv()

    for i, dev in enumerate(others):
        n_copy(i, me).wait_send()
        n_copy(i, dev).wait_recv()
    nrecv[me] = nsend[...]
    total = nrecv[0]
    for j in OTHERS:
        total = total + nrecv[j]
    total = jnp.sum(jnp.sum(total, axis=1, keepdims=True), axis=0, keepdims=True)
    clip = jnp.minimum(1.0, max_norm / (jnp.sqrt(jnp.broadcast_to(total, (8, LANES))) + CLIP_EPS))

    def wide(value, rows):
        if rows <= 8:
            return value[:rows]
        return jnp.concatenate([value] * (rows // 8), axis=0)

    def adam(g, m, v, p, first_row, rows):
        clipped = g * wide(clip, rows)
        m = wide(beta_one, rows) * m + wide(rest_one, rows) * clipped
        v = wide(beta_two, rows) * v + wide(rest_two, rows) * (clipped * clipped)
        index = first_row + lax.broadcasted_iota(jnp.int32, (rows, LANES), 0)
        update = (m * wide(hat_one, rows)) / (jnp.sqrt(v * wide(hat_two, rows)) + ADAM_EPS)
        update = update + jnp.where(index < DECAY_ROWS, wide(decay, rows) * p, 0.0)
        return m, v, p - wide(learn_rate, rows) * update

    def adam_rows(row, rows):
        at = pl.ds(row, rows)
        shifted = pl.ds(row + LEAD, rows)
        m, v, p = adam(grad[shifted, :], mom[at, :], vel[at, :], par[at, :], SHARD_ROWS * me + row, rows)
        mom[at, :] = m
        vel[at, :] = v
        par[at, :] = p
        grad[shifted, :] = p

    def adam_block(i, _):
        adam_rows(pl.multiple_of(i * 40, 8), 40)
        return 0

    def ag_sizes(owner, k, run):
        if k < 2:
            run(AG_TILES)
            return
        longer = ag_start(owner + 1) - ag_start(owner) == 3 * AG_TILES + 1

        @pl.when(longer)
        def _():
            run(AG_TILES + 1)

        @pl.when(jnp.logical_not(longer))
        def _():
            run(AG_TILES)

    def ag_each(k, mask, run, dev=me):
        owner = flip_mask(dev, ORDERS[k], mask)
        first = ag_start(owner) + k * AG_TILES
        ag_sizes(owner, k, lambda size: run(vout.at[pl.ds(first, size)], size))

    def ag_link(k, mask, link, start=True):
        dev = flip(me, ORDERS[k][link])
        slot = mask + (1 << link)

        def copy(dst, size):
            return remote(dst, dst, ag_send.at[k, slot], ag_recv.at[k, slot], dev)

        if start:
            ag_each(k, mask, lambda dst, size: copy(dst, size).start())
        pending.append(lambda: ag_each(k, mask, lambda dst, size: copy(dst, size).wait_send()))

    def ag_part(k, mask, i, run):
        owner = flip_mask(me, ORDERS[k], mask)
        first = ag_start(owner) + k * AG_TILES + i * PART_TILES
        if i < LAST_PART:
            run(vout.at[pl.ds(first, PART_TILES)])
        else:
            ag_sizes(owner, k, lambda size: run(vout.at[pl.ds(first, size - LAST_PART * PART_TILES)]))

    def last_copy(k, i, part):
        return remote(part, part, ag_send.at[k, 7], last_recv.at[k, i], flip(me, ORDERS[k][2]))

    def across_copy(k, part):
        return remote(part, part, d2d_send.at[k, 7], d2d_recv.at[k, 7], partner)

    def ag_across(k, mask, start=True):
        def copy(dst, size):
            return remote(dst, dst, d2d_send.at[k, mask], d2d_recv.at[k, mask], partner)

        if start:
            ag_each(k, mask, lambda dst, size: copy(dst, size).start())
        pending.append(lambda: ag_each(k, mask, lambda dst, size: copy(dst, size).wait_send()))

    def ag_arrived(k, mask):
        ag_each(k, mask, lambda dst, size: remote(
            dst, dst, ag_send.at[k, mask], ag_recv.at[k, mask], partner).wait_recv())

    pending = []
    base = LEAD + TILE_ROWS * ag_start(me) - SHARD_ROWS * me

    def own_part(k, skip, count, blocks):
        lax.fori_loop(*blocks, adam_block, 0)
        if k == 2:
            adam_rows(6120, 24)
            adam_rows(6144, 5)
            at = pl.ds(LEAD + SHARD_ROWS, TILE_ROWS)
            _, _, p = adam(grad[at, :], ext[0], ext[1], ext[2], SHARD_ROWS * (me + 1), TILE_ROWS)
            grad[at, :] = p
        first = ag_start(me) + k * AG_TILES

        def pack(t, _):
            put_tile(vout, first + t, grad, base + TILE_ROWS * (k * AG_TILES + t), COLS)
            return 0

        lax.fori_loop(skip, skip + (ag_start(me + 1) - first if k == 2 else count), pack, 0)

        def send(size):
            part = vout.at[pl.ds(first + skip, size)]
            for link in THIRDS:
                slot = 1 << link
                remote(part, part, ag_send.at[k, slot], ag_recv.at[k, slot], flip(me, ORDERS[k][link])).start()
            remote(part, part, d2d_send.at[k, 0], d2d_recv.at[k, 0], partner).start()

        if k == 2:
            ag_sizes(me, k, send)
        else:
            send(count)

    own_part(0, 0, 7, (0, 8))
    own_part(0, 7, 14, (8, 22))
    own_part(0, 21, 30, (22, 52))
    own_part(1, 0, AG_TILES, (52, 103))
    own_part(2, 0, None, (103, 153))
    for k in THIRDS:
        for link in THIRDS:
            ag_link(k, 0, link, start=False)
        ag_across(k, 0, start=False)
    for k in THIRDS:
        ag_arrived(k, 1)
        ag_link(k, 1, 1)
        ag_across(k, 1)
    for k in THIRDS:
        ag_link(k, 1, 2)
    for k in THIRDS:
        ag_arrived(k, 2)
        ag_link(k, 2, 2)
        ag_across(k, 2)
    for copy in ext_copies:
        copy.wait_send()
    for f in range(4):
        for k in THIRDS:
            for slot in THIRDS:
                r1_copy(slot, k, f).wait_send()
    for k in THIRDS:
        for half in PAIR:
            r3_copy(k, half).wait_send()
    for k in THIRDS:
        ag_arrived(k, 4)
        ag_across(k, 4)
    for k in THIRDS:
        ag_arrived(k, 3)
        for i in range(LAST_PART + 1):
            ag_part(k, 3, i, lambda part, k=k, i=i: last_copy(k, i, part).start())
        ag_across(k, 3)
    for mask in (5, 6):
        for k in THIRDS:
            ag_arrived(k, mask)
            ag_across(k, mask)
    def from_partner(masks):
        for mask in masks:
            for k in THIRDS:
                ag_each(k, mask, lambda dst, size, k=k, mask=mask: remote(
                    dst, dst, d2d_send.at[k, mask], d2d_recv.at[k, mask], partner).wait_recv(), partner)

    from_partner(range(5))
    for wait in pending:
        wait()
    pending.clear()
    for i in range(LAST_PART + 1):
        for k in THIRDS:
            ag_part(k, 7, i, lambda part, k=k, i=i: last_copy(k, i, part).wait_recv())
            ag_part(k, 7, i, lambda part, k=k, i=i: across_copy(k, part).start())
    for k in THIRDS:
        ag_link(k, 3, 2, start=False)
        ag_across(k, 7, start=False)
    from_partner(range(5, 8))
    for wait in pending:
        wait()


def flush(mom, vel, par, vout, embed, oq, ok, ov, oo, og, ou, od, on, oqk, m_out, v_out, p_out,
          rows, wide_out, q_out, k_out, v_new, n_out, qk_out, sem):
    copies = []

    def send(src, dst):
        copy = pltpu.make_async_copy(src, dst, sem.at[len(copies)])
        copy.start()
        copies.append(copy)

    for i in range(FLUSH_PARTS):
        part = pl.ds(i * (EMBED_TILES // FLUSH_PARTS), EMBED_TILES // FLUSH_PARTS)
        send(vout.at[part], embed.at[part])
    for src, dst in ((mom, m_out), (vel, v_out), (par, p_out)):
        send(src, dst)
    for name, dst in (("out", oo), ("down", od)):
        send(vout.at[pl.ds(*SMALL[name])], dst)
    for i, (name, dst) in enumerate((("gate", og), ("up", ou))):
        unpack_wide(vout, SMALL[name][0], wide_out.at[i], rows, 96)
        send(wide_out.at[i], dst)
    for name, block, dst, width in (("q", q_out, oq, 64), ("k", k_out, ok, 16), ("v", v_new, ov, 16)):
        unpack_narrow(vout, SMALL[name][0], block, rows, width)
        send(block, dst)
    for i in THIRDS:
        tile = vout[SMALL["norms"][0] + i].astype(jnp.float32)
        n_out[2 * i] = tile[0:4].astype(jnp.bfloat16)
        n_out[2 * i + 1] = tile[4:8].astype(jnp.bfloat16)
    send(n_out, on)
    for j in range(COLS):
        rows[pl.ds(j, 8, stride=COLS), :] = vout[SMALL["qk"][0], :, LANES * j:LANES * (j + 1)].astype(jnp.float32)
    for layer in range(LAYERS):
        four = rows[4 * layer:4 * layer + 4, :]
        pair = [jnp.concatenate([four[2 * i:2 * i + 1], four[2 * i + 1:2 * i + 2]], axis=1) for i in PAIR]
        qk_out[layer] = jnp.concatenate(pair, axis=0).astype(jnp.bfloat16)
    send(qk_out, oqk)
    for copy in copies:
        copy.wait()


def solution(mesh):
    def local_update(*arrays):
        grads = [arr.reshape(arr.shape[1:]) for arr in arrays[:GRAD_COUNT]]
        state = [arr.reshape(SHARD_ROWS, LANES) for arr in arrays[GRAD_COUNT:GRAD_COUNT + 3]]
        shapes = [grad_arr.shape for grad_arr in grads]
        any_spec = pl.BlockSpec(memory_space=pl.ANY)
        vmem_spec = pl.BlockSpec(memory_space=pltpu.VMEM)
        dma = pltpu.SemaphoreType.DMA
        bf16, f32 = jnp.bfloat16, jnp.float32
        tiled = []
        for i, grad_arr in enumerate(grads[:8]):
            if i in (1, 2, 3):
                grad_arr = jnp.swapaxes(grad_arr, 1, 2)
            tiled.append(grad_arr.reshape(-1, LANES) if i in (5, 6) else grad_arr.reshape(-1, 8, WIDTH))
        tiled += grads[8:]
        small = [jax.ShapeDtypeStruct(arr.shape, bf16) for arr in tiled[1:]]
        *kept, _ = pl.pallas_call(
            kernel,
            out_shape=[pltpu.VMEM((SHARD_ROWS, LANES), f32)] * 3
            + [pltpu.VMEM((OUT_TILES, 8, WIDTH), bf16)]
            + [pltpu.HBM((TAIL_TILES, 8, WIDTH), bf16)],
            in_specs=[any_spec] * 14,
            out_specs=[vmem_spec] * 4 + [any_spec],
            scratch_shapes=[
                pltpu.VMEM((3 * 4 * PIECE_ROWS, LANES), f32),
                pltpu.VMEM((3, 2, PIECE_ROWS, LANES), f32),
                pltpu.VMEM((3, PIECE_ROWS, LANES), f32),
                pltpu.VMEM((3, TILE_ROWS, LANES), f32),
                pltpu.SMEM((5,), f32),
                pltpu.VMEM((3, RS_TILES, 8, WIDTH), bf16),
                pltpu.VMEM((8, LANES), f32),
                pltpu.VMEM((DEVS, 8, LANES), f32),
                pltpu.VMEM((2, 3840, LANES), bf16),
                pltpu.VMEM((48, 8, WIDTH), bf16),
                pltpu.VMEM((12, 8, WIDTH), bf16),
                pltpu.VMEM((12, 8, WIDTH), bf16),
                pltpu.VMEM(shapes[8], bf16),
                pltpu.VMEM(shapes[9], bf16),
                pltpu.VMEM((4, 8, WIDTH), bf16),
                dma((7,)), dma((3,)), dma((3 + len(SMALL),)),
                dma((3, 4)), dma((3, 3, 4)), dma((3, 3, 4)), dma((3, 2)), dma((3, 2)), dma((3, 2)), dma((3, 2)),
                dma((4,)), dma((3,)), dma((3,)), dma((DEVS,)), dma((DEVS,)),
                dma((3, 8)), dma((3, 8)), dma((3, 8)), dma((3, 8)), dma((3, LAST_PART + 1)), dma((3,)),
            ],
            compiler_params=pltpu.CompilerParams(
                collective_id=0, has_side_effects=True, vmem_limit_bytes=26_960_000),
        )(*tiled, *state, arrays[GRAD_COUNT + 3])
        kept = [pltpu.with_memory_space_constraint(arr, pltpu.VMEM) for arr in kept]
        outs = pl.pallas_call(
            flush,
            out_shape=[jax.ShapeDtypeStruct((EMBED_TILES, 8, WIDTH), bf16)] + small
            + [jax.ShapeDtypeStruct((SHARD_ROWS, LANES), f32)] * 3,
            in_specs=[vmem_spec] * 4,
            out_specs=[any_spec] * 13,
            scratch_shapes=[
                pltpu.VMEM((3840, LANES), f32),
                pltpu.VMEM((2, 3840, LANES), bf16),
                pltpu.VMEM((48, 8, WIDTH), bf16),
                pltpu.VMEM((12, 8, WIDTH), bf16),
                pltpu.VMEM((12, 8, WIDTH), bf16),
                pltpu.VMEM(shapes[8], bf16),
                pltpu.VMEM(shapes[9], bf16),
                dma((FLUSH_PARTS + 16,)),
            ],
            compiler_params=pltpu.CompilerParams(has_side_effects=True, vmem_limit_bytes=4_800_000),
        )(*kept)
        params = []
        for i, dims in enumerate(shapes):
            if i in (1, 2, 3):
                params.append(jnp.swapaxes(outs[i].reshape(dims[0], dims[2], dims[1]), 1, 2))
            else:
                params.append(outs[i].reshape(dims))
        return tuple(params) + tuple(arr.reshape(-1) for arr in outs[GRAD_COUNT:])

    in_specs = tuple([P("dp")] * GRAD_COUNT + [P("dp"), P("dp"), P("dp"), P()])
    out_specs = tuple([P()] * GRAD_COUNT + [P("dp"), P("dp"), P("dp")])
    return jax.shard_map(local_update, mesh=mesh, in_specs=in_specs, out_specs=out_specs, check_vma=False)
```

```python
import functools
import math
import jax
import jax.numpy as jnp
from jax import lax
from jax.experimental import pallas as pl
from jax.experimental.pallas import tpu as pltpu
from jax.sharding import PartitionSpec as P

ADAM_STEP = 7
ADAM_EPS = 1e-8
CLIP_EPS = 1e-6
GRAD_COUNT = 10
MESH = pl.DeviceIdType.MESH

DEVS = 16
OTHERS = range(1, DEVS)
THIRDS = range(3)
PAIR = range(2)
LANES = 128
WIDTH = 640
SHARD_ROWS = 6149
TILE_ROWS = 40
EMBED_TILES = 2048
ALL_TILES = 2460
DECAY_ROWS = 98240
FIRST_TAIL = 13
TAIL_START = (SHARD_ROWS * FIRST_TAIL) // TILE_ROWS
RS_TILES = 52
TAIL_TILES = (SHARD_ROWS * 15) // TILE_ROWS + 3 * RS_TILES - TAIL_START
AG_TILES = 51
PART_TILES = 16
LAST_PART = 3
FLUSH_PARTS = 4
LEAD = 40
G_ROWS = LEAD + 3 * RS_TILES * TILE_ROWS
ORDERS = ((2, 4, 8), (4, 8, 2), (8, 2, 4))


def flip(dev, stride):
    return dev + stride - 2 * stride * lax.rem(dev // stride, 2)


def rs_tiles(k):
    return RS_TILES - k // 2


def rs_start(dev):
    return (SHARD_ROWS * dev) // TILE_ROWS


def ag_start(dev):
    return (SHARD_ROWS * dev + TILE_ROWS - 1) // TILE_ROWS


def flip_mask(dev, order, mask):
    for bit, stride in enumerate(order):
        if mask >> bit & 1:
            dev = flip(dev, stride)
    return dev


SMALL = {}
for _name, _tiles in (("q", 48), ("k", 12), ("v", 12), ("out", 48), ("gate", 96), ("up", 96),
                      ("down", 96), ("norms", 3), ("qk", 1)):
    SMALL[_name] = (EMBED_TILES if not SMALL else sum(SMALL[_last]), _tiles)
    _last = _name
LAYERS = 6
COLS = WIDTH // LANES
OUT_TILES = 48 * RS_TILES
SPARE = 42 * RS_TILES
PIECE_ROWS = RS_TILES * TILE_ROWS
QUARTERS = range(4)
QUARTER = RS_TILES // 4


def slot_tiles(slot, k, f):
    index = 36 + f * 3 + k if slot == 3 else (slot * 3 + k) * 4 + f
    return pl.ds(index * RS_TILES, rs_tiles(k))


def sum_rows(k, f):
    return pl.ds((f * 3 + k) * PIECE_ROWS, rs_tiles(k) * TILE_ROWS)


def put_tile(dst, tile, rows, first, stride):
    for j in range(COLS):
        dst[tile, :, LANES * j:LANES * (j + 1)] = rows[pl.ds(first + j, 8, stride=stride), :].astype(jnp.bfloat16)


def pack_wide(src, dst, first_tile, rows, tiles):
    def step(i, _):
        rows[pl.ds(pl.multiple_of(i * 80, 16), 80), :] = src[pl.ds(pl.multiple_of(i * 80, 16), 80), :].astype(jnp.float32)
        for half in PAIR:
            put_tile(dst, first_tile + 2 * i + half, rows, i * 80 + half * 40, COLS)
        return 0

    lax.fori_loop(0, tiles // 2, step, 0)


def pack_narrow(src, dst, first_tile, rows, width):
    folds = LANES // width
    lane = lax.broadcasted_iota(jnp.int32, (8, LANES), 1) // width
    for layer in range(LAYERS):
        block = src[pl.ds(layer * width // 8, width // 8)].astype(jnp.float32).reshape(width, WIDTH)
        rows[pl.ds(layer * WIDTH, WIDTH), :] = jnp.concatenate([block] * folds, axis=0).T
    tiles = LAYERS * width // 8

    def step(t, _):
        for j in range(COLS):
            first = folds * (40 * t + j)
            value = rows[pl.ds(first, 8, stride=folds * COLS), :]
            for fold in range(1, folds):
                value = jnp.where(lane == fold, rows[pl.ds(first + fold, 8, stride=folds * COLS), :], value)
            dst[first_tile + t, :, LANES * j:LANES * (j + 1)] = value.astype(jnp.bfloat16)
        return 0

    lax.fori_loop(0, tiles, step, 0)


def unpack_wide(src, first_tile, dst, rows, tiles):
    def step(i, _):
        for half in PAIR:
            for j in range(COLS):
                rows[pl.ds(i * 80 + half * 40 + j, 8, stride=COLS), :] = src[
                    first_tile + 2 * i + half, :, LANES * j:LANES * (j + 1)].astype(jnp.float32)
        dst[pl.ds(pl.multiple_of(i * 80, 16), 80), :] = rows[pl.ds(pl.multiple_of(i * 80, 16), 80), :].astype(jnp.bfloat16)
        return 0

    lax.fori_loop(0, tiles // 2, step, 0)


def unpack_narrow(src, first_tile, dst, rows, width):
    folds = LANES // width
    tiles = LAYERS * width // 8

    def step(t, _):
        for j in range(COLS):
            value = src[first_tile + t, :, LANES * j:LANES * (j + 1)].astype(jnp.float32)
            for fold in range(folds):
                turned = value if fold == 0 else pltpu.roll(value, LANES - fold * width, 1)
                rows[pl.ds(folds * (40 * t + j) + fold, 8, stride=folds * COLS), :] = turned
        return 0

    lax.fori_loop(0, tiles, step, 0)
    for layer in range(LAYERS):
        block = rows[pl.ds(layer * WIDTH, WIDTH), :].T[:width]
        dst[pl.ds(layer * width // 8, width // 8)] = block.reshape(width // 8, 8, WIDTH).astype(jnp.bfloat16)


def kernel(emb, gq, gk, gv, go, gg, gu, gd, gn, gqk, m_in, v_in, p_in, hyp_in, mom, vel, par, vout, tail,
           s1, r2, r3, ext, hyp, nsend, nrecv, wide_raw, q_raw, k_raw, v_raw, n_raw, qk_raw, n_tiles,
           raw_sem, relay_sem, tail_sem,
           own_sem, r1_send, r1_recv, r2_send, r2_recv, r3_send, r3_recv, st_sem,
           ext_send, ext_recv, n_send, n_recv, ag_send, ag_recv, d2d_send, d2d_recv, last_recv):
    grad = s1.at[pl.ds(0, G_ROWS)]
    me = lax.axis_index("dp")
    partner = flip(me, 1)

    def remote(src, dst, ssem, rsem, dev):
        return pltpu.make_async_remote_copy(
            src_ref=src, dst_ref=dst, send_sem=ssem, recv_sem=rsem, device_id=(dev,), device_id_type=MESH)

    def from_shard(owner, k, make, embed=True, small=True):
        first = rs_start(owner) + k * RS_TILES

        if embed:
            @pl.when(owner < FIRST_TAIL)
            def _():
                make(emb.at[pl.ds(first, rs_tiles(k))]).start()

        if small:
            @pl.when(owner >= FIRST_TAIL)
            def _():
                make(tail.at[pl.ds(first - TAIL_START, rs_tiles(k))]).start()

    def rs_owner(dev, k, f):
        return flip_mask(dev, ORDERS[k], (0 if f >= 2 else 2) + (4 if f % 2 == 0 else 0))

    state = [pltpu.make_async_copy(src, dst, st_sem.at[i])
             for i, (src, dst) in enumerate(((m_in, mom), (v_in, vel), (p_in, par), (hyp_in, hyp)))]

    def load_own(f, embed=True, small=True):
        for k in THIRDS:
            from_shard(rs_owner(me, k, f), k, lambda src, k=k: pltpu.make_async_copy(
                src, vout.at[slot_tiles(3, k, f)], own_sem.at[k, f]), embed, small)

    def first_owner(slot, k, f):
        dev = partner if slot == 2 else flip(me, ORDERS[k][0])
        if slot == 1:
            dev = flip(dev, 1)
        return dev, rs_owner(dev, k, f)

    def send_first(f, embed=True, small=True):
        for slot in THIRDS:
            for k in THIRDS:
                dev, owner = first_owner(slot, k, f)

                def make(src, k=k, slot=slot, dev=dev):
                    return remote(src, vout.at[slot_tiles(slot, k, f)], r1_send.at[slot, k, f],
                                  r1_recv.at[slot, k, f], dev)

                from_shard(owner, k, make, embed, small)

    barrier = pltpu.get_barrier_semaphore()
    near = [flip(me, order[0]) for order in ORDERS]
    near += [flip(dev, 1) for dev in near] + [partner]
    for dev in near:
        pl.semaphore_signal(barrier, inc=1, device_id=(dev,), device_id_type=MESH)
    raw = [pltpu.make_async_copy(src, dst, raw_sem.at[i]) for i, (src, dst) in enumerate((
        (gg, wide_raw.at[0]), (gu, wide_raw.at[1]), (gq, q_raw), (gk, k_raw), (gv, v_raw), (gn, n_raw), (gqk, qk_raw)))]
    for copy in raw:
        copy.start()
    edge = EMBED_TILES - TAIL_START
    relayed = []
    start = SPARE
    for i, (src, first, tiles) in enumerate(((go, SMALL["out"][0], 48), (gd, SMALL["down"][0], 96),
                                             (emb.at[pl.ds(TAIL_START, edge)], TAIL_START, edge))):
        part = vout.at[pl.ds(start, tiles)]
        copy = pltpu.make_async_copy(src, part, relay_sem.at[i])
        copy.start()
        relayed.append((copy, pltpu.make_async_copy(part, tail.at[pl.ds(first - TAIL_START, tiles)], tail_sem.at[i])))
        start += tiles
    for f in PAIR:
        load_own(f, small=False)
    pl.semaphore_wait(barrier, len(near))
    for f in THIRDS:
        send_first(f, small=False)

    for copy, onward in relayed:
        copy.wait()
        onward.start()
    onwards = [onward for _, onward in relayed]

    raw_names = list(SMALL)

    def to_tail(src, name):
        first, tiles = SMALL[name]
        copy = pltpu.make_async_copy(src, tail.at[pl.ds(first - TAIL_START, tiles)], tail_sem.at[3 + raw_names.index(name)])
        copy.start()
        onwards.append(copy)

    spare = start
    for i, name in enumerate(("gate", "up")):
        raw[i].wait()
        pack_wide(wide_raw.at[i], vout, spare, grad, 96)
        to_tail(vout.at[pl.ds(spare, 96)], name)
        onwards.pop().wait()
    for i, (name, src, width) in enumerate((("q", q_raw, 64), ("k", k_raw, 16), ("v", v_raw, 16))):
        raw[2 + i].wait()
        pack_narrow(src, vout, spare, grad, width)
        tiles = SMALL[name][1]
        to_tail(vout.at[pl.ds(spare, tiles)], name)
        spare += tiles
    raw[5].wait()
    raw[6].wait()
    for i in THIRDS:
        n_tiles[i] = jnp.concatenate([n_raw[2 * i].astype(jnp.float32), n_raw[2 * i + 1].astype(jnp.float32)],
                                     axis=0).astype(jnp.bfloat16)
    grad[24:40, :] = jnp.zeros((16, LANES), jnp.float32)
    for layer in range(LAYERS):
        pair = qk_raw[layer].astype(jnp.float32)
        for i in PAIR:
            for half in PAIR:
                row = (2 * layer + i) * 2 + half
                grad[row:row + 1, :] = pair[i:i + 1, LANES * half:LANES * (half + 1)]
    put_tile(n_tiles, 3, grad, 0, COLS)
    to_tail(n_tiles.at[pl.ds(0, 3)], "norms")
    to_tail(n_tiles.at[pl.ds(3, 1)], "qk")
    for copy in onwards:
        copy.wait()
    for f in range(4):
        send_first(f, embed=f == 3)
        load_own(f, embed=f > 1)
    before = lax.rem(me + DEVS - 1, DEVS)
    ext_copies = [remote(src.at[pl.ds(0, TILE_ROWS)], ext.at[i], ext_send.at[i], ext_recv.at[i], before)
                  for i, src in enumerate((m_in, v_in, p_in))]
    for copy in state:
        copy.start()

    def r1_copy(slot, k, f):
        return remote(emb.at[pl.ds(0, rs_tiles(k))], vout.at[slot_tiles(slot, k, f)], r1_send.at[slot, k, f],
                      r1_recv.at[slot, k, f], partner)

    def r2_copy(k, f):
        return remote(s1.at[sum_rows(k, f)], r2.at[k, f, pl.ds(0, sum_rows(k, f).size)], r2_send.at[k, f], r2_recv.at[k, f], flip(me, ORDERS[k][1]))

    def quarter(k, i):
        return i * QUARTER, min((i + 1) * QUARTER, rs_tiles(k))

    def r3_copy(k, i):
        first, end = quarter(k, i)
        rows = (end - first) * TILE_ROWS
        src = pl.ds(sum_rows(k, 2).start + first * TILE_ROWS, rows)
        dst = pl.ds(first * TILE_ROWS, rows)
        return remote(s1.at[src], r3.at[k, dst], r3_send.at[k, i], r3_recv.at[k, i], flip(me, ORDERS[k][2]))

    for f in range(4):
        for k in THIRDS:
            pltpu.make_async_copy(
                emb.at[pl.ds(0, rs_tiles(k))], vout.at[slot_tiles(3, k, f)], own_sem.at[k, f]).wait()
            for slot in (2, 0, 1):
                r1_copy(slot, k, f).wait_recv()

            def add_four(t, _, k=k, f=f):
                a, b, c, d = [vout[slot_tiles(slot, k, f).start + t].astype(jnp.float32) for slot in (3, 2, 0, 1)]
                total = (a + b) + (c + d)
                row = sum_rows(k, f).start + TILE_ROWS * t
                for j in range(COLS):
                    s1[pl.ds(pl.multiple_of(row + 8 * j, 8), 8), :] = total[:, LANES * j:LANES * (j + 1)]
                return 0

            lax.fori_loop(0, rs_tiles(k), add_four, 0, unroll=2)
            if f < 2:
                r2_copy(k, f).start()
    for f in PAIR:
        for k in THIRDS:
            r2_copy(k, f).wait_recv()

            def add_two(t, _, k=k, f=f):
                row = pl.multiple_of(TILE_ROWS * t, 8)
                at = pl.ds(pl.multiple_of(sum_rows(k, 2 + f).start + TILE_ROWS * t, 8), TILE_ROWS)
                s1[at, :] = s1[at, :] + r2[k, f, pl.ds(row, TILE_ROWS), :]
                return 0

            for i in QUARTERS:
                lax.fori_loop(*quarter(k, i), add_two, 0, unroll=2)
                if f == 0:
                    r3_copy(k, i).start()

    shift = LEAD - (SHARD_ROWS * me - TILE_ROWS * rs_start(me))
    for k in THIRDS:
        for f in PAIR:
            r2_copy(k, f).wait_send()
    def squares(i, acc):
        part = grad[pl.ds(pl.multiple_of(i * TILE_ROWS, 8), TILE_ROWS), :]
        return acc + part * part

    def finish(k, t, carry):
        row = pl.multiple_of(TILE_ROWS * t, 8)
        at = pl.ds(pl.multiple_of(sum_rows(k, 3).start + TILE_ROWS * t, 8), TILE_ROWS)
        total = (s1[at, :] + r3[k, pl.ds(row, TILE_ROWS), :]) * (1.0 / DEVS)
        row = shift + TILE_ROWS * (k * RS_TILES + t)
        for j in range(COLS):
            grad[pl.ds(row + j, 8, stride=COLS), :] = total[8 * j:8 * (j + 1), :]
        return carry

    acc = jnp.zeros((TILE_ROWS, LANES), jnp.float32)
    end = (LEAD + SHARD_ROWS) // TILE_ROWS
    for i in QUARTERS:
        for k in THIRDS:
            r3_copy(k, i).wait_recv()
            lax.fori_loop(*quarter(k, i), functools.partial(finish, k), 0, unroll=2)
        for k in THIRDS:
            blocks = [k * RS_TILES + q * QUARTER + (q % 4 == 0) for q in (i, i + 1)]
            acc = lax.fori_loop(blocks[0], min(blocks[1], end), squares, acc, unroll=3)
    for copy in ext_copies:
        copy.start()
    nsend[...] = acc[0:8] + acc[8:16] + acc[16:24] + acc[24:32] + acc[32:40]
    start = end * TILE_ROWS
    for row, rows in ((start, 8), (start + 8, 8), (start + 16, 8), (start + 24, 5)):
        part = grad[pl.ds(row, rows), :]
        nsend[0:rows, :] = nsend[0:rows, :] + part * part

    others = [flip_mask(me, (1, 2, 4, 8), mask) for mask in sorted(OTHERS, key=lambda mask: -(mask // 2).bit_count())]

    def n_copy(i, source):
        return remote(nsend, nrecv.at[source], n_send.at[i], n_recv.at[source], others[i])

    for i in range(len(others)):
        n_copy(i, me).start()

    for copy in state:
        copy.wait()

    def full(value):
        return jnp.full((8, LANES), value, jnp.float32)

    learn_rate, beta_one, beta_two, decay, max_norm = [full(hyp[i]) for i in range(5)]
    rest_one, rest_two = 1.0 - beta_one, 1.0 - beta_two
    hat_one = 1.0 / (1.0 - lax.integer_pow(beta_one, ADAM_STEP))
    hat_two = 1.0 / (1.0 - lax.integer_pow(beta_two, ADAM_STEP))
    for copy in ext_copies:
        copy.wait_recv()

    for i, dev in enumerate(others):
        n_copy(i, me).wait_send()
        n_copy(i, dev).wait_recv()
    nrecv[me] = nsend[...]
    total = nrecv[0]
    for j in OTHERS:
        total = total + nrecv[j]
    total = jnp.sum(jnp.sum(total, axis=1, keepdims=True), axis=0, keepdims=True)
    clip = jnp.minimum(1.0, max_norm / (jnp.sqrt(jnp.broadcast_to(total, (8, LANES))) + CLIP_EPS))

    def wide(value, rows):
        if rows <= 8:
            return value[:rows]
        return jnp.concatenate([value] * (rows // 8), axis=0)

    def adam(g, m, v, p, first_row, rows):
        clipped = g * wide(clip, rows)
        m = wide(beta_one, rows) * m + wide(rest_one, rows) * clipped
        v = wide(beta_two, rows) * v + wide(rest_two, rows) * (clipped * clipped)
        index = first_row + lax.broadcasted_iota(jnp.int32, (rows, LANES), 0)
        update = (m * wide(hat_one, rows)) / (jnp.sqrt(v * wide(hat_two, rows)) + ADAM_EPS)
        update = update + jnp.where(index < DECAY_ROWS, wide(decay, rows) * p, 0.0)
        return m, v, p - wide(learn_rate, rows) * update

    def adam_rows(row, rows):
        at = pl.ds(row, rows)
        shifted = pl.ds(row + LEAD, rows)
        m, v, p = adam(grad[shifted, :], mom[at, :], vel[at, :], par[at, :], SHARD_ROWS * me + row, rows)
        mom[at, :] = m
        vel[at, :] = v
        par[at, :] = p
        grad[shifted, :] = p

    def adam_block(i, _):
        adam_rows(pl.multiple_of(i * 40, 8), 40)
        return 0

    def ag_sizes(owner, k, run):
        if k < 2:
            run(AG_TILES)
            return
        longer = ag_start(owner + 1) - ag_start(owner) == 3 * AG_TILES + 1

        @pl.when(longer)
        def _():
            run(AG_TILES + 1)

        @pl.when(jnp.logical_not(longer))
        def _():
            run(AG_TILES)

    def ag_each(k, mask, run, dev=me):
        owner = flip_mask(dev, ORDERS[k], mask)
        first = ag_start(owner) + k * AG_TILES
        ag_sizes(owner, k, lambda size: run(vout.at[pl.ds(first, size)], size))

    def ag_link(k, mask, link, start=True):
        dev = flip(me, ORDERS[k][link])
        slot = mask + (1 << link)

        def copy(dst, size):
            return remote(dst, dst, ag_send.at[k, slot], ag_recv.at[k, slot], dev)

        if start:
            ag_each(k, mask, lambda dst, size: copy(dst, size).start())
        pending.append(lambda: ag_each(k, mask, lambda dst, size: copy(dst, size).wait_send()))

    def ag_part(k, mask, i, run):
        owner = flip_mask(me, ORDERS[k], mask)
        first = ag_start(owner) + k * AG_TILES + i * PART_TILES
        if i < LAST_PART:
            run(vout.at[pl.ds(first, PART_TILES)])
        else:
            ag_sizes(owner, k, lambda size: run(vout.at[pl.ds(first, size - LAST_PART * PART_TILES)]))

    def last_copy(k, i, part):
        return remote(part, part, ag_send.at[k, 7], last_recv.at[k, i], flip(me, ORDERS[k][2]))

    def across_copy(k, part):
        return remote(part, part, d2d_send.at[k, 7], d2d_recv.at[k, 7], partner)

    def ag_across(k, mask, start=True):
        def copy(dst, size):
            return remote(dst, dst, d2d_send.at[k, mask], d2d_recv.at[k, mask], partner)

        if start:
            ag_each(k, mask, lambda dst, size: copy(dst, size).start())
        pending.append(lambda: ag_each(k, mask, lambda dst, size: copy(dst, size).wait_send()))

    def ag_arrived(k, mask):
        ag_each(k, mask, lambda dst, size: remote(
            dst, dst, ag_send.at[k, mask], ag_recv.at[k, mask], partner).wait_recv())

    pending = []
    base = LEAD + TILE_ROWS * ag_start(me) - SHARD_ROWS * me

    def own_part(k, skip, count, blocks):
        lax.fori_loop(*blocks, adam_block, 0)
        if k == 2:
            adam_rows(6120, 24)
            adam_rows(6144, 5)
            at = pl.ds(LEAD + SHARD_ROWS, TILE_ROWS)
            _, _, p = adam(grad[at, :], ext[0], ext[1], ext[2], SHARD_ROWS * (me + 1), TILE_ROWS)
            grad[at, :] = p
        first = ag_start(me) + k * AG_TILES

        def pack(t, _):
            put_tile(vout, first + t, grad, base + TILE_ROWS * (k * AG_TILES + t), COLS)
            return 0

        lax.fori_loop(skip, skip + (ag_start(me + 1) - first if k == 2 else count), pack, 0)

        def send(size):
            part = vout.at[pl.ds(first + skip, size)]
            for link in THIRDS:
                slot = 1 << link
                remote(part, part, ag_send.at[k, slot], ag_recv.at[k, slot], flip(me, ORDERS[k][link])).start()
            remote(part, part, d2d_send.at[k, 0], d2d_recv.at[k, 0], partner).start()

        if k == 2:
            ag_sizes(me, k, send)
        else:
            send(count)

    own_part(0, 0, 7, (0, 8))
    own_part(0, 7, 14, (8, 22))
    own_part(0, 21, 30, (22, 52))
    own_part(1, 0, AG_TILES, (52, 103))
    own_part(2, 0, None, (103, 153))
    for k in THIRDS:
        for link in THIRDS:
            ag_link(k, 0, link, start=False)
        ag_across(k, 0, start=False)
    for k in THIRDS:
        ag_arrived(k, 1)
        ag_link(k, 1, 1)
        ag_across(k, 1)
    for k in THIRDS:
        ag_link(k, 1, 2)
    for k in THIRDS:
        ag_arrived(k, 2)
        ag_link(k, 2, 2)
        ag_across(k, 2)
    for copy in ext_copies:
        copy.wait_send()
    for f in range(4):
        for k in THIRDS:
            for slot in THIRDS:
                r1_copy(slot, k, f).wait_send()
    for k in THIRDS:
        for i in QUARTERS:
            r3_copy(k, i).wait_send()
    for k in THIRDS:
        ag_arrived(k, 4)
        ag_across(k, 4)
    for k in THIRDS:
        ag_arrived(k, 3)
        for i in range(LAST_PART + 1):
            ag_part(k, 3, i, lambda part, k=k, i=i: last_copy(k, i, part).start())
        ag_across(k, 3)
    for mask in (5, 6):
        for k in THIRDS:
            ag_arrived(k, mask)
            ag_across(k, mask)
    def from_partner(masks):
        for mask in masks:
            for k in THIRDS:
                ag_each(k, mask, lambda dst, size, k=k, mask=mask: remote(
                    dst, dst, d2d_send.at[k, mask], d2d_recv.at[k, mask], partner).wait_recv(), partner)

    from_partner(range(5))
    for wait in pending:
        wait()
    pending.clear()
    for i in range(LAST_PART + 1):
        for k in THIRDS:
            ag_part(k, 7, i, lambda part, k=k, i=i: last_copy(k, i, part).wait_recv())
            ag_part(k, 7, i, lambda part, k=k, i=i: across_copy(k, part).start())
    for k in THIRDS:
        ag_link(k, 3, 2, start=False)
        ag_across(k, 7, start=False)
    from_partner(range(5, 8))
    for wait in pending:
        wait()


def flush(mom, vel, par, vout, embed, oq, ok, ov, oo, og, ou, od, on, oqk, m_out, v_out, p_out,
          rows, wide_out, q_out, k_out, v_new, n_out, qk_out, sem):
    copies = []

    def send(src, dst):
        copy = pltpu.make_async_copy(src, dst, sem.at[len(copies)])
        copy.start()
        copies.append(copy)

    for i in range(FLUSH_PARTS):
        part = pl.ds(i * (EMBED_TILES // FLUSH_PARTS), EMBED_TILES // FLUSH_PARTS)
        send(vout.at[part], embed.at[part])
    for src, dst in ((mom, m_out), (vel, v_out), (par, p_out)):
        send(src, dst)
    for name, dst in (("out", oo), ("down", od)):
        send(vout.at[pl.ds(*SMALL[name])], dst)
    for i, (name, dst) in enumerate((("gate", og), ("up", ou))):
        unpack_wide(vout, SMALL[name][0], wide_out.at[i], rows, 96)
        send(wide_out.at[i], dst)
    for name, block, dst, width in (("q", q_out, oq, 64), ("k", k_out, ok, 16), ("v", v_new, ov, 16)):
        unpack_narrow(vout, SMALL[name][0], block, rows, width)
        send(block, dst)
    for i in THIRDS:
        tile = vout[SMALL["norms"][0] + i].astype(jnp.float32)
        n_out[2 * i] = tile[0:4].astype(jnp.bfloat16)
        n_out[2 * i + 1] = tile[4:8].astype(jnp.bfloat16)
    send(n_out, on)
    for j in range(COLS):
        rows[pl.ds(j, 8, stride=COLS), :] = vout[SMALL["qk"][0], :, LANES * j:LANES * (j + 1)].astype(jnp.float32)
    for layer in range(LAYERS):
        four = rows[4 * layer:4 * layer + 4, :]
        pair = [jnp.concatenate([four[2 * i:2 * i + 1], four[2 * i + 1:2 * i + 2]], axis=1) for i in PAIR]
        qk_out[layer] = jnp.concatenate(pair, axis=0).astype(jnp.bfloat16)
    send(qk_out, oqk)
    for copy in copies:
        copy.wait()


def solution(mesh):
    def local_update(*arrays):
        grads = [arr.reshape(arr.shape[1:]) for arr in arrays[:GRAD_COUNT]]
        state = [arr.reshape(SHARD_ROWS, LANES) for arr in arrays[GRAD_COUNT:GRAD_COUNT + 3]]
        shapes = [grad_arr.shape for grad_arr in grads]
        any_spec = pl.BlockSpec(memory_space=pl.ANY)
        vmem_spec = pl.BlockSpec(memory_space=pltpu.VMEM)
        dma = pltpu.SemaphoreType.DMA
        bf16, f32 = jnp.bfloat16, jnp.float32
        tiled = []
        for i, grad_arr in enumerate(grads[:8]):
            if i in (1, 2, 3):
                grad_arr = jnp.swapaxes(grad_arr, 1, 2)
            tiled.append(grad_arr.reshape(-1, LANES) if i in (5, 6) else grad_arr.reshape(-1, 8, WIDTH))
        tiled += grads[8:]
        small = [jax.ShapeDtypeStruct(arr.shape, bf16) for arr in tiled[1:]]
        *kept, _ = pl.pallas_call(
            kernel,
            out_shape=[pltpu.VMEM((SHARD_ROWS, LANES), f32)] * 3
            + [pltpu.VMEM((OUT_TILES, 8, WIDTH), bf16)]
            + [pltpu.HBM((TAIL_TILES, 8, WIDTH), bf16)],
            in_specs=[any_spec] * 14,
            out_specs=[vmem_spec] * 4 + [any_spec],
            scratch_shapes=[
                pltpu.VMEM((3 * 4 * PIECE_ROWS, LANES), f32),
                pltpu.VMEM((3, 2, PIECE_ROWS, LANES), f32),
                pltpu.VMEM((3, PIECE_ROWS, LANES), f32),
                pltpu.VMEM((3, TILE_ROWS, LANES), f32),
                pltpu.SMEM((5,), f32),
                pltpu.VMEM((8, LANES), f32),
                pltpu.VMEM((DEVS, 8, LANES), f32),
                pltpu.VMEM((2, 3840, LANES), bf16),
                pltpu.VMEM((48, 8, WIDTH), bf16),
                pltpu.VMEM((12, 8, WIDTH), bf16),
                pltpu.VMEM((12, 8, WIDTH), bf16),
                pltpu.VMEM(shapes[8], bf16),
                pltpu.VMEM(shapes[9], bf16),
                pltpu.VMEM((4, 8, WIDTH), bf16),
                dma((7,)), dma((3,)), dma((3 + len(SMALL),)),
                dma((3, 4)), dma((3, 3, 4)), dma((3, 3, 4)), dma((3, 2)), dma((3, 2)), dma((3, 4)), dma((3, 4)),
                dma((4,)), dma((3,)), dma((3,)), dma((DEVS,)), dma((DEVS,)),
                dma((3, 8)), dma((3, 8)), dma((3, 8)), dma((3, 8)), dma((3, LAST_PART + 1)),
            ],
            compiler_params=pltpu.CompilerParams(
                collective_id=0, has_side_effects=True, vmem_limit_bytes=26_500_000),
        )(*tiled, *state, arrays[GRAD_COUNT + 3])
        kept = [pltpu.with_memory_space_constraint(arr, pltpu.VMEM) for arr in kept]
        outs = pl.pallas_call(
            flush,
            out_shape=[jax.ShapeDtypeStruct((EMBED_TILES, 8, WIDTH), bf16)] + small
            + [jax.ShapeDtypeStruct((SHARD_ROWS, LANES), f32)] * 3,
            in_specs=[vmem_spec] * 4,
            out_specs=[any_spec] * 13,
            scratch_shapes=[
                pltpu.VMEM((3840, LANES), f32),
                pltpu.VMEM((2, 3840, LANES), bf16),
                pltpu.VMEM((48, 8, WIDTH), bf16),
                pltpu.VMEM((12, 8, WIDTH), bf16),
                pltpu.VMEM((12, 8, WIDTH), bf16),
                pltpu.VMEM(shapes[8], bf16),
                pltpu.VMEM(shapes[9], bf16),
                dma((FLUSH_PARTS + 16,)),
            ],
            compiler_params=pltpu.CompilerParams(has_side_effects=True, vmem_limit_bytes=4_800_000),
        )(*kept)
        params = []
        for i, dims in enumerate(shapes):
            if i in (1, 2, 3):
                params.append(jnp.swapaxes(outs[i].reshape(dims[0], dims[2], dims[1]), 1, 2))
            else:
                params.append(outs[i].reshape(dims))
        return tuple(params) + tuple(arr.reshape(-1) for arr in outs[GRAD_COUNT:])

    in_specs = tuple([P("dp")] * GRAD_COUNT + [P("dp"), P("dp"), P("dp"), P()])
    out_specs = tuple([P()] * GRAD_COUNT + [P("dp"), P("dp"), P("dp")])
    return jax.shard_map(local_update, mesh=mesh, in_specs=in_specs, out_specs=out_specs, check_vma=False)
```

```python
import functools
import math
import jax
import jax.numpy as jnp
from jax import lax
from jax.experimental import pallas as pl
from jax.experimental.pallas import tpu as pltpu
from jax.sharding import PartitionSpec as P

ADAM_STEP = 7
ADAM_EPS = 1e-8
CLIP_EPS = 1e-6
GRAD_COUNT = 10
MESH = pl.DeviceIdType.MESH

DEVS = 16
OTHERS = range(1, DEVS)
THIRDS = range(3)
PAIR = range(2)
LANES = 128
WIDTH = 640
SHARD_ROWS = 6149
TILE_ROWS = 40
EMBED_TILES = 2048
ALL_TILES = 2460
DECAY_ROWS = 98240
FIRST_TAIL = 13
TAIL_START = (SHARD_ROWS * FIRST_TAIL) // TILE_ROWS
RS_TILES = 52
TAIL_TILES = (SHARD_ROWS * 15) // TILE_ROWS + 3 * RS_TILES - TAIL_START
AG_TILES = 51
PART_TILES = 16
LAST_PART = 3
FLUSH_PARTS = 4
LEAD = 40
G_ROWS = LEAD + 3 * RS_TILES * TILE_ROWS
ORDERS = ((2, 4, 8), (4, 8, 2), (8, 2, 4))


def flip(dev, stride):
    return dev + stride - 2 * stride * lax.rem(dev // stride, 2)


def rs_tiles(k):
    return RS_TILES - k // 2


def rs_start(dev):
    return (SHARD_ROWS * dev) // TILE_ROWS


def ag_start(dev):
    return (SHARD_ROWS * dev + TILE_ROWS - 1) // TILE_ROWS


def flip_mask(dev, order, mask):
    for bit, stride in enumerate(order):
        if mask >> bit & 1:
            dev = flip(dev, stride)
    return dev


SMALL = {}
for _name, _tiles in (("q", 48), ("k", 12), ("v", 12), ("out", 48), ("gate", 96), ("up", 96),
                      ("down", 96), ("norms", 3), ("qk", 1)):
    SMALL[_name] = (EMBED_TILES if not SMALL else sum(SMALL[_last]), _tiles)
    _last = _name
LAYERS = 6
COLS = WIDTH // LANES
OUT_TILES = 48 * RS_TILES
SPARE = 42 * RS_TILES
PIECE_ROWS = RS_TILES * TILE_ROWS
QUARTERS = range(4)
QUARTER = RS_TILES // 4


def slot_tiles(slot, k, f):
    index = 36 + f * 3 + k if slot == 3 else (slot * 3 + k) * 4 + f
    return pl.ds(index * RS_TILES, rs_tiles(k))


def sum_rows(k, f):
    return pl.ds((f * 3 + k) * PIECE_ROWS, rs_tiles(k) * TILE_ROWS)


def put_tile(dst, tile, rows, first, stride):
    for j in range(COLS):
        dst[tile, :, LANES * j:LANES * (j + 1)] = rows[pl.ds(first + j, 8, stride=stride), :].astype(jnp.bfloat16)


def pack_wide(src, dst, first_tile, rows, tiles):
    def step(i, _):
        rows[pl.ds(pl.multiple_of(i * 80, 16), 80), :] = src[pl.ds(pl.multiple_of(i * 80, 16), 80), :].astype(jnp.float32)
        for half in PAIR:
            put_tile(dst, first_tile + 2 * i + half, rows, i * 80 + half * 40, COLS)
        return 0

    lax.fori_loop(0, tiles // 2, step, 0)


def pack_narrow(src, dst, first_tile, rows, width):
    folds = LANES // width
    lane = lax.broadcasted_iota(jnp.int32, (8, LANES), 1) // width
    for layer in range(LAYERS):
        block = src[pl.ds(layer * width // 8, width // 8)].astype(jnp.float32).reshape(width, WIDTH)
        rows[pl.ds(layer * WIDTH, WIDTH), :] = jnp.concatenate([block] * folds, axis=0).T
    tiles = LAYERS * width // 8

    def step(t, _):
        for j in range(COLS):
            first = folds * (40 * t + j)
            value = rows[pl.ds(first, 8, stride=folds * COLS), :]
            for fold in range(1, folds):
                value = jnp.where(lane == fold, rows[pl.ds(first + fold, 8, stride=folds * COLS), :], value)
            dst[first_tile + t, :, LANES * j:LANES * (j + 1)] = value.astype(jnp.bfloat16)
        return 0

    lax.fori_loop(0, tiles, step, 0)


def unpack_wide(src, first_tile, dst, rows, tiles):
    def step(i, _):
        for half in PAIR:
            for j in range(COLS):
                rows[pl.ds(i * 80 + half * 40 + j, 8, stride=COLS), :] = src[
                    first_tile + 2 * i + half, :, LANES * j:LANES * (j + 1)].astype(jnp.float32)
        dst[pl.ds(pl.multiple_of(i * 80, 16), 80), :] = rows[pl.ds(pl.multiple_of(i * 80, 16), 80), :].astype(jnp.bfloat16)
        return 0

    lax.fori_loop(0, tiles // 2, step, 0)


def unpack_narrow(src, first_tile, dst, rows, width):
    folds = LANES // width
    tiles = LAYERS * width // 8

    def step(t, _):
        for j in range(COLS):
            value = src[first_tile + t, :, LANES * j:LANES * (j + 1)].astype(jnp.float32)
            for fold in range(folds):
                turned = value if fold == 0 else pltpu.roll(value, LANES - fold * width, 1)
                rows[pl.ds(folds * (40 * t + j) + fold, 8, stride=folds * COLS), :] = turned
        return 0

    lax.fori_loop(0, tiles, step, 0)
    for layer in range(LAYERS):
        block = rows[pl.ds(layer * WIDTH, WIDTH), :].T[:width]
        dst[pl.ds(layer * width // 8, width // 8)] = block.reshape(width // 8, 8, WIDTH).astype(jnp.bfloat16)


def kernel(emb, gq, gk, gv, go, gg, gu, gd, gn, gqk, m_in, v_in, p_in, hyp_in, mom, vel, par, vout, tail,
           s1, r2, r3, ext, hyp, nsend, nrecv, wide_raw, q_raw, k_raw, v_raw, n_raw, qk_raw, n_tiles,
           raw_sem, relay_sem, tail_sem,
           own_sem, r1_send, r1_recv, r2_send, r2_recv, r3_send, r3_recv, st_sem,
           ext_send, ext_recv, n_send, n_recv, ag_send, ag_recv, d2d_send, d2d_recv, last_recv):
    grad = s1.at[pl.ds(0, G_ROWS)]
    me = lax.axis_index("dp")
    partner = flip(me, 1)

    def remote(src, dst, ssem, rsem, dev):
        return pltpu.make_async_remote_copy(
            src_ref=src, dst_ref=dst, send_sem=ssem, recv_sem=rsem, device_id=(dev,), device_id_type=MESH)

    def from_shard(owner, k, make, embed=True, small=True):
        first = rs_start(owner) + k * RS_TILES

        if embed:
            @pl.when(owner < FIRST_TAIL)
            def _():
                make(emb.at[pl.ds(first, rs_tiles(k))]).start()

        if small:
            @pl.when(owner >= FIRST_TAIL)
            def _():
                make(tail.at[pl.ds(first - TAIL_START, rs_tiles(k))]).start()

    def rs_owner(dev, k, f):
        return flip_mask(dev, ORDERS[k], (0 if f >= 2 else 2) + (4 if f % 2 == 0 else 0))

    state = [pltpu.make_async_copy(src, dst, st_sem.at[i])
             for i, (src, dst) in enumerate(((m_in, mom), (v_in, vel), (p_in, par), (hyp_in, hyp)))]

    def load_own(f, embed=True, small=True):
        for k in THIRDS:
            from_shard(rs_owner(me, k, f), k, lambda src, k=k: pltpu.make_async_copy(
                src, vout.at[slot_tiles(3, k, f)], own_sem.at[k, f]), embed, small)

    def first_owner(slot, k, f):
        dev = partner if slot == 2 else flip(me, ORDERS[k][0])
        if slot == 1:
            dev = flip(dev, 1)
        return dev, rs_owner(dev, k, f)

    def send_first(f, embed=True, small=True):
        for slot in THIRDS:
            for k in THIRDS:
                dev, owner = first_owner(slot, k, f)

                def make(src, k=k, slot=slot, dev=dev):
                    return remote(src, vout.at[slot_tiles(slot, k, f)], r1_send.at[slot, k, f],
                                  r1_recv.at[slot, k, f], dev)

                from_shard(owner, k, make, embed, small)

    barrier = pltpu.get_barrier_semaphore()
    near = [flip(me, order[0]) for order in ORDERS]
    near += [flip(dev, 1) for dev in near] + [partner]
    for dev in near:
        pl.semaphore_signal(barrier, inc=1, device_id=(dev,), device_id_type=MESH)
    raw = [pltpu.make_async_copy(src, dst, raw_sem.at[i]) for i, (src, dst) in enumerate((
        (gg, wide_raw.at[0]), (gu, wide_raw.at[1]), (gq, q_raw), (gk, k_raw), (gv, v_raw), (gn, n_raw), (gqk, qk_raw)))]
    for copy in raw:
        copy.start()
    edge = EMBED_TILES - TAIL_START
    relayed = []
    start = SPARE
    for i, (src, first, tiles) in enumerate(((go, SMALL["out"][0], 48), (gd, SMALL["down"][0], 96),
                                             (emb.at[pl.ds(TAIL_START, edge)], TAIL_START, edge))):
        part = vout.at[pl.ds(start, tiles)]
        copy = pltpu.make_async_copy(src, part, relay_sem.at[i])
        copy.start()
        relayed.append((copy, pltpu.make_async_copy(part, tail.at[pl.ds(first - TAIL_START, tiles)], tail_sem.at[i])))
        start += tiles
    for f in PAIR:
        load_own(f, small=False)
    pl.semaphore_wait(barrier, len(near))
    for f in THIRDS:
        send_first(f, small=False)

    for copy, onward in relayed:
        copy.wait()
        onward.start()
    onwards = [onward for _, onward in relayed]

    raw_names = list(SMALL)

    def to_tail(src, name):
        first, tiles = SMALL[name]
        copy = pltpu.make_async_copy(src, tail.at[pl.ds(first - TAIL_START, tiles)], tail_sem.at[3 + raw_names.index(name)])
        copy.start()
        onwards.append(copy)

    spare = start
    for i, name in enumerate(("gate", "up")):
        raw[i].wait()
        pack_wide(wide_raw.at[i], vout, spare, grad, 96)
        to_tail(vout.at[pl.ds(spare, 96)], name)
        onwards.pop().wait()
    for i, (name, src, width) in enumerate((("q", q_raw, 64), ("k", k_raw, 16), ("v", v_raw, 16))):
        raw[2 + i].wait()
        pack_narrow(src, vout, spare, grad, width)
        tiles = SMALL[name][1]
        to_tail(vout.at[pl.ds(spare, tiles)], name)
        spare += tiles
    raw[5].wait()
    raw[6].wait()
    for i in THIRDS:
        n_tiles[i] = jnp.concatenate([n_raw[2 * i].astype(jnp.float32), n_raw[2 * i + 1].astype(jnp.float32)],
                                     axis=0).astype(jnp.bfloat16)
    grad[24:40, :] = jnp.zeros((16, LANES), jnp.float32)
    for layer in range(LAYERS):
        pair = qk_raw[layer].astype(jnp.float32)
        for i in PAIR:
            for half in PAIR:
                row = (2 * layer + i) * 2 + half
                grad[row:row + 1, :] = pair[i:i + 1, LANES * half:LANES * (half + 1)]
    put_tile(n_tiles, 3, grad, 0, COLS)
    to_tail(n_tiles.at[pl.ds(0, 3)], "norms")
    to_tail(n_tiles.at[pl.ds(3, 1)], "qk")
    for copy in onwards:
        copy.wait()
    for f in range(4):
        send_first(f, embed=f == 3)
        load_own(f, embed=f > 1)
    before = lax.rem(me + DEVS - 1, DEVS)
    ext_copies = [remote(src.at[pl.ds(0, TILE_ROWS)], ext.at[i], ext_send.at[i], ext_recv.at[i], before)
                  for i, src in enumerate((m_in, v_in, p_in))]
    for copy in state:
        copy.start()

    def r1_copy(slot, k, f):
        return remote(emb.at[pl.ds(0, rs_tiles(k))], vout.at[slot_tiles(slot, k, f)], r1_send.at[slot, k, f],
                      r1_recv.at[slot, k, f], partner)

    def r2_copy(k, f):
        return remote(s1.at[sum_rows(k, f)], r2.at[k, f, pl.ds(0, sum_rows(k, f).size)], r2_send.at[k, f], r2_recv.at[k, f], flip(me, ORDERS[k][1]))

    def quarter(k, i):
        return i * QUARTER, min((i + 1) * QUARTER, rs_tiles(k))

    def r3_copy(k, i):
        first, end = quarter(k, i)
        rows = (end - first) * TILE_ROWS
        src = pl.ds(sum_rows(k, 2).start + first * TILE_ROWS, rows)
        dst = pl.ds(first * TILE_ROWS, rows)
        return remote(s1.at[src], r3.at[k, dst], r3_send.at[k, i], r3_recv.at[k, i], flip(me, ORDERS[k][2]))

    for f in range(4):
        for k in THIRDS:
            pltpu.make_async_copy(
                emb.at[pl.ds(0, rs_tiles(k))], vout.at[slot_tiles(3, k, f)], own_sem.at[k, f]).wait()
            for slot in (2, 0, 1):
                r1_copy(slot, k, f).wait_recv()

            def add_four(t, _, k=k, f=f):
                a, b, c, d = [vout[slot_tiles(slot, k, f).start + t].astype(jnp.float32) for slot in (3, 2, 0, 1)]
                total = (a + b) + (c + d)
                row = sum_rows(k, f).start + TILE_ROWS * t
                for j in range(COLS):
                    s1[pl.ds(pl.multiple_of(row + 8 * j, 8), 8), :] = total[:, LANES * j:LANES * (j + 1)]
                return 0

            lax.fori_loop(0, rs_tiles(k), add_four, 0, unroll=2)
            if f < 2:
                r2_copy(k, f).start()
    for f in PAIR:
        for k in THIRDS:
            r2_copy(k, f).wait_recv()

            def add_two(t, _, k=k, f=f):
                row = pl.multiple_of(TILE_ROWS * t, 8)
                at = pl.ds(pl.multiple_of(sum_rows(k, 2 + f).start + TILE_ROWS * t, 8), TILE_ROWS)
                s1[at, :] = s1[at, :] + r2[k, f, pl.ds(row, TILE_ROWS), :]
                return 0

            for i in QUARTERS:
                lax.fori_loop(*quarter(k, i), add_two, 0, unroll=2)
                if f == 0:
                    r3_copy(k, i).start()

    shift = LEAD - (SHARD_ROWS * me - TILE_ROWS * rs_start(me))
    for k in THIRDS:
        for f in PAIR:
            r2_copy(k, f).wait_send()
    def squares(i, acc):
        part = grad[pl.ds(pl.multiple_of(i * TILE_ROWS, 8), TILE_ROWS), :]
        return acc + part * part

    def finish(k, t, carry):
        row = pl.multiple_of(TILE_ROWS * t, 8)
        at = pl.ds(pl.multiple_of(sum_rows(k, 3).start + TILE_ROWS * t, 8), TILE_ROWS)
        total = (s1[at, :] + r3[k, pl.ds(row, TILE_ROWS), :]) * (1.0 / DEVS)
        row = shift + TILE_ROWS * (k * RS_TILES + t)
        for j in range(COLS):
            grad[pl.ds(row + j, 8, stride=COLS), :] = total[8 * j:8 * (j + 1), :]
        return carry

    acc = jnp.zeros((TILE_ROWS, LANES), jnp.float32)
    end = (LEAD + SHARD_ROWS) // TILE_ROWS
    for i in QUARTERS:
        for k in THIRDS:
            r3_copy(k, i).wait_recv()
            lax.fori_loop(*quarter(k, i), functools.partial(finish, k), 0, unroll=2)
        for k in THIRDS:
            blocks = [k * RS_TILES + q * QUARTER + (q % 4 == 0) for q in (i, i + 1)]
            acc = lax.fori_loop(blocks[0], min(blocks[1], end), squares, acc, unroll=3)
    start = end * TILE_ROWS
    total = jnp.sum(acc, axis=0, keepdims=True)
    for row, rows in ((start, 24), (start + 24, 5)):
        part = grad[pl.ds(row, rows), :]
        total = total + jnp.sum(part * part, axis=0, keepdims=True)
    nsend[...] = total

    others = [flip_mask(me, (1, 2, 4, 8), mask) for mask in sorted(OTHERS, key=lambda mask: -(mask // 2).bit_count())]

    def n_copy(i, source):
        return remote(nsend, nrecv.at[source], n_send.at[i], n_recv.at[source], others[i])

    for i in range(len(others)):
        n_copy(i, me).start()
    for copy in ext_copies:
        copy.start()

    for copy in state:
        copy.wait()

    def full(value):
        return jnp.full((8, LANES), value, jnp.float32)

    learn_rate, beta_one, beta_two, decay, max_norm = [full(hyp[i]) for i in range(5)]
    rest_one, rest_two = 1.0 - beta_one, 1.0 - beta_two
    hat_one = 1.0 / (1.0 - lax.integer_pow(beta_one, ADAM_STEP))
    hat_two = 1.0 / (1.0 - lax.integer_pow(beta_two, ADAM_STEP))

    for i, dev in enumerate(others):
        n_copy(i, me).wait_send()
        n_copy(i, dev).wait_recv()
    nrecv[me] = nsend[...]
    total = jnp.sum(jnp.sum(nrecv[...], axis=0), axis=1, keepdims=True)
    clip = jnp.minimum(1.0, max_norm / (jnp.sqrt(jnp.broadcast_to(total, (8, LANES))) + CLIP_EPS))

    def wide(value, rows):
        if rows <= 8:
            return value[:rows]
        return jnp.concatenate([value] * (rows // 8), axis=0)

    def adam(g, m, v, p, first_row, rows):
        clipped = g * wide(clip, rows)
        m = wide(beta_one, rows) * m + wide(rest_one, rows) * clipped
        v = wide(beta_two, rows) * v + wide(rest_two, rows) * (clipped * clipped)
        index = first_row + lax.broadcasted_iota(jnp.int32, (rows, LANES), 0)
        update = (m * wide(hat_one, rows)) / (jnp.sqrt(v * wide(hat_two, rows)) + ADAM_EPS)
        update = update + jnp.where(index < DECAY_ROWS, wide(decay, rows) * p, 0.0)
        return m, v, p - wide(learn_rate, rows) * update

    def adam_rows(row, rows):
        at = pl.ds(row, rows)
        shifted = pl.ds(row + LEAD, rows)
        m, v, p = adam(grad[shifted, :], mom[at, :], vel[at, :], par[at, :], SHARD_ROWS * me + row, rows)
        mom[at, :] = m
        vel[at, :] = v
        par[at, :] = p
        grad[shifted, :] = p

    def adam_block(i, _):
        adam_rows(pl.multiple_of(i * 40, 8), 40)
        return 0

    def ag_sizes(owner, k, run):
        if k < 2:
            run(AG_TILES)
            return
        longer = ag_start(owner + 1) - ag_start(owner) == 3 * AG_TILES + 1

        @pl.when(longer)
        def _():
            run(AG_TILES + 1)

        @pl.when(jnp.logical_not(longer))
        def _():
            run(AG_TILES)

    def ag_each(k, mask, run, dev=me):
        owner = flip_mask(dev, ORDERS[k], mask)
        first = ag_start(owner) + k * AG_TILES
        ag_sizes(owner, k, lambda size: run(vout.at[pl.ds(first, size)], size))

    def ag_link(k, mask, link, start=True):
        dev = flip(me, ORDERS[k][link])
        slot = mask + (1 << link)

        def copy(dst, size):
            return remote(dst, dst, ag_send.at[k, slot], ag_recv.at[k, slot], dev)

        if start:
            ag_each(k, mask, lambda dst, size: copy(dst, size).start())
        pending.append(lambda: ag_each(k, mask, lambda dst, size: copy(dst, size).wait_send()))

    def ag_part(k, mask, i, run):
        owner = flip_mask(me, ORDERS[k], mask)
        first = ag_start(owner) + k * AG_TILES + i * PART_TILES
        if i < LAST_PART:
            run(vout.at[pl.ds(first, PART_TILES)])
        else:
            ag_sizes(owner, k, lambda size: run(vout.at[pl.ds(first, size - LAST_PART * PART_TILES)]))

    def last_copy(k, i, part):
        return remote(part, part, ag_send.at[k, 7], last_recv.at[k, i], flip(me, ORDERS[k][2]))

    def across_copy(k, part):
        return remote(part, part, d2d_send.at[k, 7], d2d_recv.at[k, 7], partner)

    def ag_across(k, mask, start=True):
        def copy(dst, size):
            return remote(dst, dst, d2d_send.at[k, mask], d2d_recv.at[k, mask], partner)

        if start:
            ag_each(k, mask, lambda dst, size: copy(dst, size).start())
        pending.append(lambda: ag_each(k, mask, lambda dst, size: copy(dst, size).wait_send()))

    def ag_arrived(k, mask):
        ag_each(k, mask, lambda dst, size: remote(
            dst, dst, ag_send.at[k, mask], ag_recv.at[k, mask], partner).wait_recv())

    pending = []
    base = LEAD + TILE_ROWS * ag_start(me) - SHARD_ROWS * me

    def own_part(k, skip, count, blocks):
        lax.fori_loop(*blocks, adam_block, 0)
        if k == 2:
            adam_rows(6120, 24)
            adam_rows(6144, 5)
            for copy in ext_copies:
                copy.wait_recv()
            at = pl.ds(LEAD + SHARD_ROWS, TILE_ROWS)
            _, _, p = adam(grad[at, :], ext[0], ext[1], ext[2], SHARD_ROWS * (me + 1), TILE_ROWS)
            grad[at, :] = p
        first = ag_start(me) + k * AG_TILES

        def pack(t, _):
            put_tile(vout, first + t, grad, base + TILE_ROWS * (k * AG_TILES + t), COLS)
            return 0

        lax.fori_loop(skip, skip + (ag_start(me + 1) - first if k == 2 else count), pack, 0)

        def send(size):
            part = vout.at[pl.ds(first + skip, size)]
            for link in THIRDS:
                slot = 1 << link
                remote(part, part, ag_send.at[k, slot], ag_recv.at[k, slot], flip(me, ORDERS[k][link])).start()
            remote(part, part, d2d_send.at[k, 0], d2d_recv.at[k, 0], partner).start()

        if k == 2:
            ag_sizes(me, k, send)
        else:
            send(count)

    own_part(0, 0, 4, (0, 5))
    own_part(0, 4, 12, (5, 17))
    own_part(0, 16, 35, (17, 52))
    own_part(1, 0, AG_TILES, (52, 103))
    own_part(2, 0, None, (103, 153))
    for k in THIRDS:
        for link in THIRDS:
            ag_link(k, 0, link, start=False)
        ag_across(k, 0, start=False)
    for k in THIRDS:
        ag_arrived(k, 1)
        ag_link(k, 1, 1)
        ag_across(k, 1)
    for k in THIRDS:
        ag_link(k, 1, 2)
    for k in THIRDS:
        ag_arrived(k, 2)
        ag_link(k, 2, 2)
        ag_across(k, 2)
    for copy in ext_copies:
        copy.wait_send()
    for f in range(4):
        for k in THIRDS:
            for slot in THIRDS:
                r1_copy(slot, k, f).wait_send()
    for k in THIRDS:
        for i in QUARTERS:
            r3_copy(k, i).wait_send()
    for k in THIRDS:
        ag_arrived(k, 4)
        ag_across(k, 4)
    for k in THIRDS:
        ag_arrived(k, 3)
        for i in range(LAST_PART + 1):
            ag_part(k, 3, i, lambda part, k=k, i=i: last_copy(k, i, part).start())
        ag_across(k, 3)
    for mask in (5, 6):
        for k in THIRDS:
            ag_arrived(k, mask)
            ag_across(k, mask)
    def from_partner(masks):
        for mask in masks:
            for k in THIRDS:
                ag_each(k, mask, lambda dst, size, k=k, mask=mask: remote(
                    dst, dst, d2d_send.at[k, mask], d2d_recv.at[k, mask], partner).wait_recv(), partner)

    from_partner(range(5))
    for wait in pending:
        wait()
    pending.clear()
    for i in range(LAST_PART + 1):
        for k in THIRDS:
            ag_part(k, 7, i, lambda part, k=k, i=i: last_copy(k, i, part).wait_recv())
            ag_part(k, 7, i, lambda part, k=k, i=i: across_copy(k, part).start())
    for k in THIRDS:
        ag_link(k, 3, 2, start=False)
        ag_across(k, 7, start=False)
    from_partner(range(5, 8))
    for wait in pending:
        wait()


def flush(mom, vel, par, vout, embed, oq, ok, ov, oo, og, ou, od, on, oqk, m_out, v_out, p_out,
          rows, wide_out, q_out, k_out, v_new, n_out, qk_out, sem):
    copies = []

    def send(src, dst):
        copy = pltpu.make_async_copy(src, dst, sem.at[len(copies)])
        copy.start()
        copies.append(copy)

    for i in range(FLUSH_PARTS):
        part = pl.ds(i * (EMBED_TILES // FLUSH_PARTS), EMBED_TILES // FLUSH_PARTS)
        send(vout.at[part], embed.at[part])
    for src, dst in ((mom, m_out), (vel, v_out), (par, p_out)):
        send(src, dst)
    for name, dst in (("out", oo), ("down", od)):
        send(vout.at[pl.ds(*SMALL[name])], dst)
    for i, (name, dst) in enumerate((("gate", og), ("up", ou))):
        unpack_wide(vout, SMALL[name][0], wide_out.at[i], rows, 96)
        send(wide_out.at[i], dst)
    for name, block, dst, width in (("q", q_out, oq, 64), ("k", k_out, ok, 16), ("v", v_new, ov, 16)):
        unpack_narrow(vout, SMALL[name][0], block, rows, width)
        send(block, dst)
    for i in THIRDS:
        tile = vout[SMALL["norms"][0] + i].astype(jnp.float32)
        n_out[2 * i] = tile[0:4].astype(jnp.bfloat16)
        n_out[2 * i + 1] = tile[4:8].astype(jnp.bfloat16)
    send(n_out, on)
    for j in range(COLS):
        rows[pl.ds(j, 8, stride=COLS), :] = vout[SMALL["qk"][0], :, LANES * j:LANES * (j + 1)].astype(jnp.float32)
    for layer in range(LAYERS):
        four = rows[4 * layer:4 * layer + 4, :]
        pair = [jnp.concatenate([four[2 * i:2 * i + 1], four[2 * i + 1:2 * i + 2]], axis=1) for i in PAIR]
        qk_out[layer] = jnp.concatenate(pair, axis=0).astype(jnp.bfloat16)
    send(qk_out, oqk)
    for copy in copies:
        copy.wait()


def solution(mesh):
    def local_update(*arrays):
        grads = [arr.reshape(arr.shape[1:]) for arr in arrays[:GRAD_COUNT]]
        state = [arr.reshape(SHARD_ROWS, LANES) for arr in arrays[GRAD_COUNT:GRAD_COUNT + 3]]
        shapes = [grad_arr.shape for grad_arr in grads]
        any_spec = pl.BlockSpec(memory_space=pl.ANY)
        vmem_spec = pl.BlockSpec(memory_space=pltpu.VMEM)
        dma = pltpu.SemaphoreType.DMA
        bf16, f32 = jnp.bfloat16, jnp.float32
        tiled = []
        for i, grad_arr in enumerate(grads[:8]):
            if i in (1, 2, 3):
                grad_arr = jnp.swapaxes(grad_arr, 1, 2)
            tiled.append(grad_arr.reshape(-1, LANES) if i in (5, 6) else grad_arr.reshape(-1, 8, WIDTH))
        tiled += grads[8:]
        small = [jax.ShapeDtypeStruct(arr.shape, bf16) for arr in tiled[1:]]
        *kept, _ = pl.pallas_call(
            kernel,
            out_shape=[pltpu.VMEM((SHARD_ROWS, LANES), f32)] * 3
            + [pltpu.VMEM((OUT_TILES, 8, WIDTH), bf16)]
            + [pltpu.HBM((TAIL_TILES, 8, WIDTH), bf16)],
            in_specs=[any_spec] * 14,
            out_specs=[vmem_spec] * 4 + [any_spec],
            scratch_shapes=[
                pltpu.VMEM((3 * 4 * PIECE_ROWS, LANES), f32),
                pltpu.VMEM((3, 2, PIECE_ROWS, LANES), f32),
                pltpu.VMEM((3, PIECE_ROWS, LANES), f32),
                pltpu.VMEM((3, TILE_ROWS, LANES), f32),
                pltpu.SMEM((5,), f32),
                pltpu.VMEM((1, LANES), f32),
                pltpu.VMEM((DEVS, 1, LANES), f32),
                pltpu.VMEM((2, 3840, LANES), bf16),
                pltpu.VMEM((48, 8, WIDTH), bf16),
                pltpu.VMEM((12, 8, WIDTH), bf16),
                pltpu.VMEM((12, 8, WIDTH), bf16),
                pltpu.VMEM(shapes[8], bf16),
                pltpu.VMEM(shapes[9], bf16),
                pltpu.VMEM((4, 8, WIDTH), bf16),
                dma((7,)), dma((3,)), dma((3 + len(SMALL),)),
                dma((3, 4)), dma((3, 3, 4)), dma((3, 3, 4)), dma((3, 2)), dma((3, 2)), dma((3, 4)), dma((3, 4)),
                dma((4,)), dma((3,)), dma((3,)), dma((DEVS,)), dma((DEVS,)),
                dma((3, 8)), dma((3, 8)), dma((3, 8)), dma((3, 8)), dma((3, LAST_PART + 1)),
            ],
            compiler_params=pltpu.CompilerParams(
                collective_id=0, has_side_effects=True, vmem_limit_bytes=26_500_000),
        )(*tiled, *state, arrays[GRAD_COUNT + 3])
        kept = [pltpu.with_memory_space_constraint(arr, pltpu.VMEM) for arr in kept]
        outs = pl.pallas_call(
            flush,
            out_shape=[jax.ShapeDtypeStruct((EMBED_TILES, 8, WIDTH), bf16)] + small
            + [jax.ShapeDtypeStruct((SHARD_ROWS, LANES), f32)] * 3,
            in_specs=[vmem_spec] * 4,
            out_specs=[any_spec] * 13,
            scratch_shapes=[
                pltpu.VMEM((3840, LANES), f32),
                pltpu.VMEM((2, 3840, LANES), bf16),
                pltpu.VMEM((48, 8, WIDTH), bf16),
                pltpu.VMEM((12, 8, WIDTH), bf16),
                pltpu.VMEM((12, 8, WIDTH), bf16),
                pltpu.VMEM(shapes[8], bf16),
                pltpu.VMEM(shapes[9], bf16),
                dma((FLUSH_PARTS + 16,)),
            ],
            compiler_params=pltpu.CompilerParams(has_side_effects=True, vmem_limit_bytes=4_800_000),
        )(*kept)
        params = []
        for i, dims in enumerate(shapes):
            if i in (1, 2, 3):
                params.append(jnp.swapaxes(outs[i].reshape(dims[0], dims[2], dims[1]), 1, 2))
            else:
                params.append(outs[i].reshape(dims))
        return tuple(params) + tuple(arr.reshape(-1) for arr in outs[GRAD_COUNT:])

    in_specs = tuple([P("dp")] * GRAD_COUNT + [P("dp"), P("dp"), P("dp"), P()])
    out_specs = tuple([P()] * GRAD_COUNT + [P("dp"), P("dp"), P("dp")])
    return jax.shard_map(local_update, mesh=mesh, in_specs=in_specs, out_specs=out_specs, check_vma=False)
```

```python
import functools
import math
import jax
import jax.numpy as jnp
from jax import lax
from jax.experimental import pallas as pl
from jax.experimental.pallas import tpu as pltpu
from jax.sharding import PartitionSpec as P

ADAM_STEP = 7
ADAM_EPS = 1e-8
CLIP_EPS = 1e-6
GRAD_COUNT = 10
MESH = pl.DeviceIdType.MESH

DEVS = 16
OTHERS = range(1, DEVS)
THIRDS = range(3)
PAIR = range(2)
LANES = 128
WIDTH = 640
SHARD_ROWS = 6149
TILE_ROWS = 40
EMBED_TILES = 2048
ALL_TILES = 2460
DECAY_ROWS = 98240
FIRST_TAIL = 13
TAIL_START = (SHARD_ROWS * FIRST_TAIL) // TILE_ROWS
RS_TILES = 52
TAIL_TILES = (SHARD_ROWS * 15) // TILE_ROWS + 3 * RS_TILES - TAIL_START
AG_TILES = 51
PART_TILES = 16
LAST_PART = 3
FLUSH_PARTS = 4
LEAD = 40
G_ROWS = LEAD + 3 * RS_TILES * TILE_ROWS
ORDERS = ((2, 4, 8), (4, 8, 2), (8, 2, 4))


def flip(dev, stride):
    return dev + stride - 2 * stride * lax.rem(dev // stride, 2)


def rs_tiles(k):
    return RS_TILES - k // 2


def rs_start(dev):
    return (SHARD_ROWS * dev) // TILE_ROWS


def ag_start(dev):
    return (SHARD_ROWS * dev + TILE_ROWS - 1) // TILE_ROWS


def flip_mask(dev, order, mask):
    for bit, stride in enumerate(order):
        if mask >> bit & 1:
            dev = flip(dev, stride)
    return dev


SMALL = {}
for _name, _tiles in (("q", 48), ("k", 12), ("v", 12), ("out", 48), ("gate", 96), ("up", 96),
                      ("down", 96), ("norms", 3), ("qk", 1)):
    SMALL[_name] = (EMBED_TILES if not SMALL else sum(SMALL[_last]), _tiles)
    _last = _name
LAYERS = 6
COLS = WIDTH // LANES
OUT_TILES = 48 * RS_TILES
SPARE = 42 * RS_TILES
PIECE_ROWS = RS_TILES * TILE_ROWS
QUARTERS = range(4)
QUARTER = 16


def slot_tiles(slot, k, f):
    index = 36 + f * 3 + k if slot == 3 else (slot * 3 + k) * 4 + f
    return pl.ds(index * RS_TILES, rs_tiles(k))


def sum_rows(k, f):
    return pl.ds((f * 3 + k) * PIECE_ROWS, rs_tiles(k) * TILE_ROWS)


def put_tile(dst, tile, rows, first, stride):
    for j in range(COLS):
        dst[tile, :, LANES * j:LANES * (j + 1)] = rows[pl.ds(first + j, 8, stride=stride), :].astype(jnp.bfloat16)


def pack_wide(src, dst, first_tile, rows, tiles):
    def step(i, _):
        rows[pl.ds(pl.multiple_of(i * 80, 16), 80), :] = src[pl.ds(pl.multiple_of(i * 80, 16), 80), :].astype(jnp.float32)
        for half in PAIR:
            put_tile(dst, first_tile + 2 * i + half, rows, i * 80 + half * 40, COLS)
        return 0

    lax.fori_loop(0, tiles // 2, step, 0)


def pack_narrow(src, dst, first_tile, rows, width):
    folds = LANES // width
    lane = lax.broadcasted_iota(jnp.int32, (8, LANES), 1) // width
    for layer in range(LAYERS):
        block = src[pl.ds(layer * width // 8, width // 8)].astype(jnp.float32).reshape(width, WIDTH)
        rows[pl.ds(layer * WIDTH, WIDTH), :] = jnp.concatenate([block] * folds, axis=0).T
    tiles = LAYERS * width // 8

    def step(t, _):
        for j in range(COLS):
            first = folds * (40 * t + j)
            value = rows[pl.ds(first, 8, stride=folds * COLS), :]
            for fold in range(1, folds):
                value = jnp.where(lane == fold, rows[pl.ds(first + fold, 8, stride=folds * COLS), :], value)
            dst[first_tile + t, :, LANES * j:LANES * (j + 1)] = value.astype(jnp.bfloat16)
        return 0

    lax.fori_loop(0, tiles, step, 0)


def unpack_wide(src, first_tile, dst, rows, tiles):
    def step(i, _):
        for half in PAIR:
            for j in range(COLS):
                rows[pl.ds(i * 80 + half * 40 + j, 8, stride=COLS), :] = src[
                    first_tile + 2 * i + half, :, LANES * j:LANES * (j + 1)].astype(jnp.float32)
        dst[pl.ds(pl.multiple_of(i * 80, 16), 80), :] = rows[pl.ds(pl.multiple_of(i * 80, 16), 80), :].astype(jnp.bfloat16)
        return 0

    lax.fori_loop(0, tiles // 2, step, 0)


def unpack_narrow(src, first_tile, dst, rows, width):
    folds = LANES // width
    tiles = LAYERS * width // 8

    def step(t, _):
        for j in range(COLS):
            value = src[first_tile + t, :, LANES * j:LANES * (j + 1)].astype(jnp.float32)
            for fold in range(folds):
                turned = value if fold == 0 else pltpu.roll(value, LANES - fold * width, 1)
                rows[pl.ds(folds * (40 * t + j) + fold, 8, stride=folds * COLS), :] = turned
        return 0

    lax.fori_loop(0, tiles, step, 0)
    for layer in range(LAYERS):
        block = rows[pl.ds(layer * WIDTH, WIDTH), :].T[:width]
        dst[pl.ds(layer * width // 8, width // 8)] = block.reshape(width // 8, 8, WIDTH).astype(jnp.bfloat16)


def kernel(emb, gq, gk, gv, go, gg, gu, gd, gn, gqk, m_in, v_in, p_in, hyp_in, mom, vel, par, vout, tail,
           s1, r2, r3, ext, hyp, nsend, nrecv, wide_raw, q_raw, k_raw, v_raw, n_raw, qk_raw, n_tiles,
           raw_sem, relay_sem, tail_sem,
           own_sem, r1_send, r1_recv, r2_send, r2_recv, r3_send, r3_recv, st_sem,
           ext_send, ext_recv, n_send, n_recv, ag_send, ag_recv, d2d_send, d2d_recv, last_recv):
    grad = s1.at[pl.ds(0, G_ROWS)]
    me = lax.axis_index("dp")
    partner = flip(me, 1)

    def remote(src, dst, ssem, rsem, dev):
        return pltpu.make_async_remote_copy(
            src_ref=src, dst_ref=dst, send_sem=ssem, recv_sem=rsem, device_id=(dev,), device_id_type=MESH)

    def from_shard(owner, k, make, embed=True, small=True):
        first = rs_start(owner) + k * RS_TILES

        if embed:
            @pl.when(owner < FIRST_TAIL)
            def _():
                make(emb.at[pl.ds(first, rs_tiles(k))]).start()

        if small:
            @pl.when(owner >= FIRST_TAIL)
            def _():
                make(tail.at[pl.ds(first - TAIL_START, rs_tiles(k))]).start()

    def rs_owner(dev, k, f):
        return flip_mask(dev, ORDERS[k], (0 if f >= 2 else 2) + (4 if f % 2 == 0 else 0))

    state = [pltpu.make_async_copy(src, dst, st_sem.at[i])
             for i, (src, dst) in enumerate(((m_in, mom), (v_in, vel), (p_in, par), (hyp_in, hyp)))]

    def load_own(f, embed=True, small=True):
        for k in THIRDS:
            from_shard(rs_owner(me, k, f), k, lambda src, k=k: pltpu.make_async_copy(
                src, vout.at[slot_tiles(3, k, f)], own_sem.at[k, f]), embed, small)

    def first_owner(slot, k, f):
        dev = partner if slot == 2 else flip(me, ORDERS[k][0])
        if slot == 1:
            dev = flip(dev, 1)
        return dev, rs_owner(dev, k, f)

    def send_first(f, embed=True, small=True):
        for slot in THIRDS:
            for k in THIRDS:
                dev, owner = first_owner(slot, k, f)

                def make(src, k=k, slot=slot, dev=dev):
                    return remote(src, vout.at[slot_tiles(slot, k, f)], r1_send.at[slot, k, f],
                                  r1_recv.at[slot, k, f], dev)

                from_shard(owner, k, make, embed, small)

    barrier = pltpu.get_barrier_semaphore()
    near = [flip(me, order[0]) for order in ORDERS]
    near += [flip(dev, 1) for dev in near] + [partner]
    for dev in near:
        pl.semaphore_signal(barrier, inc=1, device_id=(dev,), device_id_type=MESH)
    raw = [pltpu.make_async_copy(src, dst, raw_sem.at[i]) for i, (src, dst) in enumerate((
        (gg, wide_raw.at[0]), (gu, wide_raw.at[1]), (gq, q_raw), (gk, k_raw), (gv, v_raw), (gn, n_raw), (gqk, qk_raw)))]
    for copy in raw:
        copy.start()
    edge = EMBED_TILES - TAIL_START
    relayed = []
    start = SPARE
    for i, (src, first, tiles) in enumerate(((go, SMALL["out"][0], 48), (gd, SMALL["down"][0], 96),
                                             (emb.at[pl.ds(TAIL_START, edge)], TAIL_START, edge))):
        part = vout.at[pl.ds(start, tiles)]
        copy = pltpu.make_async_copy(src, part, relay_sem.at[i])
        copy.start()
        relayed.append((copy, pltpu.make_async_copy(part, tail.at[pl.ds(first - TAIL_START, tiles)], tail_sem.at[i])))
        start += tiles
    for f in PAIR:
        load_own(f, small=False)
    pl.semaphore_wait(barrier, len(near))
    for f in THIRDS:
        send_first(f, small=False)

    for copy, onward in relayed:
        copy.wait()
        onward.start()
    onwards = [onward for _, onward in relayed]

    raw_names = list(SMALL)

    def to_tail(src, name):
        first, tiles = SMALL[name]
        copy = pltpu.make_async_copy(src, tail.at[pl.ds(first - TAIL_START, tiles)], tail_sem.at[3 + raw_names.index(name)])
        copy.start()
        onwards.append(copy)

    spare = start
    for i, name in enumerate(("gate", "up")):
        raw[i].wait()
        pack_wide(wide_raw.at[i], vout, spare, grad, 96)
        to_tail(vout.at[pl.ds(spare, 96)], name)
        onwards.pop().wait()
    for i, (name, src, width) in enumerate((("q", q_raw, 64), ("k", k_raw, 16), ("v", v_raw, 16))):
        raw[2 + i].wait()
        pack_narrow(src, vout, spare, grad, width)
        tiles = SMALL[name][1]
        to_tail(vout.at[pl.ds(spare, tiles)], name)
        spare += tiles
    raw[5].wait()
    raw[6].wait()
    for i in THIRDS:
        n_tiles[i] = jnp.concatenate([n_raw[2 * i].astype(jnp.float32), n_raw[2 * i + 1].astype(jnp.float32)],
                                     axis=0).astype(jnp.bfloat16)
    grad[24:40, :] = jnp.zeros((16, LANES), jnp.float32)
    for layer in range(LAYERS):
        pair = qk_raw[layer].astype(jnp.float32)
        for i in PAIR:
            for half in PAIR:
                row = (2 * layer + i) * 2 + half
                grad[row:row + 1, :] = pair[i:i + 1, LANES * half:LANES * (half + 1)]
    put_tile(n_tiles, 3, grad, 0, COLS)
    to_tail(n_tiles.at[pl.ds(0, 3)], "norms")
    to_tail(n_tiles.at[pl.ds(3, 1)], "qk")
    for copy in onwards:
        copy.wait()
    for f in range(4):
        send_first(f, embed=f == 3)
        load_own(f, embed=f > 1)
    before = lax.rem(me + DEVS - 1, DEVS)
    ext_copies = [remote(src.at[pl.ds(0, TILE_ROWS)], ext.at[i], ext_send.at[i], ext_recv.at[i], before)
                  for i, src in enumerate((m_in, v_in, p_in))]
    for copy in state:
        copy.start()

    def r1_copy(slot, k, f):
        return remote(emb.at[pl.ds(0, rs_tiles(k))], vout.at[slot_tiles(slot, k, f)], r1_send.at[slot, k, f],
                      r1_recv.at[slot, k, f], partner)

    def r2_copy(k, f):
        return remote(s1.at[sum_rows(k, f)], r2.at[k, f, pl.ds(0, sum_rows(k, f).size)], r2_send.at[k, f], r2_recv.at[k, f], flip(me, ORDERS[k][1]))

    def quarter(k, i):
        return i * QUARTER, min((i + 1) * QUARTER, rs_tiles(k))

    def r3_copy(k, i):
        first, end = quarter(k, i)
        rows = (end - first) * TILE_ROWS
        src = pl.ds(sum_rows(k, 2).start + first * TILE_ROWS, rows)
        dst = pl.ds(first * TILE_ROWS, rows)
        return remote(s1.at[src], r3.at[k, dst], r3_send.at[k, i], r3_recv.at[k, i], flip(me, ORDERS[k][2]))

    for f in range(4):
        for k in THIRDS:
            pltpu.make_async_copy(
                emb.at[pl.ds(0, rs_tiles(k))], vout.at[slot_tiles(3, k, f)], own_sem.at[k, f]).wait()
            for slot in (2, 0, 1):
                r1_copy(slot, k, f).wait_recv()

            def add_four(t, _, k=k, f=f):
                a, b, c, d = [vout[slot_tiles(slot, k, f).start + t].astype(jnp.float32) for slot in (3, 2, 0, 1)]
                total = (a + b) + (c + d)
                row = sum_rows(k, f).start + TILE_ROWS * t
                for j in range(COLS):
                    s1[pl.ds(pl.multiple_of(row + 8 * j, 8), 8), :] = total[:, LANES * j:LANES * (j + 1)]
                return 0

            lax.fori_loop(0, rs_tiles(k), add_four, 0, unroll=2)
            if f < 2:
                r2_copy(k, f).start()
    for f in PAIR:
        for k in THIRDS:
            r2_copy(k, f).wait_recv()

            def add_two(t, _, k=k, f=f):
                row = pl.multiple_of(TILE_ROWS * t, 8)
                at = pl.ds(pl.multiple_of(sum_rows(k, 2 + f).start + TILE_ROWS * t, 8), TILE_ROWS)
                s1[at, :] = s1[at, :] + r2[k, f, pl.ds(row, TILE_ROWS), :]
                return 0

            for i in QUARTERS:
                lax.fori_loop(*quarter(k, i), add_two, 0, unroll=2)
                if f == 0:
                    r3_copy(k, i).start()

    shift = LEAD - (SHARD_ROWS * me - TILE_ROWS * rs_start(me))
    for k in THIRDS:
        for f in PAIR:
            r2_copy(k, f).wait_send()
    def squares(i, acc):
        part = grad[pl.ds(pl.multiple_of(i * TILE_ROWS, 8), TILE_ROWS), :]
        return acc + part * part

    def finish(k, t, carry):
        row = pl.multiple_of(TILE_ROWS * t, 8)
        at = pl.ds(pl.multiple_of(sum_rows(k, 3).start + TILE_ROWS * t, 8), TILE_ROWS)
        total = (s1[at, :] + r3[k, pl.ds(row, TILE_ROWS), :]) * (1.0 / DEVS)
        row = shift + TILE_ROWS * (k * RS_TILES + t)
        for j in range(COLS):
            grad[pl.ds(row + j, 8, stride=COLS), :] = total[8 * j:8 * (j + 1), :]
        return carry

    acc = jnp.zeros((TILE_ROWS, LANES), jnp.float32)
    end = (LEAD + SHARD_ROWS) // TILE_ROWS
    for i in QUARTERS:
        for k in THIRDS:
            r3_copy(k, i).wait_recv()
            lax.fori_loop(*quarter(k, i), functools.partial(finish, k), 0, unroll=2)
        for k in THIRDS:
            blocks = [k * RS_TILES + min(q * QUARTER, RS_TILES) + (q % 4 == 0) for q in (i, i + 1)]
            acc = lax.fori_loop(blocks[0], min(blocks[1], end), squares, acc, unroll=3)
    start = end * TILE_ROWS
    total = jnp.sum(acc, axis=0, keepdims=True)
    for row, rows in ((start, 24), (start + 24, 5)):
        part = grad[pl.ds(row, rows), :]
        total = total + jnp.sum(part * part, axis=0, keepdims=True)
    nsend[...] = total

    others = [flip_mask(me, (1, 2, 4, 8), mask) for mask in sorted(OTHERS, key=lambda mask: -(mask // 2).bit_count())]

    def n_copy(i, source):
        return remote(nsend, nrecv.at[source], n_send.at[i], n_recv.at[source], others[i])

    for i in range(len(others)):
        n_copy(i, me).start()
    for copy in ext_copies:
        copy.start()

    for copy in state:
        copy.wait()

    def full(value):
        return jnp.full((8, LANES), value, jnp.float32)

    learn_rate, beta_one, beta_two, decay, max_norm = [full(hyp[i]) for i in range(5)]
    rest_one, rest_two = 1.0 - beta_one, 1.0 - beta_two
    hat_one = 1.0 / (1.0 - lax.integer_pow(beta_one, ADAM_STEP))
    hat_two = 1.0 / (1.0 - lax.integer_pow(beta_two, ADAM_STEP))

    for i, dev in enumerate(others):
        n_copy(i, me).wait_send()
        n_copy(i, dev).wait_recv()
    nrecv[me] = nsend[...]
    total = jnp.sum(jnp.sum(nrecv[...], axis=0), axis=1, keepdims=True)
    clip = jnp.minimum(1.0, max_norm / (jnp.sqrt(jnp.broadcast_to(total, (8, LANES))) + CLIP_EPS))

    def wide(value, rows):
        if rows <= 8:
            return value[:rows]
        return jnp.concatenate([value] * (rows // 8), axis=0)

    def adam(g, m, v, p, first_row, rows):
        clipped = g * wide(clip, rows)
        m = wide(beta_one, rows) * m + wide(rest_one, rows) * clipped
        v = wide(beta_two, rows) * v + wide(rest_two, rows) * (clipped * clipped)
        index = first_row + lax.broadcasted_iota(jnp.int32, (rows, LANES), 0)
        update = (m * wide(hat_one, rows)) / (jnp.sqrt(v * wide(hat_two, rows)) + ADAM_EPS)
        update = update + jnp.where(index < DECAY_ROWS, wide(decay, rows) * p, 0.0)
        return m, v, p - wide(learn_rate, rows) * update

    def adam_rows(row, rows):
        at = pl.ds(row, rows)
        shifted = pl.ds(row + LEAD, rows)
        m, v, p = adam(grad[shifted, :], mom[at, :], vel[at, :], par[at, :], SHARD_ROWS * me + row, rows)
        mom[at, :] = m
        vel[at, :] = v
        par[at, :] = p
        grad[shifted, :] = p

    def adam_block(i, _):
        adam_rows(pl.multiple_of(i * 40, 8), 40)
        return 0

    def ag_sizes(owner, k, run):
        if k < 2:
            run(AG_TILES)
            return
        longer = ag_start(owner + 1) - ag_start(owner) == 3 * AG_TILES + 1

        @pl.when(longer)
        def _():
            run(AG_TILES + 1)

        @pl.when(jnp.logical_not(longer))
        def _():
            run(AG_TILES)

    def ag_each(k, mask, run, dev=me):
        owner = flip_mask(dev, ORDERS[k], mask)
        first = ag_start(owner) + k * AG_TILES
        ag_sizes(owner, k, lambda size: run(vout.at[pl.ds(first, size)], size))

    def ag_link(k, mask, link, start=True):
        dev = flip(me, ORDERS[k][link])
        slot = mask + (1 << link)

        def copy(dst, size):
            return remote(dst, dst, ag_send.at[k, slot], ag_recv.at[k, slot], dev)

        if start:
            ag_each(k, mask, lambda dst, size: copy(dst, size).start())
        pending.append(lambda: ag_each(k, mask, lambda dst, size: copy(dst, size).wait_send()))

    def ag_part(k, mask, i, run):
        owner = flip_mask(me, ORDERS[k], mask)
        first = ag_start(owner) + k * AG_TILES + i * PART_TILES
        if i < LAST_PART:
            run(vout.at[pl.ds(first, PART_TILES)])
        else:
            ag_sizes(owner, k, lambda size: run(vout.at[pl.ds(first, size - LAST_PART * PART_TILES)]))

    def last_copy(k, i, part):
        return remote(part, part, ag_send.at[k, 7], last_recv.at[k, i], flip(me, ORDERS[k][2]))

    def across_copy(k, part):
        return remote(part, part, d2d_send.at[k, 7], d2d_recv.at[k, 7], partner)

    def ag_across(k, mask, start=True):
        def copy(dst, size):
            return remote(dst, dst, d2d_send.at[k, mask], d2d_recv.at[k, mask], partner)

        if start:
            ag_each(k, mask, lambda dst, size: copy(dst, size).start())
        pending.append(lambda: ag_each(k, mask, lambda dst, size: copy(dst, size).wait_send()))

    def ag_arrived(k, mask):
        ag_each(k, mask, lambda dst, size: remote(
            dst, dst, ag_send.at[k, mask], ag_recv.at[k, mask], partner).wait_recv())

    pending = []
    base = LEAD + TILE_ROWS * ag_start(me) - SHARD_ROWS * me

    def own_part(k, skip, count, blocks):
        lax.fori_loop(*blocks, adam_block, 0, unroll=2)
        if k == 2:
            adam_rows(6120, 24)
            adam_rows(6144, 5)
            for copy in ext_copies:
                copy.wait_recv()
            at = pl.ds(LEAD + SHARD_ROWS, TILE_ROWS)
            _, _, p = adam(grad[at, :], ext[0], ext[1], ext[2], SHARD_ROWS * (me + 1), TILE_ROWS)
            grad[at, :] = p
        first = ag_start(me) + k * AG_TILES

        def pack(t, _):
            put_tile(vout, first + t, grad, base + TILE_ROWS * (k * AG_TILES + t), COLS)
            return 0

        lax.fori_loop(skip, skip + (ag_start(me + 1) - first if k == 2 else count), pack, 0)

        def send(size):
            part = vout.at[pl.ds(first + skip, size)]
            for link in THIRDS:
                slot = 1 << link
                remote(part, part, ag_send.at[k, slot], ag_recv.at[k, slot], flip(me, ORDERS[k][link])).start()
            remote(part, part, d2d_send.at[k, 0], d2d_recv.at[k, 0], partner).start()

        if k == 2:
            ag_sizes(me, k, send)
        else:
            send(count)

    own_part(0, 0, 4, (0, 5))
    own_part(0, 4, 12, (5, 17))
    own_part(0, 16, 35, (17, 52))
    own_part(1, 0, AG_TILES, (52, 103))
    own_part(2, 0, None, (103, 153))
    for k in THIRDS:
        for link in THIRDS:
            ag_link(k, 0, link, start=False)
        ag_across(k, 0, start=False)
    for k in THIRDS:
        ag_arrived(k, 1)
        ag_link(k, 1, 1)
        ag_across(k, 1)
    for k in THIRDS:
        ag_link(k, 1, 2)
    for k in THIRDS:
        ag_arrived(k, 2)
        ag_link(k, 2, 2)
        ag_across(k, 2)
    for copy in ext_copies:
        copy.wait_send()
    for f in range(4):
        for k in THIRDS:
            for slot in THIRDS:
                r1_copy(slot, k, f).wait_send()
    for k in THIRDS:
        for i in QUARTERS:
            r3_copy(k, i).wait_send()
    for k in THIRDS:
        ag_arrived(k, 4)
        ag_across(k, 4)
    for k in THIRDS:
        ag_arrived(k, 3)
        for i in range(LAST_PART + 1):
            ag_part(k, 3, i, lambda part, k=k, i=i: last_copy(k, i, part).start())
        ag_across(k, 3)
    for mask in (5, 6):
        for k in THIRDS:
            ag_arrived(k, mask)
            ag_across(k, mask)
    def from_partner(masks):
        for mask in masks:
            for k in THIRDS:
                ag_each(k, mask, lambda dst, size, k=k, mask=mask: remote(
                    dst, dst, d2d_send.at[k, mask], d2d_recv.at[k, mask], partner).wait_recv(), partner)

    from_partner(range(5))
    for wait in pending:
        wait()
    pending.clear()
    for i in range(LAST_PART + 1):
        for k in THIRDS:
            ag_part(k, 7, i, lambda part, k=k, i=i: last_copy(k, i, part).wait_recv())
            ag_part(k, 7, i, lambda part, k=k, i=i: across_copy(k, part).start())
    for k in THIRDS:
        ag_link(k, 3, 2, start=False)
        ag_across(k, 7, start=False)
    from_partner(range(5, 8))
    for wait in pending:
        wait()


def flush(mom, vel, par, vout, embed, oq, ok, ov, oo, og, ou, od, on, oqk, m_out, v_out, p_out,
          rows, wide_out, q_out, k_out, v_new, n_out, qk_out, sem):
    copies = []

    def send(src, dst):
        copy = pltpu.make_async_copy(src, dst, sem.at[len(copies)])
        copy.start()
        copies.append(copy)

    for i in range(FLUSH_PARTS):
        part = pl.ds(i * (EMBED_TILES // FLUSH_PARTS), EMBED_TILES // FLUSH_PARTS)
        send(vout.at[part], embed.at[part])
    for src, dst in ((mom, m_out), (vel, v_out), (par, p_out)):
        send(src, dst)
    for name, dst in (("out", oo), ("down", od)):
        send(vout.at[pl.ds(*SMALL[name])], dst)
    for i, (name, dst) in enumerate((("gate", og), ("up", ou))):
        unpack_wide(vout, SMALL[name][0], wide_out.at[i], rows, 96)
        send(wide_out.at[i], dst)
    for name, block, dst, width in (("q", q_out, oq, 64), ("k", k_out, ok, 16), ("v", v_new, ov, 16)):
        unpack_narrow(vout, SMALL[name][0], block, rows, width)
        send(block, dst)
    for i in THIRDS:
        tile = vout[SMALL["norms"][0] + i].astype(jnp.float32)
        n_out[2 * i] = tile[0:4].astype(jnp.bfloat16)
        n_out[2 * i + 1] = tile[4:8].astype(jnp.bfloat16)
    send(n_out, on)
    for j in range(COLS):
        rows[pl.ds(j, 8, stride=COLS), :] = vout[SMALL["qk"][0], :, LANES * j:LANES * (j + 1)].astype(jnp.float32)
    for layer in range(LAYERS):
        four = rows[4 * layer:4 * layer + 4, :]
        pair = [jnp.concatenate([four[2 * i:2 * i + 1], four[2 * i + 1:2 * i + 2]], axis=1) for i in PAIR]
        qk_out[layer] = jnp.concatenate(pair, axis=0).astype(jnp.bfloat16)
    send(qk_out, oqk)
    for copy in copies:
        copy.wait()


def solution(mesh):
    def local_update(*arrays):
        grads = [arr.reshape(arr.shape[1:]) for arr in arrays[:GRAD_COUNT]]
        state = [arr.reshape(SHARD_ROWS, LANES) for arr in arrays[GRAD_COUNT:GRAD_COUNT + 3]]
        shapes = [grad_arr.shape for grad_arr in grads]
        any_spec = pl.BlockSpec(memory_space=pl.ANY)
        vmem_spec = pl.BlockSpec(memory_space=pltpu.VMEM)
        dma = pltpu.SemaphoreType.DMA
        bf16, f32 = jnp.bfloat16, jnp.float32
        tiled = []
        for i, grad_arr in enumerate(grads[:8]):
            if i in (1, 2, 3):
                grad_arr = jnp.swapaxes(grad_arr, 1, 2)
            tiled.append(grad_arr.reshape(-1, LANES) if i in (5, 6) else grad_arr.reshape(-1, 8, WIDTH))
        tiled += grads[8:]
        small = [jax.ShapeDtypeStruct(arr.shape, bf16) for arr in tiled[1:]]
        *kept, _ = pl.pallas_call(
            kernel,
            out_shape=[pltpu.VMEM((SHARD_ROWS, LANES), f32)] * 3
            + [pltpu.VMEM((OUT_TILES, 8, WIDTH), bf16)]
            + [pltpu.HBM((TAIL_TILES, 8, WIDTH), bf16)],
            in_specs=[any_spec] * 14,
            out_specs=[vmem_spec] * 4 + [any_spec],
            scratch_shapes=[
                pltpu.VMEM((3 * 4 * PIECE_ROWS, LANES), f32),
                pltpu.VMEM((3, 2, PIECE_ROWS, LANES), f32),
                pltpu.VMEM((3, PIECE_ROWS, LANES), f32),
                pltpu.VMEM((3, TILE_ROWS, LANES), f32),
                pltpu.SMEM((5,), f32),
                pltpu.VMEM((1, LANES), f32),
                pltpu.VMEM((DEVS, 1, LANES), f32),
                pltpu.VMEM((2, 3840, LANES), bf16),
                pltpu.VMEM((48, 8, WIDTH), bf16),
                pltpu.VMEM((12, 8, WIDTH), bf16),
                pltpu.VMEM((12, 8, WIDTH), bf16),
                pltpu.VMEM(shapes[8], bf16),
                pltpu.VMEM(shapes[9], bf16),
                pltpu.VMEM((4, 8, WIDTH), bf16),
                dma((7,)), dma((3,)), dma((3 + len(SMALL),)),
                dma((3, 4)), dma((3, 3, 4)), dma((3, 3, 4)), dma((3, 2)), dma((3, 2)), dma((3, 4)), dma((3, 4)),
                dma((4,)), dma((3,)), dma((3,)), dma((DEVS,)), dma((DEVS,)),
                dma((3, 8)), dma((3, 8)), dma((3, 8)), dma((3, 8)), dma((3, LAST_PART + 1)),
            ],
            compiler_params=pltpu.CompilerParams(
                collective_id=0, has_side_effects=True, vmem_limit_bytes=26_500_000),
        )(*tiled, *state, arrays[GRAD_COUNT + 3])
        kept = [pltpu.with_memory_space_constraint(arr, pltpu.VMEM) for arr in kept]
        outs = pl.pallas_call(
            flush,
            out_shape=[jax.ShapeDtypeStruct((EMBED_TILES, 8, WIDTH), bf16)] + small
            + [jax.ShapeDtypeStruct((SHARD_ROWS, LANES), f32)] * 3,
            in_specs=[vmem_spec] * 4,
            out_specs=[any_spec] * 13,
            scratch_shapes=[
                pltpu.VMEM((3840, LANES), f32),
                pltpu.VMEM((2, 3840, LANES), bf16),
                pltpu.VMEM((48, 8, WIDTH), bf16),
                pltpu.VMEM((12, 8, WIDTH), bf16),
                pltpu.VMEM((12, 8, WIDTH), bf16),
                pltpu.VMEM(shapes[8], bf16),
                pltpu.VMEM(shapes[9], bf16),
                dma((FLUSH_PARTS + 16,)),
            ],
            compiler_params=pltpu.CompilerParams(has_side_effects=True, vmem_limit_bytes=4_800_000),
        )(*kept)
        params = []
        for i, dims in enumerate(shapes):
            if i in (1, 2, 3):
                params.append(jnp.swapaxes(outs[i].reshape(dims[0], dims[2], dims[1]), 1, 2))
            else:
                params.append(outs[i].reshape(dims))
        return tuple(params) + tuple(arr.reshape(-1) for arr in outs[GRAD_COUNT:])

    in_specs = tuple([P("dp")] * GRAD_COUNT + [P("dp"), P("dp"), P("dp"), P()])
    out_specs = tuple([P()] * GRAD_COUNT + [P("dp"), P("dp"), P("dp")])
    return jax.shard_map(local_update, mesh=mesh, in_specs=in_specs, out_specs=out_specs, check_vma=False)
```

```python
import functools
import math
import jax
import jax.numpy as jnp
from jax import lax
from jax.experimental import pallas as pl
from jax.experimental.pallas import tpu as pltpu
from jax.sharding import PartitionSpec as P

ADAM_STEP = 7
ADAM_EPS = 1e-8
CLIP_EPS = 1e-6
GRAD_COUNT = 10
MESH = pl.DeviceIdType.MESH

DEVS = 16
OTHERS = range(1, DEVS)
THIRDS = range(3)
PAIR = range(2)
LANES = 128
WIDTH = 640
SHARD_ROWS = 6149
TILE_ROWS = 40
EMBED_TILES = 2048
ALL_TILES = 2460
DECAY_ROWS = 98240
FIRST_TAIL = 13
TAIL_START = (SHARD_ROWS * FIRST_TAIL) // TILE_ROWS
RS_TILES = 52
TAIL_TILES = (SHARD_ROWS * 15) // TILE_ROWS + 3 * RS_TILES - TAIL_START
AG_TILES = 51
PART_STARTS = (0, 24, 40, 48)
LAST_PART = 3
FLUSH_PARTS = 4
LEAD = 40
G_ROWS = LEAD + 3 * RS_TILES * TILE_ROWS
ORDERS = ((2, 4, 8), (4, 8, 2), (8, 2, 4))


def flip(dev, stride):
    return dev + stride - 2 * stride * lax.rem(dev // stride, 2)


def rs_tiles(k):
    return RS_TILES - k // 2


def rs_start(dev):
    return (SHARD_ROWS * dev) // TILE_ROWS


def ag_start(dev):
    return (SHARD_ROWS * dev + TILE_ROWS - 1) // TILE_ROWS


def flip_mask(dev, order, mask):
    for bit, stride in enumerate(order):
        if mask >> bit & 1:
            dev = flip(dev, stride)
    return dev


SMALL = {}
for _name, _tiles in (("q", 48), ("k", 12), ("v", 12), ("out", 48), ("gate", 96), ("up", 96),
                      ("down", 96), ("norms", 3), ("qk", 1)):
    SMALL[_name] = (EMBED_TILES if not SMALL else sum(SMALL[_last]), _tiles)
    _last = _name
LAYERS = 6
COLS = WIDTH // LANES
OUT_TILES = 48 * RS_TILES
SPARE = 42 * RS_TILES
PIECE_ROWS = RS_TILES * TILE_ROWS
QUARTERS = range(4)
QUARTER = 16


def slot_tiles(slot, k, f):
    index = 36 + f * 3 + k if slot == 3 else (slot * 3 + k) * 4 + f
    return pl.ds(index * RS_TILES, rs_tiles(k))


def sum_rows(k, f):
    return pl.ds((f * 3 + k) * PIECE_ROWS, rs_tiles(k) * TILE_ROWS)


def put_tile(dst, tile, rows, first, stride):
    for j in range(COLS):
        dst[tile, :, LANES * j:LANES * (j + 1)] = rows[pl.ds(first + j, 8, stride=stride), :].astype(jnp.bfloat16)


def pack_wide(src, dst, first_tile, rows, tiles):
    def step(i, _):
        rows[pl.ds(pl.multiple_of(i * 80, 16), 80), :] = src[pl.ds(pl.multiple_of(i * 80, 16), 80), :].astype(jnp.float32)
        for half in PAIR:
            put_tile(dst, first_tile + 2 * i + half, rows, i * 80 + half * 40, COLS)
        return 0

    lax.fori_loop(0, tiles // 2, step, 0)


def pack_narrow(src, dst, first_tile, rows, width):
    folds = LANES // width
    lane = lax.broadcasted_iota(jnp.int32, (8, LANES), 1) // width
    for layer in range(LAYERS):
        block = src[pl.ds(layer * width // 8, width // 8)].astype(jnp.float32).reshape(width, WIDTH)
        rows[pl.ds(layer * WIDTH, WIDTH), :] = jnp.concatenate([block] * folds, axis=0).T
    tiles = LAYERS * width // 8

    def step(t, _):
        for j in range(COLS):
            first = folds * (40 * t + j)
            value = rows[pl.ds(first, 8, stride=folds * COLS), :]
            for fold in range(1, folds):
                value = jnp.where(lane == fold, rows[pl.ds(first + fold, 8, stride=folds * COLS), :], value)
            dst[first_tile + t, :, LANES * j:LANES * (j + 1)] = value.astype(jnp.bfloat16)
        return 0

    lax.fori_loop(0, tiles, step, 0)


def unpack_wide(src, first_tile, dst, rows, tiles):
    def step(i, _):
        for half in PAIR:
            for j in range(COLS):
                rows[pl.ds(i * 80 + half * 40 + j, 8, stride=COLS), :] = src[
                    first_tile + 2 * i + half, :, LANES * j:LANES * (j + 1)].astype(jnp.float32)
        dst[pl.ds(pl.multiple_of(i * 80, 16), 80), :] = rows[pl.ds(pl.multiple_of(i * 80, 16), 80), :].astype(jnp.bfloat16)
        return 0

    lax.fori_loop(0, tiles // 2, step, 0)


def unpack_narrow(src, first_tile, dst, rows, width):
    folds = LANES // width
    tiles = LAYERS * width // 8

    def step(t, _):
        for j in range(COLS):
            value = src[first_tile + t, :, LANES * j:LANES * (j + 1)].astype(jnp.float32)
            for fold in range(folds):
                turned = value if fold == 0 else pltpu.roll(value, LANES - fold * width, 1)
                rows[pl.ds(folds * (40 * t + j) + fold, 8, stride=folds * COLS), :] = turned
        return 0

    lax.fori_loop(0, tiles, step, 0)
    for layer in range(LAYERS):
        block = rows[pl.ds(layer * WIDTH, WIDTH), :].T[:width]
        dst[pl.ds(layer * width // 8, width // 8)] = block.reshape(width // 8, 8, WIDTH).astype(jnp.bfloat16)


def kernel(emb, gq, gk, gv, go, gg, gu, gd, gn, gqk, m_in, v_in, p_in, hyp_in, mom, vel, par, vout, tail,
           s1, r2, r3, ext, hyp, nsend, nrecv, wide_raw, q_raw, k_raw, v_raw, n_raw, qk_raw, n_tiles,
           raw_sem, relay_sem, tail_sem,
           own_sem, r1_send, r1_recv, r2_send, r2_recv, r3_send, r3_recv, st_sem,
           ext_send, ext_recv, n_send, n_recv, ag_send, ag_recv, d2d_send, d2d_recv, last_recv):
    grad = s1.at[pl.ds(0, G_ROWS)]
    me = lax.axis_index("dp")
    partner = flip(me, 1)

    def remote(src, dst, ssem, rsem, dev):
        return pltpu.make_async_remote_copy(
            src_ref=src, dst_ref=dst, send_sem=ssem, recv_sem=rsem, device_id=(dev,), device_id_type=MESH)

    def from_shard(owner, k, make, embed=True, small=True):
        first = rs_start(owner) + k * RS_TILES

        if embed:
            @pl.when(owner < FIRST_TAIL)
            def _():
                make(emb.at[pl.ds(first, rs_tiles(k))]).start()

        if small:
            @pl.when(owner >= FIRST_TAIL)
            def _():
                make(tail.at[pl.ds(first - TAIL_START, rs_tiles(k))]).start()

    def rs_owner(dev, k, f):
        return flip_mask(dev, ORDERS[k], (0 if f >= 2 else 2) + (4 if f % 2 == 0 else 0))

    state = [pltpu.make_async_copy(src, dst, st_sem.at[i])
             for i, (src, dst) in enumerate(((m_in, mom), (v_in, vel), (p_in, par), (hyp_in, hyp)))]

    def load_own(f, embed=True, small=True):
        for k in THIRDS:
            from_shard(rs_owner(me, k, f), k, lambda src, k=k: pltpu.make_async_copy(
                src, vout.at[slot_tiles(3, k, f)], own_sem.at[k, f]), embed, small)

    def first_owner(slot, k, f):
        dev = partner if slot == 2 else flip(me, ORDERS[k][0])
        if slot == 1:
            dev = flip(dev, 1)
        return dev, rs_owner(dev, k, f)

    def send_first(f, embed=True, small=True):
        for slot in THIRDS:
            for k in THIRDS:
                dev, owner = first_owner(slot, k, f)

                def make(src, k=k, slot=slot, dev=dev):
                    return remote(src, vout.at[slot_tiles(slot, k, f)], r1_send.at[slot, k, f],
                                  r1_recv.at[slot, k, f], dev)

                from_shard(owner, k, make, embed, small)

    barrier = pltpu.get_barrier_semaphore()
    near = [flip(me, order[0]) for order in ORDERS]
    near += [flip(dev, 1) for dev in near] + [partner]
    for dev in near:
        pl.semaphore_signal(barrier, inc=1, device_id=(dev,), device_id_type=MESH)
    raw = [pltpu.make_async_copy(src, dst, raw_sem.at[i]) for i, (src, dst) in enumerate((
        (gg, wide_raw.at[0]), (gu, wide_raw.at[1]), (gq, q_raw), (gk, k_raw), (gv, v_raw), (gn, n_raw), (gqk, qk_raw)))]
    for copy in raw:
        copy.start()
    edge = EMBED_TILES - TAIL_START
    relayed = []
    start = SPARE
    for i, (src, first, tiles) in enumerate(((go, SMALL["out"][0], 48), (gd, SMALL["down"][0], 96),
                                             (emb.at[pl.ds(TAIL_START, edge)], TAIL_START, edge))):
        part = vout.at[pl.ds(start, tiles)]
        copy = pltpu.make_async_copy(src, part, relay_sem.at[i])
        copy.start()
        relayed.append((copy, pltpu.make_async_copy(part, tail.at[pl.ds(first - TAIL_START, tiles)], tail_sem.at[i])))
        start += tiles
    for f in PAIR:
        load_own(f, small=False)
    pl.semaphore_wait(barrier, len(near))
    for f in THIRDS:
        send_first(f, small=False)

    for copy, onward in relayed:
        copy.wait()
        onward.start()
    onwards = [onward for _, onward in relayed]

    raw_names = list(SMALL)

    def to_tail(src, name):
        first, tiles = SMALL[name]
        copy = pltpu.make_async_copy(src, tail.at[pl.ds(first - TAIL_START, tiles)], tail_sem.at[3 + raw_names.index(name)])
        copy.start()
        onwards.append(copy)

    spare = start
    for i, name in enumerate(("gate", "up")):
        raw[i].wait()
        pack_wide(wide_raw.at[i], vout, spare, grad, 96)
        to_tail(vout.at[pl.ds(spare, 96)], name)
        onwards.pop().wait()
    for i, (name, src, width) in enumerate((("q", q_raw, 64), ("k", k_raw, 16), ("v", v_raw, 16))):
        raw[2 + i].wait()
        pack_narrow(src, vout, spare, grad, width)
        tiles = SMALL[name][1]
        to_tail(vout.at[pl.ds(spare, tiles)], name)
        spare += tiles
    raw[5].wait()
    raw[6].wait()
    for i in THIRDS:
        n_tiles[i] = jnp.concatenate([n_raw[2 * i].astype(jnp.float32), n_raw[2 * i + 1].astype(jnp.float32)],
                                     axis=0).astype(jnp.bfloat16)
    grad[24:40, :] = jnp.zeros((16, LANES), jnp.float32)
    for layer in range(LAYERS):
        pair = qk_raw[layer].astype(jnp.float32)
        for i in PAIR:
            for half in PAIR:
                row = (2 * layer + i) * 2 + half
                grad[row:row + 1, :] = pair[i:i + 1, LANES * half:LANES * (half + 1)]
    put_tile(n_tiles, 3, grad, 0, COLS)
    to_tail(n_tiles.at[pl.ds(0, 3)], "norms")
    to_tail(n_tiles.at[pl.ds(3, 1)], "qk")
    for copy in onwards:
        copy.wait()
    for f in range(4):
        send_first(f, embed=f == 3)
        load_own(f, embed=f > 1)
    before = lax.rem(me + DEVS - 1, DEVS)
    ext_copies = [remote(src.at[pl.ds(0, TILE_ROWS)], ext.at[i], ext_send.at[i], ext_recv.at[i], before)
                  for i, src in enumerate((m_in, v_in, p_in))]
    for copy in state:
        copy.start()

    def r1_copy(slot, k, f):
        return remote(emb.at[pl.ds(0, rs_tiles(k))], vout.at[slot_tiles(slot, k, f)], r1_send.at[slot, k, f],
                      r1_recv.at[slot, k, f], partner)

    def r2_copy(k, f):
        return remote(s1.at[sum_rows(k, f)], r2.at[k, f, pl.ds(0, sum_rows(k, f).size)], r2_send.at[k, f], r2_recv.at[k, f], flip(me, ORDERS[k][1]))

    def quarter(k, i):
        return i * QUARTER, min((i + 1) * QUARTER, rs_tiles(k))

    def r3_copy(k, i):
        first, end = quarter(k, i)
        rows = (end - first) * TILE_ROWS
        src = pl.ds(sum_rows(k, 2).start + first * TILE_ROWS, rows)
        dst = pl.ds(first * TILE_ROWS, rows)
        return remote(s1.at[src], r3.at[k, dst], r3_send.at[k, i], r3_recv.at[k, i], flip(me, ORDERS[k][2]))

    for f in range(4):
        for k in THIRDS:
            pltpu.make_async_copy(
                emb.at[pl.ds(0, rs_tiles(k))], vout.at[slot_tiles(3, k, f)], own_sem.at[k, f]).wait()
            for slot in (2, 0, 1):
                r1_copy(slot, k, f).wait_recv()

            def add_four(t, _, k=k, f=f):
                a, b, c, d = [vout[slot_tiles(slot, k, f).start + t].astype(jnp.float32) for slot in (3, 2, 0, 1)]
                total = (a + b) + (c + d)
                row = sum_rows(k, f).start + TILE_ROWS * t
                for j in range(COLS):
                    s1[pl.ds(pl.multiple_of(row + 8 * j, 8), 8), :] = total[:, LANES * j:LANES * (j + 1)]
                return 0

            lax.fori_loop(0, rs_tiles(k), add_four, 0, unroll=2)
            if f < 2:
                r2_copy(k, f).start()
    for f in PAIR:
        for k in THIRDS:
            r2_copy(k, f).wait_recv()

            def add_two(t, _, k=k, f=f):
                row = pl.multiple_of(TILE_ROWS * t, 8)
                at = pl.ds(pl.multiple_of(sum_rows(k, 2 + f).start + TILE_ROWS * t, 8), TILE_ROWS)
                s1[at, :] = s1[at, :] + r2[k, f, pl.ds(row, TILE_ROWS), :]
                return 0

            for i in QUARTERS:
                lax.fori_loop(*quarter(k, i), add_two, 0, unroll=2)
                if f == 0:
                    r3_copy(k, i).start()

    shift = LEAD - (SHARD_ROWS * me - TILE_ROWS * rs_start(me))
    for k in THIRDS:
        for f in PAIR:
            r2_copy(k, f).wait_send()
    def squares(i, acc):
        part = grad[pl.ds(pl.multiple_of(i * TILE_ROWS, 8), TILE_ROWS), :]
        return acc + part * part

    def finish(k, t, carry):
        row = pl.multiple_of(TILE_ROWS * t, 8)
        at = pl.ds(pl.multiple_of(sum_rows(k, 3).start + TILE_ROWS * t, 8), TILE_ROWS)
        total = (s1[at, :] + r3[k, pl.ds(row, TILE_ROWS), :]) * (1.0 / DEVS)
        row = shift + TILE_ROWS * (k * RS_TILES + t)
        for j in range(COLS):
            grad[pl.ds(row + j, 8, stride=COLS), :] = total[8 * j:8 * (j + 1), :]
        return carry

    acc = jnp.zeros((TILE_ROWS, LANES), jnp.float32)
    end = (LEAD + SHARD_ROWS) // TILE_ROWS
    for i in QUARTERS:
        for k in THIRDS:
            r3_copy(k, i).wait_recv()
            lax.fori_loop(*quarter(k, i), functools.partial(finish, k), 0, unroll=2)
        for k in THIRDS:
            blocks = [k * RS_TILES + min(q * QUARTER, RS_TILES) + (q % 4 == 0) for q in (i, i + 1)]
            acc = lax.fori_loop(blocks[0], min(blocks[1], end), squares, acc, unroll=3)
    start = end * TILE_ROWS
    total = jnp.sum(acc, axis=0, keepdims=True)
    for row, rows in ((start, 24), (start + 24, 5)):
        part = grad[pl.ds(row, rows), :]
        total = total + jnp.sum(part * part, axis=0, keepdims=True)
    nsend[...] = total

    others = [flip_mask(me, (1, 2, 4, 8), mask) for mask in sorted(OTHERS, key=lambda mask: -(mask // 2).bit_count())]

    def n_copy(i, source):
        return remote(nsend, nrecv.at[source], n_send.at[i], n_recv.at[source], others[i])

    for i in range(len(others)):
        n_copy(i, me).start()
    for copy in ext_copies:
        copy.start()

    for copy in state:
        copy.wait()

    def full(value):
        return jnp.full((8, LANES), value, jnp.float32)

    learn_rate, beta_one, beta_two, decay, max_norm = [full(hyp[i]) for i in range(5)]
    rest_one, rest_two = 1.0 - beta_one, 1.0 - beta_two
    hat_one = 1.0 / (1.0 - lax.integer_pow(beta_one, ADAM_STEP))
    hat_two = 1.0 / (1.0 - lax.integer_pow(beta_two, ADAM_STEP))

    for i, dev in enumerate(others):
        n_copy(i, me).wait_send()
        n_copy(i, dev).wait_recv()
    nrecv[me] = nsend[...]
    total = jnp.sum(jnp.sum(nrecv[...], axis=0), axis=1, keepdims=True)
    clip = jnp.minimum(1.0, max_norm / (jnp.sqrt(jnp.broadcast_to(total, (8, LANES))) + CLIP_EPS))

    def wide(value, rows):
        if rows <= 8:
            return value[:rows]
        return jnp.concatenate([value] * (rows // 8), axis=0)

    def adam(g, m, v, p, first_row, rows):
        clipped = g * wide(clip, rows)
        m = wide(beta_one, rows) * m + wide(rest_one, rows) * clipped
        v = wide(beta_two, rows) * v + wide(rest_two, rows) * (clipped * clipped)
        index = first_row + lax.broadcasted_iota(jnp.int32, (rows, LANES), 0)
        update = (m * wide(hat_one, rows)) / (jnp.sqrt(v * wide(hat_two, rows)) + ADAM_EPS)
        update = update + jnp.where(index < DECAY_ROWS, wide(decay, rows) * p, 0.0)
        return m, v, p - wide(learn_rate, rows) * update

    def adam_rows(row, rows):
        at = pl.ds(row, rows)
        shifted = pl.ds(row + LEAD, rows)
        m, v, p = adam(grad[shifted, :], mom[at, :], vel[at, :], par[at, :], SHARD_ROWS * me + row, rows)
        mom[at, :] = m
        vel[at, :] = v
        par[at, :] = p
        grad[shifted, :] = p

    def adam_block(i, _):
        adam_rows(pl.multiple_of(i * 40, 8), 40)
        return 0

    def ag_sizes(owner, k, run):
        if k < 2:
            run(AG_TILES)
            return
        longer = ag_start(owner + 1) - ag_start(owner) == 3 * AG_TILES + 1

        @pl.when(longer)
        def _():
            run(AG_TILES + 1)

        @pl.when(jnp.logical_not(longer))
        def _():
            run(AG_TILES)

    def ag_each(k, mask, run, dev=me):
        owner = flip_mask(dev, ORDERS[k], mask)
        first = ag_start(owner) + k * AG_TILES
        ag_sizes(owner, k, lambda size: run(vout.at[pl.ds(first, size)], size))

    def ag_link(k, mask, link, start=True):
        dev = flip(me, ORDERS[k][link])
        slot = mask + (1 << link)

        def copy(dst, size):
            return remote(dst, dst, ag_send.at[k, slot], ag_recv.at[k, slot], dev)

        if start:
            ag_each(k, mask, lambda dst, size: copy(dst, size).start())
        pending.append(lambda: ag_each(k, mask, lambda dst, size: copy(dst, size).wait_send()))

    def ag_part(k, mask, i, run):
        owner = flip_mask(me, ORDERS[k], mask)
        first = ag_start(owner) + k * AG_TILES + PART_STARTS[i]
        if i < LAST_PART:
            run(vout.at[pl.ds(first, PART_STARTS[i + 1] - PART_STARTS[i])])
        else:
            ag_sizes(owner, k, lambda size: run(vout.at[pl.ds(first, size - PART_STARTS[i])]))

    def last_copy(k, i, part):
        return remote(part, part, ag_send.at[k, 7], last_recv.at[k, i], flip(me, ORDERS[k][2]))

    def across_copy(k, part):
        return remote(part, part, d2d_send.at[k, 7], d2d_recv.at[k, 7], partner)

    def ag_across(k, mask, start=True):
        def copy(dst, size):
            return remote(dst, dst, d2d_send.at[k, mask], d2d_recv.at[k, mask], partner)

        if start:
            ag_each(k, mask, lambda dst, size: copy(dst, size).start())
        pending.append(lambda: ag_each(k, mask, lambda dst, size: copy(dst, size).wait_send()))

    def ag_arrived(k, mask):
        ag_each(k, mask, lambda dst, size: remote(
            dst, dst, ag_send.at[k, mask], ag_recv.at[k, mask], partner).wait_recv())

    pending = []
    base = LEAD + TILE_ROWS * ag_start(me) - SHARD_ROWS * me

    def own_part(k, skip, count, blocks):
        lax.fori_loop(*blocks, adam_block, 0, unroll=2)
        if k == 2:
            adam_rows(6120, 24)
            adam_rows(6144, 5)
            for copy in ext_copies:
                copy.wait_recv()
            at = pl.ds(LEAD + SHARD_ROWS, TILE_ROWS)
            _, _, p = adam(grad[at, :], ext[0], ext[1], ext[2], SHARD_ROWS * (me + 1), TILE_ROWS)
            grad[at, :] = p
        first = ag_start(me) + k * AG_TILES

        def pack(t, _):
            put_tile(vout, first + t, grad, base + TILE_ROWS * (k * AG_TILES + t), COLS)
            return 0

        lax.fori_loop(skip, skip + (ag_start(me + 1) - first if k == 2 else count), pack, 0)

        def send(size):
            part = vout.at[pl.ds(first + skip, size)]
            for link in THIRDS:
                slot = 1 << link
                remote(part, part, ag_send.at[k, slot], ag_recv.at[k, slot], flip(me, ORDERS[k][link])).start()
            remote(part, part, d2d_send.at[k, 0], d2d_recv.at[k, 0], partner).start()

        if k == 2:
            ag_sizes(me, k, send)
        else:
            send(count)

    own_part(0, 0, 4, (0, 5))
    own_part(0, 4, 12, (5, 17))
    own_part(0, 16, 35, (17, 52))
    own_part(1, 0, AG_TILES, (52, 103))
    own_part(2, 0, None, (103, 153))
    for k in THIRDS:
        for link in THIRDS:
            ag_link(k, 0, link, start=False)
        ag_across(k, 0, start=False)
    for k in THIRDS:
        ag_arrived(k, 1)
        ag_link(k, 1, 1)
        ag_across(k, 1)
    for k in THIRDS:
        ag_link(k, 1, 2)
    for k in THIRDS:
        ag_arrived(k, 2)
        ag_link(k, 2, 2)
        ag_across(k, 2)
    for copy in ext_copies:
        copy.wait_send()
    for f in range(4):
        for k in THIRDS:
            for slot in THIRDS:
                r1_copy(slot, k, f).wait_send()
    for k in THIRDS:
        for i in QUARTERS:
            r3_copy(k, i).wait_send()
    for k in THIRDS:
        ag_arrived(k, 4)
        ag_across(k, 4)
    for k in THIRDS:
        ag_arrived(k, 3)
        for i in range(LAST_PART + 1):
            ag_part(k, 3, i, lambda part, k=k, i=i: last_copy(k, i, part).start())
        ag_across(k, 3)
    for mask in (5, 6):
        for k in THIRDS:
            ag_arrived(k, mask)
            ag_across(k, mask)
    def from_partner(masks):
        for mask in masks:
            for k in THIRDS:
                ag_each(k, mask, lambda dst, size, k=k, mask=mask: remote(
                    dst, dst, d2d_send.at[k, mask], d2d_recv.at[k, mask], partner).wait_recv(), partner)

    from_partner(range(5))
    for wait in pending:
        wait()
    pending.clear()
    for i in range(LAST_PART + 1):
        for k in THIRDS:
            ag_part(k, 7, i, lambda part, k=k, i=i: last_copy(k, i, part).wait_recv())
            ag_part(k, 7, i, lambda part, k=k, i=i: across_copy(k, part).start())
    for k in THIRDS:
        ag_link(k, 3, 2, start=False)
        ag_across(k, 7, start=False)
    from_partner(range(5, 8))
    for wait in pending:
        wait()


def flush(mom, vel, par, vout, embed, oq, ok, ov, oo, og, ou, od, on, oqk, m_out, v_out, p_out,
          rows, wide_out, q_out, k_out, v_new, n_out, qk_out, sem):
    copies = []

    def send(src, dst):
        copy = pltpu.make_async_copy(src, dst, sem.at[len(copies)])
        copy.start()
        copies.append(copy)

    for i in range(FLUSH_PARTS):
        part = pl.ds(i * (EMBED_TILES // FLUSH_PARTS), EMBED_TILES // FLUSH_PARTS)
        send(vout.at[part], embed.at[part])
    for src, dst in ((mom, m_out), (vel, v_out), (par, p_out)):
        send(src, dst)
    for name, dst in (("out", oo), ("down", od)):
        send(vout.at[pl.ds(*SMALL[name])], dst)
    for i, (name, dst) in enumerate((("gate", og), ("up", ou))):
        unpack_wide(vout, SMALL[name][0], wide_out.at[i], rows, 96)
        send(wide_out.at[i], dst)
    for name, block, dst, width in (("q", q_out, oq, 64), ("k", k_out, ok, 16), ("v", v_new, ov, 16)):
        unpack_narrow(vout, SMALL[name][0], block, rows, width)
        send(block, dst)
    for i in THIRDS:
        tile = vout[SMALL["norms"][0] + i].astype(jnp.float32)
        n_out[2 * i] = tile[0:4].astype(jnp.bfloat16)
        n_out[2 * i + 1] = tile[4:8].astype(jnp.bfloat16)
    send(n_out, on)
    for j in range(COLS):
        rows[pl.ds(j, 8, stride=COLS), :] = vout[SMALL["qk"][0], :, LANES * j:LANES * (j + 1)].astype(jnp.float32)
    for layer in range(LAYERS):
        four = rows[4 * layer:4 * layer + 4, :]
        pair = [jnp.concatenate([four[2 * i:2 * i + 1], four[2 * i + 1:2 * i + 2]], axis=1) for i in PAIR]
        qk_out[layer] = jnp.concatenate(pair, axis=0).astype(jnp.bfloat16)
    send(qk_out, oqk)
    for copy in copies:
        copy.wait()


def solution(mesh):
    def local_update(*arrays):
        grads = [arr.reshape(arr.shape[1:]) for arr in arrays[:GRAD_COUNT]]
        state = [arr.reshape(SHARD_ROWS, LANES) for arr in arrays[GRAD_COUNT:GRAD_COUNT + 3]]
        shapes = [grad_arr.shape for grad_arr in grads]
        any_spec = pl.BlockSpec(memory_space=pl.ANY)
        vmem_spec = pl.BlockSpec(memory_space=pltpu.VMEM)
        dma = pltpu.SemaphoreType.DMA
        bf16, f32 = jnp.bfloat16, jnp.float32
        tiled = []
        for i, grad_arr in enumerate(grads[:8]):
            if i in (1, 2, 3):
                grad_arr = jnp.swapaxes(grad_arr, 1, 2)
            tiled.append(grad_arr.reshape(-1, LANES) if i in (5, 6) else grad_arr.reshape(-1, 8, WIDTH))
        tiled += grads[8:]
        small = [jax.ShapeDtypeStruct(arr.shape, bf16) for arr in tiled[1:]]
        *kept, _ = pl.pallas_call(
            kernel,
            out_shape=[pltpu.VMEM((SHARD_ROWS, LANES), f32)] * 3
            + [pltpu.VMEM((OUT_TILES, 8, WIDTH), bf16)]
            + [pltpu.HBM((TAIL_TILES, 8, WIDTH), bf16)],
            in_specs=[any_spec] * 14,
            out_specs=[vmem_spec] * 4 + [any_spec],
            scratch_shapes=[
                pltpu.VMEM((3 * 4 * PIECE_ROWS, LANES), f32),
                pltpu.VMEM((3, 2, PIECE_ROWS, LANES), f32),
                pltpu.VMEM((3, PIECE_ROWS, LANES), f32),
                pltpu.VMEM((3, TILE_ROWS, LANES), f32),
                pltpu.SMEM((5,), f32),
                pltpu.VMEM((1, LANES), f32),
                pltpu.VMEM((DEVS, 1, LANES), f32),
                pltpu.VMEM((2, 3840, LANES), bf16),
                pltpu.VMEM((48, 8, WIDTH), bf16),
                pltpu.VMEM((12, 8, WIDTH), bf16),
                pltpu.VMEM((12, 8, WIDTH), bf16),
                pltpu.VMEM(shapes[8], bf16),
                pltpu.VMEM(shapes[9], bf16),
                pltpu.VMEM((4, 8, WIDTH), bf16),
                dma((7,)), dma((3,)), dma((3 + len(SMALL),)),
                dma((3, 4)), dma((3, 3, 4)), dma((3, 3, 4)), dma((3, 2)), dma((3, 2)), dma((3, 4)), dma((3, 4)),
                dma((4,)), dma((3,)), dma((3,)), dma((DEVS,)), dma((DEVS,)),
                dma((3, 8)), dma((3, 8)), dma((3, 8)), dma((3, 8)), dma((3, LAST_PART + 1)),
            ],
            compiler_params=pltpu.CompilerParams(
                collective_id=0, has_side_effects=True, vmem_limit_bytes=26_500_000),
        )(*tiled, *state, arrays[GRAD_COUNT + 3])
        kept = [pltpu.with_memory_space_constraint(arr, pltpu.VMEM) for arr in kept]
        outs = pl.pallas_call(
            flush,
            out_shape=[jax.ShapeDtypeStruct((EMBED_TILES, 8, WIDTH), bf16)] + small
            + [jax.ShapeDtypeStruct((SHARD_ROWS, LANES), f32)] * 3,
            in_specs=[vmem_spec] * 4,
            out_specs=[any_spec] * 13,
            scratch_shapes=[
                pltpu.VMEM((3840, LANES), f32),
                pltpu.VMEM((2, 3840, LANES), bf16),
                pltpu.VMEM((48, 8, WIDTH), bf16),
                pltpu.VMEM((12, 8, WIDTH), bf16),
                pltpu.VMEM((12, 8, WIDTH), bf16),
                pltpu.VMEM(shapes[8], bf16),
                pltpu.VMEM(shapes[9], bf16),
                dma((FLUSH_PARTS + 16,)),
            ],
            compiler_params=pltpu.CompilerParams(has_side_effects=True, vmem_limit_bytes=4_800_000),
        )(*kept)
        params = []
        for i, dims in enumerate(shapes):
            if i in (1, 2, 3):
                params.append(jnp.swapaxes(outs[i].reshape(dims[0], dims[2], dims[1]), 1, 2))
            else:
                params.append(outs[i].reshape(dims))
        return tuple(params) + tuple(arr.reshape(-1) for arr in outs[GRAD_COUNT:])

    in_specs = tuple([P("dp")] * GRAD_COUNT + [P("dp"), P("dp"), P("dp"), P()])
    out_specs = tuple([P()] * GRAD_COUNT + [P("dp"), P("dp"), P("dp")])
    return jax.shard_map(local_update, mesh=mesh, in_specs=in_specs, out_specs=out_specs, check_vma=False)
```
